256 devices in a mesh: dp: 32 (over z, y), tp: 8 (over x, core).
Axes of the slice: x: 4, y: 4, z: 8, core: 2. Of those that a mesh axis runs over, the one named last changes fastest.
Arguments:
- embed_table: bfloat16 [50304, 2048], P('tp')
- tok_ids: int32 [32, 512], P('dp')
- tok_labels: int32 [32, 512], P('dp')
- trunk_out: bfloat16 [32, 512, 2048], P('dp')
Outputs:
- output 1: float32 [], replicated
- output 2: bfloat16 [32, 512, 2048], P('dp')
- output 3: float32 [50304, 2048], P('tp')
All inputs are finite; a program needn't handle non-finite values.
Results may differ from the reference program's by a relative error of at most 0.001.
Values sent between devices are 32-bit elements.
A program may use at most 768 MiB of HBM per device.

```python
import math
import jax
import jax.numpy as jnp
from jax import lax

VOCAB = 50304
WIDTH = 2048
BATCH = 32
SEQ_LEN = 512
TOKEN_BLOCK = 512
ZIPF_LEVELS = 12
LN_EPS = 1e-5


def skewed_ids(rand_key, out_shape):
    level_key, id_key = jax.random.split(rand_key)
    levels = jax.random.randint(level_key, out_shape, 0, ZIPF_LEVELS, dtype=jnp.int32)
    id_bound = jnp.right_shift(jnp.full(out_shape, VOCAB, jnp.int32), levels)
    drawn_ids = jax.random.randint(id_key, out_shape, 0, id_bound, dtype=jnp.int32)
    return drawn_ids.at[0, 0].set(VOCAB - 1)


def setup_inputs(seed: int = 0) -> dict:
    root_key = jax.random.key(seed)
    table_key, ids_key, label_key, trunk_key = jax.random.split(root_key, 4)
    init_scale = 2.0 / math.sqrt(WIDTH)
    embed_table = (jax.random.normal(table_key, (VOCAB, WIDTH), jnp.float32) * init_scale).astype(jnp.bfloat16)
    tok_ids = skewed_ids(ids_key, (BATCH, SEQ_LEN))
    tok_labels = skewed_ids(label_key, (BATCH, SEQ_LEN))
    trunk_out = (jax.random.normal(trunk_key, (BATCH, SEQ_LEN, WIDTH), jnp.float32) * init_scale).astype(jnp.bfloat16)
    return {'embed_table': embed_table, 'tok_ids': tok_ids, 'tok_labels': tok_labels, 'trunk_out': trunk_out}


def layer_norm(hidden):
    mean_h = jnp.mean(hidden, axis=-1, keepdims=True)
    centered = hidden - mean_h
    inv_std = lax.rsqrt(jnp.mean(centered * centered, axis=-1, keepdims=True) + LN_EPS)
    return centered * inv_std, inv_std


def reference(embed_table, tok_ids, tok_labels, trunk_out):
    rows_blk = min(BATCH, max(1, TOKEN_BLOCK // SEQ_LEN))
    n_blocks = BATCH // rows_blk
    blk_tokens = rows_blk * SEQ_LEN
    tok_total = BATCH * SEQ_LEN
    vocab_pos = jnp.arange(VOCAB)

    def block_step(acc_state, block_in):
        grad_acc, loss_acc = acc_state
        ids_blk, labels_blk, trunk_blk = block_in
        hidden = embed_table[ids_blk].astype(jnp.float32) + trunk_blk.astype(jnp.float32)
        normed, inv_std = layer_norm(hidden)
        normed_bf = normed.astype(jnp.bfloat16)
        logits = jnp.dot(normed_bf, embed_table.T, preferred_element_type=jnp.float32)
        row_max = jnp.max(logits, axis=-1, keepdims=True)
        shifted = jnp.exp(logits - row_max)
        sum_exp = jnp.sum(shifted, axis=-1, keepdims=True)
        onehot = (vocab_pos[None, :] == labels_blk[:, None]).astype(jnp.float32)
        label_logit = jnp.sum(logits * onehot, axis=-1)
        tok_loss = jnp.log(sum_exp[:, 0]) + row_max[:, 0] - label_logit
        grad_logits = ((shifted / sum_exp - onehot) / tok_total).astype(jnp.bfloat16)
        grad_normed = jnp.dot(grad_logits, embed_table, preferred_element_type=jnp.float32)
        mean_g = jnp.mean(grad_normed, axis=-1, keepdims=True)
        mean_gu = jnp.mean(grad_normed * normed, axis=-1, keepdims=True)
        grad_hidden = inv_std * (grad_normed - mean_g - normed * mean_gu)
        head_grad = jnp.dot(grad_logits.T, normed_bf, preferred_element_type=jnp.float32)
        grad_acc = (grad_acc + head_grad).at[ids_blk].add(grad_hidden)
        return (grad_acc, loss_acc + jnp.sum(tok_loss)), grad_hidden.astype(jnp.bfloat16)

    block_in = (tok_ids.reshape(n_blocks, blk_tokens), tok_labels.reshape(n_blocks, blk_tokens), trunk_out.reshape(n_blocks, blk_tokens, WIDTH))
    state_init = (jnp.zeros((VOCAB, WIDTH), jnp.float32), jnp.zeros((), jnp.float32))
    (d_table, loss_sum), d_trunk = lax.scan(block_step, state_init, block_in)
    return loss_sum / tok_total, d_trunk.reshape(BATCH, SEQ_LEN, WIDTH), d_table
```

```python
import functools
import heapq

import jax
import jax.numpy as jnp
from jax import lax
from jax.experimental import pallas as pl
from jax.experimental.pallas import tpu as pltpu
from jax.sharding import PartitionSpec as P

LN_EPS = 1e-5
MESH = pl.DeviceIdType.MESH
F32, BF16 = jnp.float32, jnp.bfloat16
NY, NTP, NX = 4, 8, 4
WAYS = (1, -1)
ALL = Ellipsis
NEG = float(jnp.finfo(jnp.float32).min)
VT = 512
NT_DIMS = (((1,), (1,)), ((), ()))
NN_DIMS = (((1,), (0,)), ((), ()))


def rem(a, b):
    return lax.rem(a, jnp.int32(b))


class Place:
    def __init__(self, nz):
        self.nz = nz
        self.dp = lax.axis_index("dp")
        self.tp = lax.axis_index("tp")
        self.z, self.y = lax.div(self.dp, jnp.int32(NY)), rem(self.dp, NY)
        self.x, self.c = lax.div(self.tp, jnp.int32(2)), rem(self.tp, 2)
        self.partner = 2 * self.x + (1 - self.c)

    def tp_of(self, step, other=False):
        c = 1 - self.c if other else self.c
        return 2 * rem(self.x + step + NX, NX) + c

    def y_of(self, step):
        return rem(self.y + step + NY, NY)

    def dp_of_y(self, step):
        return self.z * NY + self.y_of(step)

    def dp_of_z(self, step):
        return rem(self.z + step + self.nz, self.nz) * NY + self.y


def to_tp(tp):
    return {"tp": tp}


def to_dp(dp):
    return {"dp": dp}


def rdma(src, dst, send_sem, recv_sem, device):
    return pltpu.make_async_remote_copy(
        src_ref=src, dst_ref=dst, send_sem=send_sem, recv_sem=recv_sem, device_id=device, device_id_type=MESH
    )


def greet(devices):
    barrier = pltpu.get_barrier_semaphore()
    for device in devices:
        pl.semaphore_signal(barrier, inc=1, device_id=device, device_id_type=MESH)
    pl.semaphore_wait(barrier, len(devices))


def reduce_scatter_tp(at, src, own, pb, rl, fin, send, recv, meanwhile=lambda: None):
    half = own // 2
    pair = []
    for i, step in enumerate((2, 1, -1, 0)):
        row = pl.multiple_of(at.tp_of(step, True) * own, own)
        pair.append(rdma(src.at[pl.ds(row, own)], pb.at[i], send.at[i], recv.at[i], to_tp(at.partner)))
        pair[-1].start()
    rows = [pl.multiple_of(at.tp_of(step) * own, own) for step in (2, 1, -1, 0)]
    plus, minus = to_tp(at.tp_of(1)), to_tp(at.tp_of(-1))

    def merge(i):
        pair[i].wait_recv()
        pb[i] = pb[i] + src[pl.ds(rows[i], own), :]

    def half_of(i, h):
        return pb.at[i, pl.ds(h * half, half)]

    merge(0)
    far = [
        rdma(half_of(0, 0), rl.at[0], send.at[4], recv.at[4], plus),
        rdma(half_of(0, 1), rl.at[1], send.at[5], recv.at[5], minus),
    ]
    for copy in far:
        copy.start()
    merge(1)
    merge(2)
    near = [
        rdma(half_of(1, 1), fin.at[0], send.at[6], recv.at[6], plus),
        rdma(half_of(2, 0), fin.at[1], send.at[7], recv.at[7], minus),
        rdma(half_of(1, 0), fin.at[2], send.at[8], recv.at[8], plus),
        rdma(half_of(2, 1), fin.at[3], send.at[9], recv.at[9], minus),
    ]
    near[0].start()
    near[1].start()
    far[0].wait_recv()
    pb[1, pl.ds(0, half)] = pb[1, pl.ds(0, half)] + rl[0]
    near[2].start()
    far[1].wait_recv()
    pb[2, pl.ds(half, half)] = pb[2, pl.ds(half, half)] + rl[1]
    near[3].start()
    merge(3)
    meanwhile()
    for copy in near:
        copy.wait_recv()
    top = pb[3, pl.ds(0, half)] + fin[2] + fin[1]
    low = pb[3, pl.ds(half, half)] + fin[0] + fin[3]
    for copy in pair + far + near:
        copy.wait_send()
    return jnp.concatenate([top, low], axis=0)


def gather_plan(sizes, parts, latency, busy=(), hold=0):
    sends, events, heap, busy = [], [], [], dict(busy)

    def post(axis, way, off, lo, hi, order, now):
        end = max(now, busy.get((axis, way), now)) + hi - lo
        busy[axis, way] = end
        there = tuple(o - way * (a == axis) for a, o in enumerate(off))
        heapq.heappush(heap, (end + latency, len(sends), there, lo, hi, order))
        sends.append((axis, way, off, lo, hi))
        return len(sends) - 1

    def ring(axis, way, off, lo, hi, order, now):
        last = sizes[axis] // 2
        gone = abs(off[axis]) + 1
        if gone > last or lo == hi:
            return []
        if gone == last:
            mid = lo + 8 * pl.cdiv(hi - lo, 16)
            lo, hi = (lo, mid) if way > 0 else (mid, hi)
        return [post(axis, way, off, lo, hi, order, now)]

    starts = [[] for _ in parts]
    for leg in range(2):
        for begin, (lo, hi, order, now) in zip(starts, parts):
            for way in WAYS:
                begin += ring(order[leg], way, (0, 0), lo, hi, order, now)
    while heap:
        now, i, off, lo, hi, order = heapq.heappop(heap)
        axis, way = sends[i][:2]
        if off[1] and now < hold:
            heapq.heappush(heap, (hold, i, off, lo, hi, order))
            continue
        new = ring(axis, way, off, lo, hi, order, now)
        if axis == order[0]:
            for w in WAYS:
                new += ring(order[1], w, off, lo, hi, order, now)
        events.append((i, new, now))
    return sends, starts, events


def two_colours(lo, hi, share, now=0):
    split = lo + 8 * round((hi - lo) * share / 8)
    return [(lo, split, (0, 1), now), (split, hi, (1, 0), now)]


class Spread:
    def __init__(self, at, plan, rows, block, send, recv):
        self.sends, self.starts, self.events = plan
        self.block, self.send, self.recv, self.rows = block, send, recv, rows
        self.count = len(self.sends)
        self.other = to_tp(at.partner)
        self.device = {}
        for way in WAYS:
            self.device[0, way] = to_tp(at.tp_of(way))
            self.device[1, way] = to_dp(at.dp_of_y(way))

    def goal(self, i):
        axis, way, off = self.sends[i][:3]
        return tuple(o - way * (a == axis) for a, o in enumerate(off))

    def copy(self, i):
        axis, way, off, lo, hi = self.sends[i]
        src, dst = self.block(*off, False, lo, hi), self.block(off[0], self.goal(i)[1], False, lo, hi)
        return rdma(src, dst, self.send.at[i], self.recv.at[i], self.device[axis, way])

    def forward(self, i, cross=False):
        off, (lo, hi) = ((0, 0), (0, self.rows)) if i == self.count else (self.goal(i), self.sends[i][-2:])
        ref = self.block(*off, cross, lo, hi)
        return rdma(ref, ref, self.send.at[self.count + i], self.recv.at[self.count + i], self.other)

    def begin(self):
        for i in sum(self.starts, []):
            self.copy(i).start()
        self.forward(self.count).start()

    def run(self, events):
        for i, new, _ in events:
            ref = self.block(*self.goal(i), False, *self.sends[i][-2:])
            rdma(ref, ref, self.send.at[i], self.recv.at[i], self.other).wait_recv()
            for j in new:
                self.copy(j).start()
            self.forward(i).start()

    def take(self, i):
        self.forward(i, True).wait_recv()

    def end(self):
        for i in range(self.count):
            self.copy(i).wait_send()
        for i in range(self.count + 1):
            self.forward(i).wait_send()


def token_kernel(
    nz, tok_total, plan, table, part, trunk, lab_col, lab_row, ids,
    du, ub_out, ub_far, u_out, r_out, stats, tiles,
    table_v, ub_v, z_v, run, mine, theirs, row_out, row_in, tile_out, tile_in, pb, rl, fin, land,
    load_sem, part_sem, st_send, st_recv, row_send, row_recv, t_send, t_recv, rs_send, rs_recv, x_send, x_recv,
):
    at = Place(nz)
    rows, width = table_v.shape
    toks = ub_v.shape[0]
    own = trunk.shape[0]
    steps = z_v.shape[0]
    whole = rows // VT
    tail = rows - whole * VT

    part_copy = pltpu.make_async_copy(part, du, part_sem)
    part_copy.start()

    def load(i):
        start = pl.multiple_of(i * VT, 16)
        return pltpu.make_async_copy(table.at[pl.ds(start, VT)], table_v.at[pl.ds(start, VT)], load_sem.at[i])

    tail_copy = pltpu.make_async_copy(
        table.at[pl.ds(whole * VT, tail)], table_v.at[pl.ds(whole * VT, tail)], load_sem.at[whole]
    )
    greet([to_tp(rem(at.tp + i, NTP)) for i in range(1, NTP)] + [to_dp(at.dp_of_y(i)) for i in range(1, NY)])
    part_copy.wait()
    for i in range(whole):
        load(i).start()
    tail_copy.start()
    hidden = reduce_scatter_tp(at, du, own, pb, rl, fin, rs_send, rs_recv) + trunk[ALL].astype(F32)
    centered = hidden - jnp.mean(hidden, axis=-1, keepdims=True)
    inv_std = lax.rsqrt(jnp.mean(centered * centered, axis=-1, keepdims=True) + LN_EPS)
    normed = centered * inv_std
    land[at.tp] = normed.astype(BF16).astype(F32)

    def block(dx, dy, cross, lo, hi):
        tp, cut = at.tp_of(dx, cross), pl.ds(lo, hi - lo)
        return ub_far.at[dy % NY - 1, tp, cut] if dy % NY else land.at[tp, cut]

    spread = Spread(at, plan, own, block, x_send, x_recv)
    spread.begin()
    u_out[ALL] = normed
    r_out[ALL] = jnp.broadcast_to(inv_std, r_out.shape)
    near = [e for e in spread.events if spread.goal(e[0])[1] == 0]
    spread.run(near)
    for e in near:
        spread.take(e[0])
    spread.take(spread.count)
    groups = {}
    pace = own / 7.5
    for e in [e for e in spread.events if e not in near]:
        due = max(0, int((e[-1] - near[-1][-1]) / pace)) + 2
        groups.setdefault(due if due <= steps else max(steps, due - 5), []).append(e)
    late = [e for due in sorted(groups) if due >= 2 * steps for e in groups[due]]

    def attend(step):
        for due, events in groups.items():
            if due < 2 * steps:

                @pl.when(step == due)
                def _(events=events):
                    spread.run(events)

    keep = pltpu.make_async_copy(land, ub_out, part_sem)
    keep.start()
    ub_v[ALL] = land[ALL].reshape(toks, width).astype(BF16)
    run[0] = jnp.full(run.shape[1:], NEG, F32)
    run[1] = jnp.zeros(run.shape[1:], F32)
    lane = lax.broadcasted_iota(jnp.int32, (toks, VT), 1)

    def start_of(i):
        return pl.multiple_of(jnp.minimum(i * VT, rows - VT), 16)

    def fold(op, v):
        return functools.reduce(op, [v[:, j : j + 128] for j in range(0, VT, 128)])

    def forward(i, carry):
        attend(i)

        @pl.when(i < whole)
        def _():
            load(i).wait()

        @pl.when(i == whole)
        def _():
            tail_copy.wait()

        start = start_of(i)
        z = lax.dot_general(ub_v[ALL], table_v[pl.ds(start, VT), :], NT_DIMS, preferred_element_type=F32)
        z = jnp.where(lane >= i * VT - start, z, NEG)
        z_v[i] = z
        run[0] = jnp.maximum(run[0], fold(jnp.maximum, z))
        hit = (lane + start == lab_col[ALL]) & (lane >= i * VT - start)
        run[1] = run[1] + fold(jnp.add, jnp.where(hit, z, 0.0))
        return carry

    lax.fori_loop(0, steps, forward, 0)
    top = jnp.max(run[0], axis=1, keepdims=True)
    run[0] = jnp.zeros(run.shape[1:], F32)

    def exps(i, carry):
        run[0] = run[0] + fold(jnp.add, jnp.exp(z_v[i] - top))
        return carry

    lax.fori_loop(0, steps, exps, 0)
    sums = jnp.sum(run[0], axis=1, keepdims=True)
    label = jnp.sum(run[1], axis=1, keepdims=True)
    narrow = lax.broadcasted_iota(jnp.int32, (toks, 128), 1)
    packed = jnp.where(narrow == 0, top, jnp.where(narrow == 1, sums, jnp.where(narrow == 2, label, 0.0)))
    mine[ALL] = jnp.transpose(packed)[:8]
    stat = []
    for i in range(1, NTP):
        stat.append(rdma(mine, theirs.at[i], st_send.at[i], st_recv.at[i], to_tp(rem(at.tp + i, NTP))))
        stat[-1].start()
    theirs[0] = mine[ALL]
    for copy in stat:
        copy.wait_recv()
    parts = [theirs[rem(at.tp - j + NTP, NTP)] for j in range(NTP)]
    peak = functools.reduce(jnp.maximum, [p[0:1] for p in parts])
    total = functools.reduce(jnp.add, [p[1:2] * jnp.exp(p[0:1] - peak) for p in parts])
    label = functools.reduce(jnp.add, [p[2:3] for p in parts])
    lse = peak + jnp.log(total)
    loss = jnp.sum(jnp.log(total) + peak - label, axis=1, keepdims=True)
    sub = lax.broadcasted_iota(jnp.int32, (8, toks), 0)
    row_out[ALL] = jnp.where(sub == 0, lse, jnp.where(sub == 1, lab_row[ALL], 0.0))
    tiles[0, 0:8] = ids[ALL]
    tiles[0, 8:16] = jnp.broadcast_to(loss, ids.shape)
    tile_out[ALL] = tiles[0]
    rows_sent = []
    for i in range(NY - 1):
        to_y = to_dp(at.dp_of_y(NY - 1 - i))
        rows_sent.append(rdma(row_out, row_in.at[i], row_send.at[i], row_recv.at[i], to_y))
        rows_sent.append(rdma(tile_out, tile_in.at[i], t_send.at[i], t_recv.at[i], to_y))
    for copy in rows_sent:
        copy.start()
    run[0] = jnp.transpose(jnp.broadcast_to(lse, (128, toks)))
    wide = min(512, width)
    inv_total = 1.0 / tok_total
    du[ALL] = jnp.zeros(du.shape, F32)

    def backward(i, carry):
        attend(i + steps)
        start = start_of(i)
        shift = jnp.concatenate([run[0]] * (VT // 128), axis=1)
        prob = jnp.exp(z_v[i] - shift)
        hit = (lane + start == lab_col[ALL]) & (lane >= i * VT - start)
        grad = ((prob - jnp.where(hit, 1.0, 0.0)) * inv_total).astype(BF16)
        for n in range(width // wide):
            cols = pl.ds(n * wide, wide)
            du[:, cols] = du[:, cols] + lax.dot_general(
                grad, table_v[pl.ds(start, VT), cols], NN_DIMS, preferred_element_type=F32
            )
        return carry

    lax.fori_loop(0, steps, backward, 0)
    spread.run(late)
    for e in spread.events:
        if e not in near:
            spread.take(e[0])
    for copy in rows_sent:
        copy.wait_recv()
    stats[0] = row_out[ALL]
    for i in range(NY - 1):
        stats[i + 1] = row_in[i]
        tiles[i + 1] = tile_in[i]
    keep.wait()
    spread.end()
    for copy in stat + rows_sent:
        copy.wait_send()


def head_kernel(nz, stride, tok_total, table, ub, ub_far, stats, out, table_v, ub_v, stage, grad_v, load_sem, stage_sem):
    step = pl.program_id(0)
    dp, tp = lax.axis_index("dp"), lax.axis_index("tp")
    win, width = table_v.shape
    tile = out.shape[1]
    toks = stage.shape[1]
    first = pl.multiple_of(rem(dp, NY) * stride, 16)

    @pl.when(step == 0)
    def _():
        load = pltpu.make_async_copy(table.at[pl.ds(first, win)], table_v, load_sem)
        load.start()
        copies = [pltpu.make_async_copy(ub, stage.at[0], stage_sem.at[0])]
        for i in range(1, NY):
            copies.append(pltpu.make_async_copy(ub_far.at[i - 1], stage.at[i % 2], stage_sem.at[i % 2]))
        copies[0].start()
        copies[1].start()
        for i in range(NY):
            copies[i].wait()
            ub_v[pl.ds(i * toks, toks)] = stage[i % 2].astype(BF16)
            if i + 2 < NY:
                copies[i + 2].start()
        load.wait()

    begin = pl.multiple_of(step * tile, 16)
    vocab = tp * table.shape[0] + first + begin + lax.broadcasted_iota(jnp.int32, (tile, toks), 0)
    inv_total = 1.0 / tok_total

    def logits(n, carry):
        at_tok = pl.multiple_of(n * toks, 128)
        z = lax.dot_general(
            table_v[pl.ds(begin, tile), :], ub_v[pl.ds(at_tok, toks), :], NT_DIMS, preferred_element_type=F32
        )
        row = stats[n]
        prob = jnp.exp(z - row[0:1])
        hit = vocab == row[1:2].astype(jnp.int32)
        grad_v[:, pl.ds(at_tok, toks)] = ((prob - jnp.where(hit, 1.0, 0.0)) * inv_total).astype(BF16)
        return carry

    lax.fori_loop(0, NY, logits, 0)
    cols = out.shape[2]

    def sums(n, carry):
        at_col = pl.multiple_of(n * cols, 128)
        out[n] = jnp.dot(grad_v[ALL], ub_v[:, pl.ds(at_col, cols)], preferred_element_type=F32)
        return carry

    lax.fori_loop(0, nz, sums, 0)


class SumZ:
    def __init__(self, at, source, parts, came, total, chunks, send, recv):
        self.at, self.source, self.parts, self.came, self.total = at, source, parts, came, total
        self.chunks, self.send, self.recv = chunks, send, recv
        self.last = at.nz // 2

    def rows(self, c, s, way):
        lo, hi = self.chunks[c]
        if s == 1:
            mid = lo + 8 * pl.cdiv(hi - lo, 16)
            lo, hi = (lo, mid) if way > 0 else (mid, hi)
        return pl.ds(lo, hi - lo)

    def goal(self, s, way):
        return rem(self.at.z + way * (self.last + 1 - s) + self.at.nz, self.at.nz)

    def copy(self, c, s, way):
        rows, w = self.rows(c, s, way), WAYS.index(way)
        src = (self.source if s == 1 else self.parts).at[self.goal(s, way), rows]
        sems = self.send.at[w, s, c], self.recv.at[w, s, c]
        return rdma(src, self.came.at[w, s - 1, rows], *sems, to_dp(self.at.dp_of_z(way)))

    def begin(self):
        for c in range(len(self.chunks)):
            for way in WAYS:
                self.copy(c, 1, way).start()

    def run(self, c, s):
        for w, way in enumerate(WAYS):
            self.copy(c, s, way).wait_recv()
            rows = self.rows(c, s, way)
            if s < self.last:
                goal = self.goal(s + 1, way)
                self.parts[goal, rows] = self.parts[goal, rows] + self.came[w, s - 1, rows]
                self.copy(c, s + 1, way).start()
            else:
                self.total[rows] = self.total[rows] + self.came[w, s - 1, rows]

    def end(self):
        for c in range(len(self.chunks)):
            for s in range(self.last):
                for way in WAYS:
                    self.copy(c, s + 1, way).wait_send()


def finish_kernel(
    nz, stride, vocab_loc, row_plan, dh_plan, table_plan, chunks, du, u, r, tiles, head,
    d_trunk, loss, stack,
    pb, rl, fin, land, all_dh, all_tiles, parts, came, total,
    rs_send, rs_recv, row_send, row_recv, z_send, z_recv, i_send, i_recv, x_send, x_recv, s_send, s_recv, t_send, t_recv,
    load_sem,
):
    at = Place(nz)
    own, width = u.shape
    cols = width // nz
    block = nz * own
    load = pltpu.make_async_copy(head, parts, load_sem)
    load.start()
    greet(
        [to_tp(rem(at.tp + i, NTP)) for i in range(1, NTP)]
        + [to_dp(at.dp_of_z(i)) for i in range(1, nz)]
        + [to_dp(at.dp_of_y(way)) for way in WAYS]
    )
    sums = SumZ(at, head, parts, came, total, chunks, s_send, s_recv)
    sums.begin()
    todo = [(c, s) for s in range(1, sums.last + 1) for c in range(len(chunks))]

    def first_sum():
        load.wait()
        total[ALL] = parts[at.z]
        sums.run(*todo[0])

    grad = reduce_scatter_tp(at, du, own, pb, rl, fin, rs_send, rs_recv, first_sum)
    normed = u[ALL]
    mean_g = jnp.mean(grad, axis=-1, keepdims=True)
    mean_gu = jnp.mean(grad * normed, axis=-1, keepdims=True)
    land[at.tp] = r[:, 0:1] * (grad - mean_g - normed * mean_gu)

    def row_block(dx, dy, cross, lo, hi):
        return land.at[at.tp_of(dx, cross), pl.ds(lo, hi - lo)]

    whole_rows = Spread(at, row_plan, own, row_block, row_send, row_recv)
    whole_rows.begin()
    here = pl.multiple_of(at.z * own, own)
    turned = []
    for i in range(1, nz):
        col, to_z = pl.multiple_of(rem(at.z + i, nz) * cols, 128), to_dp(at.dp_of_z(i))
        turned.append(
            rdma(
                land.at[at.tp, :, pl.ds(col, cols)], all_dh.at[at.tp, 0, pl.ds(here, own)],
                z_send.at[i], z_recv.at[i], to_z,
            )
        )
        turned.append(rdma(tiles, all_tiles.at[at.z], i_send.at[i], i_recv.at[i], to_z))
    for copy in turned:
        copy.start()
    my_col = pl.multiple_of(at.z * cols, 128)
    all_dh[at.tp, 0, pl.ds(here, own)] = land[at.tp, :, pl.ds(my_col, cols)]
    all_tiles[at.z] = tiles[ALL]
    for c, s in todo[1 : len(chunks)]:
        sums.run(c, s)
    whole_rows.run(whole_rows.events)
    for copy in turned:
        copy.wait_recv()

    def dh_block(dx, dy, cross, lo, hi):
        return all_dh.at[at.tp_of(dx, cross), dy % NY, pl.ds(lo, hi - lo)]

    blocks = Spread(at, dh_plan, block, dh_block, x_send, x_recv)
    blocks.begin()
    for i in range(whole_rows.count + 1):
        whole_rows.take(i)
    d_trunk[ALL] = land[ALL].reshape(d_trunk.shape).astype(BF16)
    loss[ALL] = sum(
        all_tiles[z, rem(y - at.y + NY, NY), 8:16] for z in range(nz) for y in range(NY)
    )

    pieces = {(0, 0): [(blocks.count, [], 0)]}
    for e in blocks.events:
        dx, dy = blocks.goal(e[0])
        pieces.setdefault((dx % NX, dy % NY), []).append(e)
    order = sorted((pieces[p][-1][-1] + cross * (block // 3), *p, cross) for p in pieces for cross in range(2))
    left = list(blocks.events)
    due = []
    for time, dx, dy, cross in order:
        due.append([e for e in left if e[-1] <= time])
        left = [e for e in left if e[-1] > time]
    code = [dx + NX * (dy + NY * cross) for _, dx, dy, cross in order]
    beside = {k * len(order) // 3: todo[len(chunks) + k] for k in range(min(3, len(todo) - len(chunks)))}

    win = total.shape[0]
    tile = win // 3 if win % 48 == 0 else win
    low = (at.tp * vocab_loc + at.y * stride).astype(F32)

    def piece(e, carry):
        mark = jnp.int32(code[0])
        for k in range(len(order)):
            mark = jnp.where(e == k, code[k], mark)
            _, dx, dy, cross = order[k]
            if due[k] or cross or k in beside:

                @pl.when(e == k)
                def _(k=k, dx=dx, dy=dy, cross=cross):
                    if k in beside:
                        sums.run(*beside[k])
                    blocks.run(due[k])
                    if cross:
                        for part in pieces[dx, dy]:
                            blocks.take(part[0])

        core = jnp.where(mark >= NX * NY, 1 - at.c, at.c)
        tp = 2 * rem(at.x + rem(mark, NX), NX) + core
        far = rem(lax.div(mark, jnp.int32(NX)), NY)
        ids = jnp.concatenate(
            [
                all_tiles[2 * j, far, pl.ds(tp, 1), :] + all_tiles[2 * j + 1, far, pl.ds(tp, 1), :]
                for j in range(nz // 2)
            ],
            axis=1,
        )
        dh = all_dh[tp, far]
        hi = dh.astype(BF16)
        rest = dh - hi.astype(F32)
        mid = rest.astype(BF16)
        lo = (rest - mid.astype(F32)).astype(BF16)
        ids = (ids - low).astype(jnp.int32)
        for begin in range(0, win, tile):
            row = lax.broadcasted_iota(jnp.int32, (tile, block), 0) + begin
            pick = jnp.where(row == ids, 1.0, 0.0).astype(BF16)
            found = sum(jnp.dot(pick, term, preferred_element_type=F32) for term in (hi, mid, lo))
            total[begin : begin + tile] = total[begin : begin + tile] + found
        return carry

    lax.fori_loop(0, len(order), piece, 0)
    for copy in turned:
        copy.wait_send()

    sends, starts, events = table_plan
    device = {(0, way): to_dp(at.dp_of_z(way)) for way in WAYS} | {(1, way): to_dp(at.dp_of_y(way)) for way in WAYS}

    def copy_of(i, arrives=False):
        axis, way, off, lo, hi = sends[i]
        if arrives:
            off = tuple(o - way * (a == axis) for a, o in enumerate(off))
        dst = stack.at[rem(at.z + off[0] + nz, nz), at.y_of(off[1]), pl.ds(lo, hi - lo)]
        src = dst if any(off) else total.at[pl.ds(lo, hi - lo)]
        return rdma(src, dst, t_send.at[i], t_recv.at[i], device[axis, way])

    keeps = []
    after = todo[len(chunks) + len(beside) :]
    for c, (lo, hi) in enumerate(chunks):
        while (c, sums.last) in after:
            sums.run(*after.pop(0))
        for i in sum(starts[2 * c : 2 * c + 2], []):
            copy_of(i).start()
        rows = pl.ds(lo, hi - lo)
        keeps.append(pltpu.make_async_copy(total.at[rows], stack.at[at.z, at.y, rows], load_sem))
    for i, new, _ in events:
        copy_of(i, True).wait_recv()
        for j in new:
            copy_of(j).start()
    for keep in keeps:
        keep.start()
        keep.wait()
    for i in range(len(sends)):
        copy_of(i).wait_send()
    sums.end()
    whole_rows.end()
    blocks.end()


def place_kernel(chunk, stack, out, slots, load_sem, store_sem):
    nz, ny, have, cols = stack.shape
    depth = slots.shape[0]
    per = have // chunk
    total = ny * per
    ahead = depth // 2

    def load(i):
        y, row = lax.div(i, jnp.int32(per)), pl.multiple_of(rem(i, per) * chunk, 8)
        s = rem(i, depth)
        return pltpu.make_async_copy(stack.at[:, y, pl.ds(row, chunk)], slots.at[s], load_sem.at[s])

    def stores(i):
        s, row = rem(i, depth), pl.multiple_of(i * chunk, 8)
        return [
            pltpu.make_async_copy(slots.at[s, j], out.at[pl.ds(row, chunk), pl.ds(j * cols, cols)], store_sem.at[s, j])
            for j in range(nz)
        ]

    def prime(i, carry):
        load(i).start()
        return carry

    def body(i, carry):
        load(i).wait()
        for copy in stores(i):
            copy.start()

        @pl.when(i + ahead < total)
        def _():
            @pl.when(i >= ahead)
            def _():
                for copy in stores(i - ahead):
                    copy.wait()

            load(i + ahead).start()

        return carry

    def drain(i, carry):
        for copy in stores(i):
            copy.wait()
        return carry

    lax.fori_loop(0, ahead, prime, 0)
    lax.fori_loop(0, total, body, 0)
    lax.fori_loop(total - 2 * ahead, total, drain, 0)
    used = per * chunk
    left = have - used
    rest = pltpu.make_async_copy(stack.at[:, ny - 1, pl.ds(used, left)], slots.at[0, :, pl.ds(0, left)], load_sem.at[0])
    rest.start()
    rest.wait()
    tails = [
        pltpu.make_async_copy(
            slots.at[0, j, pl.ds(0, left)], out.at[pl.ds(ny * used, left), pl.ds(j * cols, cols)], store_sem.at[0, j]
        )
        for j in range(nz)
    ]
    for copy in tails:
        copy.start()
    for copy in tails:
        copy.wait()


def vmem():
    return pl.BlockSpec(memory_space=pltpu.VMEM)


def anywhere():
    return pl.BlockSpec(memory_space=pl.ANY)


def dma(*shape):
    return pltpu.SemaphoreType.DMA(shape)


def solution(mesh):
    ndp, ntp = mesh.shape["dp"], mesh.shape["tp"]
    nz = ndp // NY

    def per_device(table, ids, labels, trunk):
        vocab_loc, width = table.shape
        batch, seq = ids.shape
        toks = batch * seq
        own = toks // NTP
        tok_total = toks * ndp
        stride = (vocab_loc - 16) // NY
        win = stride + 16
        cols = width // nz
        block = nz * own
        big = 66_000_000
        dp, tp = lax.axis_index("dp"), lax.axis_index("tp")
        row_start = tp * vocab_loc
        local_ids = ids.reshape(toks) - row_start
        own_ids = jnp.where((local_ids >= 0) & (local_ids < vocab_loc), local_ids, vocab_loc)
        part = jnp.take(table, own_ids, axis=0, mode="fill", fill_value=0).astype(F32)
        trunk_own = lax.dynamic_slice_in_dim(trunk.reshape(toks, width), tp * own, own, 0)

        tp_scratch = [
            pltpu.VMEM((4, own, width), F32),
            pltpu.VMEM((2, own // 2, width), F32),
            pltpu.VMEM((4, own // 2, width), F32),
            pltpu.VMEM((NTP, own, width), F32),
        ]
        ids_f = ids.reshape(NTP, own).astype(F32)
        blank = jnp.zeros_like(ids_f)
        even = rem(lax.div(dp, jnp.int32(NY)), 2) == 0
        pad = ((0, 0), (0, 128 - 2 * own))
        ids_tile = jnp.pad(jnp.concatenate([jnp.where(even, ids_f, blank), jnp.where(even, blank, ids_f)], axis=1), pad)
        lab_col = labels.reshape(toks, 1) - row_start
        lab_row = labels.reshape(1, toks).astype(F32)
        steps = pl.cdiv(vocab_loc, VT)
        token_plan = gather_plan((NX, NY), two_colours(0, own, 0.5), 16, hold=2 * own)
        sends = 2 * len(token_plan[0]) + 1
        du, ub, ub_far, u_own, r_own, stats, tiles = pl.pallas_call(
            functools.partial(token_kernel, nz, tok_total, token_plan),
            out_shape=(
                jax.ShapeDtypeStruct((toks, width), F32),
                jax.ShapeDtypeStruct((NTP, own, width), F32),
                jax.ShapeDtypeStruct((NY - 1, NTP, own, width), F32),
                jax.ShapeDtypeStruct((own, width), F32),
                jax.ShapeDtypeStruct((own, 128), F32),
                jax.ShapeDtypeStruct((NY, 8, toks), F32),
                jax.ShapeDtypeStruct((NY, 16, 128), F32),
            ),
            in_specs=[anywhere(), anywhere(), vmem(), vmem(), vmem(), vmem()],
            out_specs=(vmem(), anywhere(), anywhere(), vmem(), vmem(), vmem(), vmem()),
            scratch_shapes=[
                pltpu.VMEM((vocab_loc, width), BF16),
                pltpu.VMEM((toks, width), BF16),
                pltpu.VMEM((steps, toks, VT), F32),
                pltpu.VMEM((2, toks, 128), F32),
                pltpu.VMEM((8, toks), F32),
                pltpu.VMEM((NTP, 8, toks), F32),
                pltpu.VMEM((8, toks), F32),
                pltpu.VMEM((NY - 1, 8, toks), F32),
                pltpu.VMEM((16, 128), F32),
                pltpu.VMEM((NY - 1, 16, 128), F32),
                *tp_scratch,
                dma(steps), pltpu.SemaphoreType.DMA, dma(NTP), dma(NTP),
                dma(NY - 1), dma(NY - 1), dma(NY - 1), dma(NY - 1), dma(10), dma(10), dma(sends), dma(sends),
            ],
            compiler_params=pltpu.CompilerParams(collective_id=0, has_side_effects=True, vmem_limit_bytes=big),
            name="token",
        )(table, part, trunk_own, lab_col, lab_row, ids_tile)

        tile = win // 3 if win % 48 == 0 else win
        head = pl.pallas_call(
            functools.partial(head_kernel, nz, stride, tok_total),
            out_shape=jax.ShapeDtypeStruct((nz, win, cols), F32),
            grid=(win // tile,),
            in_specs=[anywhere(), anywhere(), anywhere(), vmem()],
            out_specs=pl.BlockSpec((nz, tile, cols), lambda i: (0, i, 0)),
            scratch_shapes=[
                pltpu.VMEM((win, width), BF16),
                pltpu.VMEM((NY * toks, width), BF16),
                pltpu.VMEM((2, toks, width), F32),
                pltpu.VMEM((tile, NY * toks), BF16),
                pltpu.SemaphoreType.DMA, dma(2),
            ],
            compiler_params=pltpu.CompilerParams(vmem_limit_bytes=big),
            cost_estimate=pl.CostEstimate(flops=4 * NY * toks * win * width, bytes_accessed=40_000_000, transcendentals=0),
            name="head",
        )(table, ub.reshape(toks, width), ub_far.reshape(NY - 1, toks, width), stats)

        row_plan = gather_plan((NX, 1), two_colours(0, own, 1), 16)
        dh_plan = gather_plan((NX, NY), two_colours(0, block, 0.5), block // 4)
        half = 8 * pl.cdiv(win, 16)
        chunks = ((0, half), (half, win))
        share = 0.62 if nz == 8 else 0.5
        table_parts = two_colours(0, half, share) + two_colours(half, win, share, half)
        table_plan = gather_plan((nz, NY), table_parts, 60, {(0, way): half for way in WAYS})
        counts = [2 * len(p[0]) + 1 for p in (row_plan, dh_plan, table_plan)]
        zs = (2, nz // 2 + 1, len(chunks))
        d_rows, loss, stack = pl.pallas_call(
            functools.partial(finish_kernel, nz, stride, vocab_loc, row_plan, dh_plan, table_plan, chunks),
            out_shape=(
                jax.ShapeDtypeStruct((toks, width), BF16),
                jax.ShapeDtypeStruct((8, 128), F32),
                jax.ShapeDtypeStruct((nz, NY, win, cols), F32),
            ),
            in_specs=[vmem(), vmem(), vmem(), vmem(), anywhere()],
            out_specs=(vmem(), vmem(), anywhere()),
            scratch_shapes=[
                *tp_scratch,
                pltpu.VMEM((NTP, NY, block, cols), F32),
                pltpu.VMEM((nz, NY, 16, 128), F32),
                pltpu.VMEM((nz, win, cols), F32),
                pltpu.VMEM((2, nz // 2, win, cols), F32),
                pltpu.VMEM((win, cols), F32),
                dma(10), dma(10), dma(counts[0]), dma(counts[0]), dma(nz), dma(nz), dma(nz), dma(nz),
                dma(counts[1]), dma(counts[1]), dma(*zs), dma(*zs), dma(counts[2]), dma(counts[2]),
                pltpu.SemaphoreType.DMA,
            ],
            compiler_params=pltpu.CompilerParams(collective_id=1, has_side_effects=True, vmem_limit_bytes=67_000_000),
            name="finish",
        )(du, u_own, r_own, tiles, head)
        depth = 8
        chunk = next(n for n in range(224, 0, -8) if stride % n == 0 and NY * stride >= n * depth)
        d_table = pl.pallas_call(
            functools.partial(place_kernel, chunk),
            out_shape=jax.ShapeDtypeStruct((vocab_loc, width), F32),
            in_specs=[anywhere()],
            out_specs=anywhere(),
            scratch_shapes=[pltpu.VMEM((depth, nz, chunk, cols), F32), dma(depth), dma(depth, nz)],
            compiler_params=pltpu.CompilerParams(vmem_limit_bytes=big),
            name="place",
        )(stack)
        mean_loss = loss[0, 0] / tok_total
        return mean_loss, d_rows.reshape(trunk.shape), d_table

    return jax.shard_map(
        per_device,
        mesh=mesh,
        in_specs=(P("tp", None), P("dp", None), P("dp", None), P("dp", None, None)),
        out_specs=(P(), P("dp", None, None), P("tp", None)),
        check_vma=False,
    )
```

```python
import functools
import heapq

import jax
import jax.numpy as jnp
from jax import lax
from jax.experimental import pallas as pl
from jax.experimental.pallas import tpu as pltpu
from jax.sharding import PartitionSpec as P

LN_EPS = 1e-5
MESH = pl.DeviceIdType.MESH
F32, BF16 = jnp.float32, jnp.bfloat16
NY, NTP, NX = 4, 8, 4
WAYS = (1, -1)
PACE = ((10, 0), (20, 15), (20, 26))
SHARES = (0.55, 0.55, 0.7)
ALL = Ellipsis
NEG = float(jnp.finfo(jnp.float32).min)
VT = 512
NT_DIMS = (((1,), (1,)), ((), ()))
NN_DIMS = (((1,), (0,)), ((), ()))


def rem(a, b):
    return lax.rem(a, jnp.int32(b))


class Place:
    def __init__(self, nz):
        self.nz = nz
        self.dp = lax.axis_index("dp")
        self.tp = lax.axis_index("tp")
        self.z, self.y = lax.div(self.dp, jnp.int32(NY)), rem(self.dp, NY)
        self.x, self.c = lax.div(self.tp, jnp.int32(2)), rem(self.tp, 2)
        self.partner = 2 * self.x + (1 - self.c)

    def tp_of(self, step, other=False):
        c = 1 - self.c if other else self.c
        return 2 * rem(self.x + step + NX, NX) + c

    def y_of(self, step):
        return rem(self.y + step + NY, NY)

    def dp_of_y(self, step):
        return self.z * NY + self.y_of(step)

    def dp_of_z(self, step):
        return rem(self.z + step + self.nz, self.nz) * NY + self.y


def to_tp(tp):
    return {"tp": tp}


def to_dp(dp):
    return {"dp": dp}


def rdma(src, dst, send_sem, recv_sem, device):
    return pltpu.make_async_remote_copy(
        src_ref=src, dst_ref=dst, send_sem=send_sem, recv_sem=recv_sem, device_id=device, device_id_type=MESH
    )


def greet(devices):
    barrier = pltpu.get_barrier_semaphore()
    for device in devices:
        pl.semaphore_signal(barrier, inc=1, device_id=device, device_id_type=MESH)
    pl.semaphore_wait(barrier, len(devices))


class SumTp:
    def __init__(self, at, src, own, pb, rl, fin, send, recv):
        self.src, self.own, self.half, self.pb, self.rl, self.fin = src, own, own // 2, pb, rl, fin
        self.at, self.send, self.recv = at, send, recv
        self.steps = (2, 1, -1, 0)
        self.copies = []

    def copy(self, i, src, dst, tp):
        self.copies.append(rdma(src, dst, self.send.at[i], self.recv.at[i], to_tp(tp)))
        return self.copies[-1]

    def rows(self, step, other):
        return pl.ds(pl.multiple_of(self.at.tp_of(step, other) * self.own, self.own), self.own)

    def part(self, i, h):
        return self.pb.at[i, pl.ds(h * self.half, self.half)]

    def begin(self):
        for i, step in enumerate(self.steps):
            self.copy(i, self.src.at[self.rows(step, True)], self.pb.at[i], self.at.partner).start()

    def merge(self, i):
        self.copies[i].wait_recv()
        self.pb[i] = self.pb[i] + self.src[self.rows(self.steps[i], False), :]

    def pass_on(self):
        plus, minus = self.at.tp_of(1), self.at.tp_of(-1)
        self.merge(0)
        for h, tp in enumerate((plus, minus)):
            self.copy(4 + h, self.part(0, h), self.rl.at[h], tp).start()
        self.merge(1)
        self.merge(2)
        self.copy(6, self.part(1, 1), self.fin.at[0], plus).start()
        self.copy(7, self.part(2, 0), self.fin.at[1], minus).start()

    def join(self):
        for h, tp in enumerate((self.at.tp_of(1), self.at.tp_of(-1))):
            self.copies[4 + h].wait_recv()
            rows = pl.ds(h * self.half, self.half)
            self.pb[1 + h, rows] = self.pb[1 + h, rows] + self.rl[h]
            self.copy(8 + h, self.part(1 + h, h), self.fin.at[2 + h], tp).start()
        self.merge(3)

    def result(self):
        for copy in self.copies[6:]:
            copy.wait_recv()
        top = self.pb[3, 0 : self.half] + self.fin[2] + self.fin[1]
        low = self.pb[3, self.half : self.own] + self.fin[0] + self.fin[3]
        for copy in self.copies:
            copy.wait_send()
        return jnp.concatenate([top, low], axis=0)


def gather_plan(sizes, parts, latency, hold=0):
    sends, events, heap, busy = [], [], [], {}

    def post(axis, way, off, lo, hi, order, now):
        end = max(now, busy.get((axis, way), now)) + hi - lo
        busy[axis, way] = end
        there = tuple(o - way * (a == axis) for a, o in enumerate(off))
        heapq.heappush(heap, (end + latency, len(sends), there, lo, hi, order))
        sends.append((axis, way, off, lo, hi))
        return len(sends) - 1

    def ring(axis, way, off, lo, hi, order, now):
        last = sizes[axis] // 2
        gone = abs(off[axis]) + 1
        if gone > last:
            return []
        if gone == last:
            mid = lo + 8 * pl.cdiv(hi - lo, 16)
            lo, hi = (lo, mid) if way > 0 else (mid, hi)
        return [] if lo == hi else [post(axis, way, off, lo, hi, order, now)]

    starts = [[] for _ in parts]
    for leg in range(2):
        for begin, (lo, hi, order, now) in zip(starts, parts):
            for way in WAYS:
                begin += ring(order[leg], way, (0, 0), lo, hi, order, now)
    while heap:
        now, i, off, lo, hi, order = heapq.heappop(heap)
        axis, way = sends[i][:2]
        if off[1] and now < hold:
            heapq.heappush(heap, (hold, i, off, lo, hi, order))
            continue
        new = ring(axis, way, off, lo, hi, order, now)
        if axis == order[0]:
            for w in WAYS:
                new += ring(order[1], w, off, lo, hi, order, now)
        events.append((i, new, now))
    return sends, starts, events


def two_colours(lo, hi, share, now=0):
    split = lo + 8 * round((hi - lo) * share / 8)
    return [(lo, split, (0, 1), now), (split, hi, (1, 0), now)]


class Spread:
    def __init__(self, at, plan, rows, block, send, recv):
        self.sends, self.starts, self.events = plan
        self.block, self.send, self.recv, self.rows = block, send, recv, rows
        self.count = len(self.sends)
        self.other = to_tp(at.partner)
        self.device = {}
        for way in WAYS:
            self.device[0, way] = to_tp(at.tp_of(way))
            self.device[1, way] = to_dp(at.dp_of_y(way))

    def goal(self, i):
        axis, way, off = self.sends[i][:3]
        return tuple(o - way * (a == axis) for a, o in enumerate(off))

    def copy(self, i):
        axis, way, off, lo, hi = self.sends[i]
        src, dst = self.block(*off, False, lo, hi), self.block(off[0], self.goal(i)[1], False, lo, hi)
        return rdma(src, dst, self.send.at[i], self.recv.at[i], self.device[axis, way])

    def forward(self, i, cross=False):
        off, (lo, hi) = ((0, 0), (0, self.rows)) if i == self.count else (self.goal(i), self.sends[i][-2:])
        ref = self.block(*off, cross, lo, hi)
        return rdma(ref, ref, self.send.at[self.count + i], self.recv.at[self.count + i], self.other)

    def begin(self):
        for i in sum(self.starts, []):
            self.copy(i).start()
        self.forward(self.count).start()

    def run(self, events):
        for i, new, _ in events:
            ref = self.block(*self.goal(i), False, *self.sends[i][-2:])
            rdma(ref, ref, self.send.at[i], self.recv.at[i], self.other).wait_recv()
            for j in new:
                self.copy(j).start()
            self.forward(i).start()

    def take(self, i):
        self.forward(i, True).wait_recv()

    def end(self):
        for i in range(self.count):
            self.copy(i).wait_send()
        for i in range(self.count + 1):
            self.forward(i).wait_send()


def token_kernel(
    nz, tok_total, plan, table, part, trunk, marks, lab_row, ids,
    du, ub_all, u_out, r_out, stats, tiles,
    table_v, ub_v, z_v, run, mine, theirs, row_out, row_in, tile_out, tile_in, pb, rl, fin, land,
    load_sem, part_sem, st_send, st_recv, row_send, row_recv, t_send, t_recv, rs_send, rs_recv, x_send, x_recv,
):
    at = Place(nz)
    rows, width = table_v.shape
    toks = ub_v.shape[0]
    own = trunk.shape[0]
    steps = z_v.shape[0]
    whole = rows // VT
    tail = rows - whole * VT

    part_copy = pltpu.make_async_copy(part, ub_v, part_sem)
    part_copy.start()

    def load(i):
        start = pl.multiple_of(i * VT, 16)
        return pltpu.make_async_copy(table.at[pl.ds(start, VT)], table_v.at[pl.ds(start, VT)], load_sem.at[i])

    tail_copy = pltpu.make_async_copy(
        table.at[pl.ds(whole * VT, tail)], table_v.at[pl.ds(whole * VT, tail)], load_sem.at[whole]
    )
    greet([to_tp(rem(at.tp + i, NTP)) for i in range(1, NTP)] + [to_dp(at.dp_of_y(i)) for i in range(1, NY)])
    part_copy.wait()
    for i in range(whole):
        load(i).start()
    tail_copy.start()
    mine_only = (marks[:, 1:2] >= 0) & (marks[:, 1:2] < rows)
    du[ALL] = jnp.where(mine_only, ub_v[ALL].astype(F32), 0.0)
    sums = SumTp(at, du, own, pb, rl, fin, rs_send, rs_recv)
    sums.begin()
    sums.pass_on()
    sums.join()
    hidden = sums.result() + trunk[ALL].astype(F32)
    centered = hidden - jnp.mean(hidden, axis=-1, keepdims=True)
    inv_std = lax.rsqrt(jnp.mean(centered * centered, axis=-1, keepdims=True) + LN_EPS)
    normed = centered * inv_std
    land[at.tp] = normed.astype(BF16).astype(F32)

    def block(dx, dy, cross, lo, hi):
        tp, cut = at.tp_of(dx, cross), pl.ds(lo, hi - lo)
        return ub_all.at[dy % NY, tp, cut] if dy % NY else land.at[tp, cut]

    spread = Spread(at, plan, own, block, x_send, x_recv)
    spread.begin()
    u_out[ALL] = normed
    r_out[ALL] = jnp.broadcast_to(inv_std, r_out.shape)
    near = [e for e in spread.events if spread.goal(e[0])[1] == 0]
    spread.run(near)
    for e in near:
        spread.take(e[0])
    spread.take(spread.count)
    groups = {}
    pace = own / 7.5
    for e in [e for e in spread.events if e not in near]:
        due = max(0, int((e[-1] - near[-1][-1]) / pace)) + 2
        groups.setdefault(due if due <= steps else max(steps, due - 5), []).append(e)
    late = [e for due in sorted(groups) if due >= 2 * steps for e in groups[due]]

    def attend(step):
        for due, events in groups.items():
            if due < 2 * steps:

                @pl.when(step == due)
                def _(events=events):
                    spread.run(events)

    keep = pltpu.make_async_copy(land, ub_all.at[0], part_sem)
    keep.start()
    ub_v[ALL] = land[ALL].reshape(toks, width).astype(BF16)
    run[0] = jnp.full(run.shape[1:], NEG, F32)
    run[1] = jnp.zeros(run.shape[1:], F32)
    lane = lax.broadcasted_iota(jnp.int32, (toks, VT), 1)

    def start_of(i):
        return pl.multiple_of(jnp.minimum(i * VT, rows - VT), 16)

    def fold(op, v):
        return functools.reduce(op, [v[:, j : j + 128] for j in range(0, VT, 128)])

    def forward(i, carry):
        attend(i)

        @pl.when(i < whole)
        def _():
            load(i).wait()

        @pl.when(i == whole)
        def _():
            tail_copy.wait()

        start = start_of(i)
        z = lax.dot_general(ub_v[ALL], table_v[pl.ds(start, VT), :], NT_DIMS, preferred_element_type=F32)
        z = jnp.where(lane >= i * VT - start, z, NEG)
        z_v[i] = z
        run[0] = jnp.maximum(run[0], fold(jnp.maximum, z))
        hit = (lane + start == marks[:, 0:1]) & (lane >= i * VT - start)
        run[1] = run[1] + fold(jnp.add, jnp.where(hit, z, 0.0))
        return carry

    lax.fori_loop(0, steps, forward, 0)
    top = jnp.max(run[0], axis=1, keepdims=True)
    run[0] = jnp.zeros(run.shape[1:], F32)

    def exps(i, carry):
        run[0] = run[0] + fold(jnp.add, jnp.exp(z_v[i] - top))
        return carry

    lax.fori_loop(0, steps, exps, 0)
    total = jnp.sum(run[0], axis=1, keepdims=True)
    label = jnp.sum(run[1], axis=1, keepdims=True)
    narrow = lax.broadcasted_iota(jnp.int32, (toks, 128), 1)
    packed = jnp.where(narrow == 0, top, jnp.where(narrow == 1, total, jnp.where(narrow == 2, label, 0.0)))
    mine[ALL] = jnp.transpose(packed)[:8]
    stat = []
    for i in range(1, NTP):
        stat.append(rdma(mine, theirs.at[i], st_send.at[i], st_recv.at[i], to_tp(rem(at.tp + i, NTP))))
        stat[-1].start()
    theirs[0] = mine[ALL]
    for copy in stat:
        copy.wait_recv()
    parts = [theirs[rem(at.tp - j + NTP, NTP)] for j in range(NTP)]
    peak = functools.reduce(jnp.maximum, [p[0:1] for p in parts])
    total = functools.reduce(jnp.add, [p[1:2] * jnp.exp(p[0:1] - peak) for p in parts])
    label = functools.reduce(jnp.add, [p[2:3] for p in parts])
    lse = peak + jnp.log(total)
    loss = jnp.sum(jnp.log(total) + peak - label, axis=1, keepdims=True)
    sub = lax.broadcasted_iota(jnp.int32, (8, toks), 0)
    row_out[ALL] = jnp.where(sub == 0, lse, jnp.where(sub == 1, lab_row[ALL], 0.0))
    upper = lax.broadcasted_iota(jnp.int32, ids.shape, 1) >= 64
    tile_out[ALL] = jnp.where(upper == (rem(at.z, 2) == 1), ids[ALL], loss)
    tiles[0] = tile_out[ALL]
    rows_sent = []
    for i in range(NY - 1):
        to_y = to_dp(at.dp_of_y(NY - 1 - i))
        rows_sent.append(rdma(row_out, row_in.at[i], row_send.at[i], row_recv.at[i], to_y))
        rows_sent.append(rdma(tile_out, tile_in.at[i], t_send.at[i], t_recv.at[i], to_y))
    for copy in rows_sent:
        copy.start()
    run[0] = jnp.transpose(jnp.broadcast_to(lse, (128, toks)))
    wide = min(512, width)
    inv_total = 1.0 / tok_total
    du[ALL] = jnp.zeros(du.shape, F32)

    def backward(i, carry):
        attend(i + steps)
        start = start_of(i)
        shift = jnp.concatenate([run[0]] * (VT // 128), axis=1)
        prob = jnp.exp(z_v[i] - shift)
        hit = (lane + start == marks[:, 0:1]) & (lane >= i * VT - start)
        grad = ((prob - jnp.where(hit, 1.0, 0.0)) * inv_total).astype(BF16)
        for n in range(width // wide):
            cols = pl.ds(n * wide, wide)
            du[:, cols] = du[:, cols] + lax.dot_general(
                grad, table_v[pl.ds(start, VT), cols], NN_DIMS, preferred_element_type=F32
            )
        return carry

    lax.fori_loop(0, steps, backward, 0)
    spread.run(late)
    for e in spread.events:
        if e not in near:
            spread.take(e[0])
    for copy in rows_sent:
        copy.wait_recv()
    stats[0] = row_out[ALL]
    for i in range(NY - 1):
        stats[i + 1] = row_in[i]
        tiles[i + 1] = tile_in[i]
    keep.wait()
    spread.end()
    for copy in stat + rows_sent:
        copy.wait_send()


class SumZ:
    def __init__(self, at, parts, came, total, chunks, send, recv):
        self.at, self.parts, self.came, self.total = at, parts, came, total
        self.chunks, self.send, self.recv = chunks, send, recv
        self.last = at.nz // 2

    def rows(self, c, s, way):
        lo, hi = self.chunks[c]
        if s == 1:
            mid = lo + 8 * pl.cdiv(hi - lo, 16)
            lo, hi = (lo, mid) if way > 0 else (mid, hi)
        return pl.ds(lo, hi - lo)

    def slot(self, s, way):
        return 0 if s == 1 else 2 * (s - 1) - (way > 0)

    def goal(self, s, way):
        return rem(self.at.z + way * (self.last + 1 - s) + self.at.nz, self.at.nz)

    def copy(self, c, s, way):
        rows, w = self.rows(c, s, way), WAYS.index(way)
        sems = self.send.at[w, s, c], self.recv.at[w, s, c]
        src = self.parts.at[self.goal(s, way), rows]
        return rdma(src, self.came.at[self.slot(s, way), rows], *sems, to_dp(self.at.dp_of_z(way)))

    def begin(self, c):
        rows = pl.ds(self.chunks[c][0], self.chunks[c][1] - self.chunks[c][0])
        self.total[rows] = self.parts[self.at.z, rows]
        for way in WAYS:
            self.copy(c, 1, way).start()

    def run(self, c, s):
        for way in WAYS:
            self.copy(c, s, way).wait_recv()
            rows, slot = self.rows(c, s, way), self.slot(s, way)
            if s < self.last:
                goal = self.goal(s + 1, way)
                self.parts[goal, rows] = self.parts[goal, rows] + self.came[slot, rows]
                self.copy(c, s + 1, way).start()
            else:
                self.total[rows] = self.total[rows] + self.came[slot, rows]

    def end(self):
        for c in range(len(self.chunks)):
            for s in range(self.last):
                for way in WAYS:
                    self.copy(c, s + 1, way).wait_send()


def finish_kernel(
    nz, stride, vocab_loc, tok_total, row_plan, dh_plan, table_plan, chunks,
    table, ub, stats, du, u, r, tiles,
    d_trunk, loss, stack, all_dh,
    pb, rl, fin, land, all_tiles, table_v, ub_v, stage, grad_v, parts, came, total, dh_v,
    rs_send, rs_recv, row_send, row_recv, z_send, z_recv, i_send, i_recv, x_send, x_recv, s_send, s_recv, t_send, t_recv,
    load_sem, stage_sem, dh_sem,
):
    at = Place(nz)
    own, width = u.shape
    win, cols = total.shape
    toks = stats.shape[2]
    block = nz * own
    slab = stage.shape[1]
    first = pl.multiple_of(at.y * stride, 16)
    load = pltpu.make_async_copy(table.at[pl.ds(first, win)], table_v, load_sem)

    depth, per = stage.shape[0], toks // slab
    slabs = NY * per

    def fill(i):
        rows = pl.ds(pl.multiple_of(rem(i, per) * slab, slab), slab)
        at_slot = rem(i, depth)
        return pltpu.make_async_copy(ub.at[lax.div(i, jnp.int32(per)), rows], stage.at[at_slot], stage_sem.at[at_slot])

    for i in range(depth):
        fill(jnp.int32(i)).start()
    load.start()
    greet(
        [to_tp(rem(at.tp + i, NTP)) for i in range(1, NTP)]
        + [to_dp(at.dp_of_z(i)) for i in range(1, nz)]
        + [to_dp(at.dp_of_y(way)) for way in WAYS]
    )
    sum_tp = SumTp(at, du, own, pb, rl, fin, rs_send, rs_recv)
    sum_tp.begin()

    def narrow(n):
        def body(k, carry):
            i = n * per + k
            fill(i).wait()
            ub_v[pl.ds(pl.multiple_of(i * slab, slab), slab)] = stage[rem(i, depth)].astype(BF16)

            @pl.when(i + depth < slabs)
            def _():
                fill(i + depth).start()

            return carry

        lax.fori_loop(0, per, body, 0)

    narrow(0)
    sum_tp.pass_on()
    load.wait()

    inv_total = 1.0 / tok_total

    def logits(lo, hi, ahead=lambda n: None):
        vocab = at.tp * vocab_loc + first + lo + lax.broadcasted_iota(jnp.int32, (hi - lo, toks), 0)

        def body(n, carry):
            ahead(n)
            cut = pl.ds(pl.multiple_of(n * toks, 128), toks)
            z = lax.dot_general(table_v[lo:hi, :], ub_v[cut, :], NT_DIMS, preferred_element_type=F32)
            row = stats[n]
            prob = jnp.exp(z - row[0:1])
            hit = vocab == row[1:2].astype(jnp.int32)
            grad_v[0 : hi - lo, cut] = ((prob - jnp.where(hit, 1.0, 0.0)) * inv_total).astype(BF16)
            return carry

        lax.fori_loop(0, NY, body, 0)

    def head(lo, hi):
        def body(n, carry):
            cut = pl.ds(pl.multiple_of(n * cols, 128), cols)
            parts[n, lo:hi] = jnp.dot(grad_v[0 : hi - lo, :], ub_v[:, cut], preferred_element_type=F32)
            return carry

        lax.fori_loop(0, nz, body, 0)

    sums = SumZ(at, parts, came, total, chunks, s_send, s_recv)
    todo = [(c, s) for _, c, s in sorted((k * s + late, c, s) for s in range(1, sums.last + 1) for c, (k, late) in enumerate(PACE))]

    def narrow_next(n):
        @pl.when(n + 1 < NY)
        def _():
            narrow(n + 1)

    logits(*chunks[0], narrow_next)
    head(*chunks[0])
    sums.begin(0)
    sum_tp.join()
    logits(*chunks[1])
    sums.run(*todo[0])
    grad = sum_tp.result()
    normed = u[ALL]
    mean_g = jnp.mean(grad, axis=-1, keepdims=True)
    mean_gu = jnp.mean(grad * normed, axis=-1, keepdims=True)
    land[at.tp] = r[:, 0:1] * (grad - mean_g - normed * mean_gu)

    def row_block(dx, dy, cross, lo, hi):
        return land.at[at.tp_of(dx, cross), pl.ds(lo, hi - lo)]

    whole_rows = Spread(at, row_plan, own, row_block, row_send, row_recv)
    whole_rows.begin()
    here = pl.ds(pl.multiple_of(at.z * own, own), own)
    turned = []
    for i in range(1, nz):
        col, to_z = pl.multiple_of(rem(at.z + i, nz) * cols, 128), to_dp(at.dp_of_z(i))
        src = land.at[at.tp, :, pl.ds(col, cols)]
        turned.append(rdma(src, all_dh.at[at.tp, 0, here], z_send.at[i], z_recv.at[i], to_z))
        turned.append(rdma(tiles, all_tiles.at[at.z], i_send.at[i], i_recv.at[i], to_z))
    for copy in turned:
        copy.start()
    my_col = pl.multiple_of(at.z * cols, 128)
    mine = pltpu.make_async_copy(land.at[at.tp, :, pl.ds(my_col, cols)], all_dh.at[at.tp, 0, here], load_sem)
    mine.start()
    all_tiles[at.z] = tiles[ALL]
    head(*chunks[1])
    sums.begin(1)
    sums.run(*todo[1])
    logits(*chunks[2])
    whole_rows.run(whole_rows.events)
    mine.wait()
    for copy in turned:
        copy.wait_recv()

    def dh_block(dx, dy, cross, lo, hi):
        return all_dh.at[at.tp_of(dx, cross), dy % NY, pl.ds(lo, hi - lo)]

    blocks = Spread(at, dh_plan, block, dh_block, x_send, x_recv)
    blocks.begin()
    head(*chunks[2])
    sums.begin(2)

    pieces = {(0, 0): [(blocks.count, [], 0)]}
    for e in blocks.events:
        dx, dy = blocks.goal(e[0])
        pieces.setdefault((dx % NX, dy % NY), []).append(e)
    order = sorted((pieces[p][-1][-1] + cross * (block // 3), *p, cross) for p in pieces for cross in range(2))
    left = list(blocks.events)
    due = []
    for time, dx, dy, cross in order:
        due.append([e for e in left if e[-1] <= time])
        left = [e for e in left if e[-1] > time]
    code = [dx + NX * (dy + NY * cross) for _, dx, dy, cross in order]
    ready = 2

    def meet(k):
        blocks.run(due[k])
        _, dx, dy, cross = order[k]
        if cross:
            for part in pieces[dx, dy]:
                blocks.take(part[0])

    for k in range(ready):
        meet(k)
    for i in range(whole_rows.count + 1):
        whole_rows.take(i)
    d_trunk[ALL] = land[ALL].reshape(d_trunk.shape).astype(BF16)
    upper = lax.broadcasted_iota(jnp.int32, loss.shape, 1) >= 64
    loss[ALL] = sum(
        jnp.where(upper == (z % 2 == 0), all_tiles[z, rem(y - at.y + NY, NY)], 0.0) for z in range(nz) for y in range(NY)
    )

    beside = {at_piece: todo[2 + k] for k, at_piece in enumerate((0, 1, 4, 7, 15, 24)) if 2 + k < len(todo)}
    low = (at.tp * vocab_loc + at.y * stride).astype(F32)

    def place_of(e):
        mark = jnp.int32(code[0])
        for k in range(1, len(order)):
            mark = jnp.where(e == k, code[k], mark)
        core = jnp.where(mark >= NX * NY, 1 - at.c, at.c)
        return 2 * rem(at.x + rem(mark, NX), NX) + core, rem(lax.div(mark, jnp.int32(NX)), NY)

    def fetch(e):
        tp, far = place_of(e)
        half = rem(e, 2)
        return pltpu.make_async_copy(all_dh.at[tp, far], dh_v.at[half], dh_sem.at[half])

    def piece(e, carry):
        for k in range(len(order)):
            met = k + 1 if k + 1 < len(order) and k + 1 >= ready else 0
            if k in beside or met:

                @pl.when(e == k)
                def _(k=k, met=met):
                    if k in beside:
                        sums.run(*beside[k])
                    if met:
                        meet(met)

        @pl.when(e + 1 < len(order))
        def _():
            fetch(e + 1).start()

        tp, far = place_of(e)
        ids = jnp.concatenate(
            [
                jnp.where(upper[0:1], all_tiles[2 * j + 1, far, pl.ds(tp, 1), :], all_tiles[2 * j, far, pl.ds(tp, 1), :])
                for j in range(nz // 2)
            ],
            axis=1,
        )
        fetch(e).wait()
        dh = dh_v[rem(e, 2)]
        hi = dh.astype(BF16)
        rest = dh - hi.astype(F32)
        mid = rest.astype(BF16)
        lo = (rest - mid.astype(F32)).astype(BF16)
        ids = (ids - low).astype(jnp.int32)
        for begin, end in chunks:
            row = lax.broadcasted_iota(jnp.int32, (end - begin, block), 0) + begin
            pick = jnp.where(row == ids, 1.0, 0.0).astype(BF16)
            found = sum(jnp.dot(pick, term, preferred_element_type=F32) for term in (hi, mid, lo))
            total[begin:end] = total[begin:end] + found
        return carry

    fetch(jnp.int32(0)).start()
    lax.fori_loop(0, len(order), piece, 0)
    for copy in turned:
        copy.wait_send()

    sends, starts, events = table_plan
    device = {(0, way): to_dp(at.dp_of_z(way)) for way in WAYS} | {(1, way): to_dp(at.dp_of_y(way)) for way in WAYS}

    def copy_of(i, arrives=False):
        axis, way, off, lo, hi = sends[i]
        if arrives:
            off = tuple(o - way * (a == axis) for a, o in enumerate(off))
        dst = stack.at[rem(at.z + off[0] + nz, nz), at.y_of(off[1]), pl.ds(lo, hi - lo)]
        src = dst if any(off) else total.at[pl.ds(lo, hi - lo)]
        return rdma(src, dst, t_send.at[i], t_recv.at[i], device[axis, way])

    for step in todo[2 + len(beside) :]:
        sums.run(*step)
    for i in sum(starts, []):
        copy_of(i).start()
    keep = pltpu.make_async_copy(total, stack.at[at.z, at.y], load_sem)
    keep.start()
    for i, new, _ in events:
        copy_of(i, True).wait_recv()
        for j in new:
            copy_of(j).start()
    keep.wait()
    for i in range(len(sends)):
        copy_of(i).wait_send()
    sums.end()
    whole_rows.end()
    blocks.end()


def place_kernel(chunk, tok_total, stack, rows_in, loss_in, out, rows_out, loss_out, slots, rows_v, load_sem, store_sem, rows_sem):
    nz, ny, have, cols = stack.shape
    depth = slots.shape[0]
    per = have // chunk
    total = ny * per
    ahead = depth // 2

    def load(i):
        y, row = lax.div(i, jnp.int32(per)), pl.multiple_of(rem(i, per) * chunk, 8)
        s = rem(i, depth)
        return pltpu.make_async_copy(stack.at[:, y, pl.ds(row, chunk)], slots.at[s], load_sem.at[s])

    def stores(i):
        s, row = rem(i, depth), pl.multiple_of(i * chunk, 8)
        return [
            pltpu.make_async_copy(slots.at[s, j], out.at[pl.ds(row, chunk), pl.ds(j * cols, cols)], store_sem.at[s, j])
            for j in range(nz)
        ]

    def prime(i, carry):
        load(i).start()
        return carry

    def body(i, carry):
        load(i).wait()
        for copy in stores(i):
            copy.start()

        @pl.when(i + ahead < total)
        def _():
            @pl.when(i >= ahead)
            def _():
                for copy in stores(i - ahead):
                    copy.wait()

            load(i + ahead).start()

        return carry

    def drain(i, carry):
        for copy in stores(i):
            copy.wait()
        return carry

    rows_load = pltpu.make_async_copy(rows_in, rows_v, rows_sem)
    rows_store = pltpu.make_async_copy(rows_v, rows_out, rows_sem)
    lax.fori_loop(0, ahead, prime, 0)
    rows_load.start()
    lane = lax.broadcasted_iota(jnp.int32, (1, 128), 1)
    loss_out[0, 0] = jnp.sum(jnp.where(rem(lane, 64) == 0, loss_in[0:1], 0.0)) / tok_total
    rows_load.wait()
    rows_store.start()
    lax.fori_loop(0, total, body, 0)
    lax.fori_loop(total - 2 * ahead, total, drain, 0)
    used = per * chunk
    left = have - used
    rest = pltpu.make_async_copy(stack.at[:, ny - 1, pl.ds(used, left)], slots.at[0, :, pl.ds(0, left)], load_sem.at[0])
    rest.start()
    rest.wait()
    tails = [
        pltpu.make_async_copy(
            slots.at[0, j, pl.ds(0, left)], out.at[pl.ds(ny * used, left), pl.ds(j * cols, cols)], store_sem.at[0, j]
        )
        for j in range(nz)
    ]
    for copy in tails:
        copy.start()
    for copy in tails:
        copy.wait()
    rows_store.wait()


def vmem():
    return pl.BlockSpec(memory_space=pltpu.VMEM)


def anywhere():
    return pl.BlockSpec(memory_space=pl.ANY)


def dma(*shape):
    return pltpu.SemaphoreType.DMA(shape)


def solution(mesh):
    ndp, ntp = mesh.shape["dp"], mesh.shape["tp"]
    nz = ndp // NY

    def per_device(table, ids, labels, trunk):
        vocab_loc, width = table.shape
        batch, seq = ids.shape
        toks = batch * seq
        own = toks // NTP
        tok_total = toks * ndp
        stride = (vocab_loc - 16) // NY
        win = stride + 16
        cols = width // nz
        block = nz * own
        big = 66_000_000
        dp, tp = lax.axis_index("dp"), lax.axis_index("tp")
        row_start = tp * vocab_loc
        local_ids = ids.reshape(toks) - row_start
        part = jnp.take(table, local_ids, axis=0, mode="clip")
        trunk_own = lax.dynamic_slice_in_dim(trunk.reshape(toks, width), tp * own, own, 0)

        tp_scratch = [
            pltpu.VMEM((4, own, width), F32),
            pltpu.VMEM((2, own // 2, width), F32),
            pltpu.VMEM((4, own // 2, width), F32),
            pltpu.VMEM((NTP, own, width), F32),
        ]
        ids_f = ids.reshape(NTP, own).astype(F32)
        blank = jnp.zeros_like(ids_f)
        even = rem(lax.div(dp, jnp.int32(NY)), 2) == 0
        pad = ((0, 0), (0, 128 - 2 * own))
        ids_tile = jnp.pad(jnp.concatenate([jnp.where(even, ids_f, blank), jnp.where(even, blank, ids_f)], axis=1), pad)
        marks = jnp.stack([labels.reshape(toks) - row_start, local_ids], axis=1)
        lab_row = labels.reshape(1, toks).astype(F32)
        steps = pl.cdiv(vocab_loc, VT)
        token_plan = gather_plan((NX, NY), two_colours(0, own, 0.5), 16, hold=2 * own)
        sends = 2 * len(token_plan[0]) + 1
        du, ub, u_own, r_own, stats, tiles = pl.pallas_call(
            functools.partial(token_kernel, nz, tok_total, token_plan),
            out_shape=(
                jax.ShapeDtypeStruct((toks, width), F32),
                jax.ShapeDtypeStruct((NY, NTP, own, width), F32),
                jax.ShapeDtypeStruct((own, width), F32),
                jax.ShapeDtypeStruct((own, 128), F32),
                jax.ShapeDtypeStruct((NY, 8, toks), F32),
                jax.ShapeDtypeStruct((NY, 8, 128), F32),
            ),
            in_specs=[anywhere(), anywhere(), vmem(), vmem(), vmem(), vmem()],
            out_specs=(vmem(), anywhere(), vmem(), vmem(), vmem(), vmem()),
            scratch_shapes=[
                pltpu.VMEM((vocab_loc, width), BF16),
                pltpu.VMEM((toks, width), BF16),
                pltpu.VMEM((steps, toks, VT), F32),
                pltpu.VMEM((2, toks, 128), F32),
                pltpu.VMEM((8, toks), F32),
                pltpu.VMEM((NTP, 8, toks), F32),
                pltpu.VMEM((8, toks), F32),
                pltpu.VMEM((NY - 1, 8, toks), F32),
                pltpu.VMEM((8, 128), F32),
                pltpu.VMEM((NY - 1, 8, 128), F32),
                *tp_scratch,
                dma(steps), pltpu.SemaphoreType.DMA, dma(NTP), dma(NTP),
                dma(NY - 1), dma(NY - 1), dma(NY - 1), dma(NY - 1), dma(10), dma(10), dma(sends), dma(sends),
            ],
            compiler_params=pltpu.CompilerParams(collective_id=0, has_side_effects=True, vmem_limit_bytes=big),
            name="token",
        )(table, part, trunk_own, marks, lab_row, ids_tile)

        row_plan = gather_plan((NX, 1), two_colours(0, own, 1), 16)
        dh_plan = gather_plan((NX, NY), two_colours(0, block, 0.5), block // 4)
        lead = 16 * (win // 96)
        middle = lead + 16 * pl.cdiv(win - lead, 32)
        chunks = ((0, lead), (lead, middle), (middle, win))
        third = 8 * pl.cdiv(win, 24)
        table_chunks = ((0, third), (third, 2 * third), (2 * third, win))
        shares = SHARES if nz == 8 else (0.5,) * 3
        table_parts = sum((two_colours(lo, hi, share) for (lo, hi), share in zip(table_chunks, shares)), [])
        table_plan = gather_plan((nz, NY), table_parts, 60)
        counts = [2 * len(p[0]) + 1 for p in (row_plan, dh_plan, table_plan)]
        zs = (2, nz // 2 + 1, len(chunks))
        d_rows, loss, stack, _ = pl.pallas_call(
            functools.partial(
                finish_kernel, nz, stride, vocab_loc, tok_total, row_plan, dh_plan, table_plan, chunks
            ),
            out_shape=(
                jax.ShapeDtypeStruct((toks, width), BF16),
                jax.ShapeDtypeStruct((8, 128), F32),
                jax.ShapeDtypeStruct((nz, NY, win, cols), F32),
                jax.ShapeDtypeStruct((NTP, NY, block, cols), F32),
            ),
            in_specs=[anywhere(), anywhere(), vmem(), vmem(), vmem(), vmem(), vmem()],
            out_specs=(vmem(), vmem(), anywhere(), anywhere()),
            scratch_shapes=[
                *tp_scratch,
                pltpu.VMEM((nz, NY, 8, 128), F32),
                pltpu.VMEM((win, width), BF16),
                pltpu.VMEM((NY * toks, width), BF16),
                pltpu.VMEM((4, 128, width), F32),
                pltpu.VMEM((middle - lead, NY * toks), BF16),
                pltpu.VMEM((nz, win, cols), F32),
                pltpu.VMEM((nz - 1, win, cols), F32),
                pltpu.VMEM((win, cols), F32),
                pltpu.VMEM((2, block, cols), F32),
                dma(10), dma(10), dma(counts[0]), dma(counts[0]), dma(nz), dma(nz), dma(nz), dma(nz),
                dma(counts[1]), dma(counts[1]), dma(*zs), dma(*zs), dma(counts[2]), dma(counts[2]),
                pltpu.SemaphoreType.DMA, dma(4), dma(2),
            ],
            compiler_params=pltpu.CompilerParams(collective_id=1, has_side_effects=True, vmem_limit_bytes=67_000_000),
            name="finish",
        )(table, ub.reshape(NY, toks, width), stats, du, u_own, r_own, tiles)
        depth = 8
        chunk = next(n for n in range(224, 0, -8) if stride % n == 0 and NY * stride >= n * depth)
        d_table, d_rows, mean_loss = pl.pallas_call(
            functools.partial(place_kernel, chunk, tok_total),
            out_shape=(
                jax.ShapeDtypeStruct((vocab_loc, width), F32),
                jax.ShapeDtypeStruct((toks, width), BF16),
                jax.ShapeDtypeStruct((1, 1), F32),
            ),
            in_specs=[anywhere(), anywhere(), vmem()],
            out_specs=(anywhere(), anywhere(), pl.BlockSpec(memory_space=pltpu.SMEM)),
            scratch_shapes=[
                pltpu.VMEM((depth, nz, chunk, cols), F32), pltpu.VMEM((toks, width), BF16),
                dma(depth), dma(depth, nz), pltpu.SemaphoreType.DMA,
            ],
            compiler_params=pltpu.CompilerParams(vmem_limit_bytes=big),
            name="place",
        )(stack, d_rows, loss)
        return mean_loss.reshape(()), d_rows.reshape(trunk.shape), d_table

    return jax.shard_map(
        per_device,
        mesh=mesh,
        in_specs=(P("tp", None), P("dp", None), P("dp", None), P("dp", None, None)),
        out_specs=(P(), P("dp", None, None), P("tp", None)),
        check_vma=False,
    )
```

```python
import functools
import heapq

import jax
import jax.numpy as jnp
from jax import lax
from jax.experimental import pallas as pl
from jax.experimental.pallas import tpu as pltpu
from jax.sharding import PartitionSpec as P

LN_EPS = 1e-5
MESH = pl.DeviceIdType.MESH
F32, BF16 = jnp.float32, jnp.bfloat16
NY, NTP, NX = 4, 8, 4
WAYS = (1, -1)
BESIDE = ((0, 2, 1), (6, 1, 2), (13, 2, 2), (20, 1, 3), (26, 2, 3))
SHARES = (0.55, 0.55, 0.7)
ALL = Ellipsis
NEG = float(jnp.finfo(jnp.float32).min)
VT = 512
NT_DIMS = (((1,), (1,)), ((), ()))
NN_DIMS = (((1,), (0,)), ((), ()))


def rem(a, b):
    return lax.rem(a, jnp.int32(b))


class Place:
    def __init__(self, nz):
        self.nz = nz
        self.dp = lax.axis_index("dp")
        self.tp = lax.axis_index("tp")
        self.z, self.y = lax.div(self.dp, jnp.int32(NY)), rem(self.dp, NY)
        self.x, self.c = lax.div(self.tp, jnp.int32(2)), rem(self.tp, 2)
        self.partner = 2 * self.x + (1 - self.c)

    def tp_of(self, step, other=False):
        c = 1 - self.c if other else self.c
        return 2 * rem(self.x + step + NX, NX) + c

    def y_of(self, step):
        return rem(self.y + step + NY, NY)

    def dp_of_y(self, step):
        return self.z * NY + self.y_of(step)

    def dp_of_z(self, step):
        return rem(self.z + step + self.nz, self.nz) * NY + self.y


def to_tp(tp):
    return {"tp": tp}


def to_dp(dp):
    return {"dp": dp}


def rdma(src, dst, send_sem, recv_sem, device):
    return pltpu.make_async_remote_copy(
        src_ref=src, dst_ref=dst, send_sem=send_sem, recv_sem=recv_sem, device_id=device, device_id_type=MESH
    )


def greet(devices):
    barrier = pltpu.get_barrier_semaphore()
    for device in devices:
        pl.semaphore_signal(barrier, inc=1, device_id=device, device_id_type=MESH)
    pl.semaphore_wait(barrier, len(devices))


class SumTp:
    def __init__(self, at, src, own, pb, rl, fin, send, recv):
        self.src, self.own, self.half, self.pb, self.rl, self.fin = src, own, own // 2, pb, rl, fin
        self.at, self.send, self.recv = at, send, recv
        self.steps = (2, 1, -1, 0)
        self.copies = []

    def copy(self, i, src, dst, tp):
        self.copies.append(rdma(src, dst, self.send.at[i], self.recv.at[i], to_tp(tp)))
        return self.copies[-1]

    def rows(self, step, other):
        return pl.ds(pl.multiple_of(self.at.tp_of(step, other) * self.own, self.own), self.own)

    def part(self, i, h):
        return self.pb.at[i, pl.ds(h * self.half, self.half)]

    def begin(self):
        for i, step in enumerate(self.steps):
            self.copy(i, self.src.at[self.rows(step, True)], self.pb.at[i], self.at.partner).start()

    def merge(self, i):
        self.copies[i].wait_recv()
        self.pb[i] = self.pb[i] + self.src[self.rows(self.steps[i], False), :]

    def pass_on(self):
        plus, minus = self.at.tp_of(1), self.at.tp_of(-1)
        self.merge(0)
        for h, tp in enumerate((plus, minus)):
            self.copy(4 + h, self.part(0, h), self.rl.at[h], tp).start()
        self.merge(1)
        self.merge(2)
        self.copy(6, self.part(1, 1), self.fin.at[0], plus).start()
        self.copy(7, self.part(2, 0), self.fin.at[1], minus).start()

    def join(self):
        for h, tp in enumerate((self.at.tp_of(1), self.at.tp_of(-1))):
            self.copies[4 + h].wait_recv()
            rows = pl.ds(h * self.half, self.half)
            self.pb[1 + h, rows] = self.pb[1 + h, rows] + self.rl[h]
            self.copy(8 + h, self.part(1 + h, h), self.fin.at[2 + h], tp).start()
        self.merge(3)

    def result(self):
        for copy in self.copies[6:]:
            copy.wait_recv()
        top = self.pb[3, 0 : self.half] + self.fin[2] + self.fin[1]
        low = self.pb[3, self.half : self.own] + self.fin[0] + self.fin[3]
        for copy in self.copies:
            copy.wait_send()
        return jnp.concatenate([top, low], axis=0)


def gather_plan(sizes, parts, latency, hold=0):
    sends, events, heap, busy = [], [], [], {}

    def post(axis, way, off, lo, hi, order, now):
        end = max(now, busy.get((axis, way), now)) + hi - lo
        busy[axis, way] = end
        there = tuple(o - way * (a == axis) for a, o in enumerate(off))
        heapq.heappush(heap, (end + latency, len(sends), there, lo, hi, order))
        sends.append((axis, way, off, lo, hi))
        return len(sends) - 1

    def ring(axis, way, off, lo, hi, order, now):
        last = sizes[axis] // 2
        gone = abs(off[axis]) + 1
        if gone > last:
            return []
        if gone == last:
            mid = lo + 8 * pl.cdiv(hi - lo, 16)
            lo, hi = (lo, mid) if way > 0 else (mid, hi)
        return [] if lo == hi else [post(axis, way, off, lo, hi, order, now)]

    starts = [[] for _ in parts]
    for leg in range(2):
        for begin, (lo, hi, order, now) in zip(starts, parts):
            for way in WAYS:
                begin += ring(order[leg], way, (0, 0), lo, hi, order, now)
    while heap:
        now, i, off, lo, hi, order = heapq.heappop(heap)
        axis, way = sends[i][:2]
        if off[1] and now < hold:
            heapq.heappush(heap, (hold, i, off, lo, hi, order))
            continue
        new = ring(axis, way, off, lo, hi, order, now)
        if axis == order[0]:
            for w in WAYS:
                new += ring(order[1], w, off, lo, hi, order, now)
        events.append((i, new, now))
    return sends, starts, events


def two_colours(lo, hi, share, now=0):
    split = lo + 8 * round((hi - lo) * share / 8)
    return [(lo, split, (0, 1), now), (split, hi, (1, 0), now)]


class Spread:
    def __init__(self, at, plan, rows, block, send, recv):
        self.sends, self.starts, self.events = plan
        self.block, self.send, self.recv, self.rows = block, send, recv, rows
        self.count = len(self.sends)
        self.other = to_tp(at.partner)
        self.device = {}
        for way in WAYS:
            self.device[0, way] = to_tp(at.tp_of(way))
            self.device[1, way] = to_dp(at.dp_of_y(way))

    def goal(self, i):
        axis, way, off = self.sends[i][:3]
        return tuple(o - way * (a == axis) for a, o in enumerate(off))

    def copy(self, i):
        axis, way, off, lo, hi = self.sends[i]
        src, dst = self.block(*off, False, lo, hi), self.block(off[0], self.goal(i)[1], False, lo, hi)
        return rdma(src, dst, self.send.at[i], self.recv.at[i], self.device[axis, way])

    def forward(self, i, cross=False):
        off, (lo, hi) = ((0, 0), (0, self.rows)) if i == self.count else (self.goal(i), self.sends[i][-2:])
        ref = self.block(*off, cross, lo, hi)
        return rdma(ref, ref, self.send.at[self.count + i], self.recv.at[self.count + i], self.other)

    def begin(self):
        for i in sum(self.starts, []):
            self.copy(i).start()
        self.forward(self.count).start()

    def run(self, events):
        for i, new, _ in events:
            ref = self.block(*self.goal(i), False, *self.sends[i][-2:])
            rdma(ref, ref, self.send.at[i], self.recv.at[i], self.other).wait_recv()
            for j in new:
                self.copy(j).start()
            self.forward(i).start()

    def take(self, i):
        self.forward(i, True).wait_recv()

    def end(self):
        for i in range(self.count):
            self.copy(i).wait_send()
        for i in range(self.count + 1):
            self.forward(i).wait_send()


def token_kernel(
    nz, tok_total, plan, table, part, trunk, marks, lab_row, ids,
    grads, ub_all, u_out, r_out, stats, tiles,
    du, trunk_v, grad_v, table_v, ub_v, z_v, run, mine, theirs, row_out, row_in, tile_out, tile_in, pb, rl, fin, land,
    load_sem, part_sem, st_send, st_recv, row_send, row_recv, t_send, t_recv, rs_send, rs_recv, x_send, x_recv,
    grad_sem,
):
    at = Place(nz)
    rows, width = table_v.shape
    toks = ub_v.shape[0]
    own = trunk_v.shape[0]
    steps = z_v.shape[0]
    whole = rows // VT
    tail = rows - whole * VT

    part_copy = pltpu.make_async_copy(part, ub_v, part_sem)
    part_copy.start()
    trunk_copy = pltpu.make_async_copy(trunk.at[pl.ds(pl.multiple_of(at.tp * own, own), own)], trunk_v, grad_sem.at[0])
    trunk_copy.start()

    def load(i):
        start = pl.multiple_of(i * VT, 16)
        return pltpu.make_async_copy(table.at[pl.ds(start, VT)], table_v.at[pl.ds(start, VT)], load_sem.at[i])

    tail_copy = pltpu.make_async_copy(
        table.at[pl.ds(whole * VT, tail)], table_v.at[pl.ds(whole * VT, tail)], load_sem.at[whole]
    )
    greet([to_tp(rem(at.tp + i, NTP)) for i in range(1, NTP)] + [to_dp(at.dp_of_y(i)) for i in range(1, NY)])
    part_copy.wait()
    for i in range(whole):
        load(i).start()
    tail_copy.start()
    mine_only = (marks[:, 1:2] >= 0) & (marks[:, 1:2] < rows)
    du[ALL] = jnp.where(mine_only, ub_v[ALL].astype(F32), 0.0)
    sums = SumTp(at, du, own, pb, rl, fin, rs_send, rs_recv)
    sums.begin()
    sums.pass_on()
    sums.join()
    trunk_copy.wait()
    hidden = sums.result() + trunk_v[ALL].astype(F32)
    centered = hidden - jnp.mean(hidden, axis=-1, keepdims=True)
    inv_std = lax.rsqrt(jnp.mean(centered * centered, axis=-1, keepdims=True) + LN_EPS)
    normed = centered * inv_std
    land[at.tp] = normed.astype(BF16).astype(F32)

    def block(dx, dy, cross, lo, hi):
        tp, cut = at.tp_of(dx, cross), pl.ds(lo, hi - lo)
        return ub_all.at[dy % NY, tp, cut] if dy % NY else land.at[tp, cut]

    spread = Spread(at, plan, own, block, x_send, x_recv)
    spread.begin()
    u_out[ALL] = normed
    r_out[ALL] = jnp.broadcast_to(inv_std, r_out.shape)
    near = [e for e in spread.events if spread.goal(e[0])[1] == 0]
    spread.run(near)
    for e in near:
        spread.take(e[0])
    spread.take(spread.count)
    groups = {}
    pace = own / 7.5
    for e in [e for e in spread.events if e not in near]:
        due = max(0, int((e[-1] - near[-1][-1]) / pace)) + 2
        groups.setdefault(due, []).append(e)
    middle, late = ([e for due in sorted(groups) if (due >= steps) and (due < steps + 6) == m for e in groups[due]] for m in (True, False))

    def attend(step):
        for due, events in groups.items():
            if due < steps:

                @pl.when(step == due)
                def _(events=events):
                    spread.run(events)

    keep = pltpu.make_async_copy(land, ub_all.at[0], part_sem)
    keep.start()
    ub_v[ALL] = land[ALL].reshape(toks, width).astype(BF16)
    run[0] = jnp.full(run.shape[1:], NEG, F32)
    run[1] = jnp.zeros(run.shape[1:], F32)
    lane = lax.broadcasted_iota(jnp.int32, (toks, VT), 1)

    def start_of(i):
        return pl.multiple_of(jnp.minimum(i * VT, rows - VT), 16)

    def fold(op, v):
        return functools.reduce(op, [v[:, j : j + 128] for j in range(0, VT, 128)])

    def forward(i, carry):
        attend(i)

        @pl.when(i < whole)
        def _():
            load(i).wait()

        @pl.when(i == whole)
        def _():
            tail_copy.wait()

        start = start_of(i)
        z = lax.dot_general(ub_v[ALL], table_v[pl.ds(start, VT), :], NT_DIMS, preferred_element_type=F32)
        z = jnp.where(lane >= i * VT - start, z, NEG)
        z_v[i] = z
        run[0] = jnp.maximum(run[0], fold(jnp.maximum, z))
        hit = (lane + start == marks[:, 0:1]) & (lane >= i * VT - start)
        run[1] = run[1] + fold(jnp.add, jnp.where(hit, z, 0.0))
        return carry

    lax.fori_loop(0, steps, forward, 0)
    top = jnp.max(run[0], axis=1, keepdims=True)
    run[0] = jnp.zeros(run.shape[1:], F32)

    def exps(i, carry):
        run[0] = run[0] + fold(jnp.add, jnp.exp(z_v[i] - top))
        return carry

    lax.fori_loop(0, steps, exps, 0)
    total = jnp.sum(run[0], axis=1, keepdims=True)
    label = jnp.sum(run[1], axis=1, keepdims=True)
    narrow = lax.broadcasted_iota(jnp.int32, (toks, 128), 1)
    packed = jnp.where(narrow == 0, top, jnp.where(narrow == 1, total, jnp.where(narrow == 2, label, 0.0)))
    mine[ALL] = jnp.transpose(packed)[:8]
    stat = []
    for i in range(1, NTP):
        stat.append(rdma(mine, theirs.at[i], st_send.at[i], st_recv.at[i], to_tp(rem(at.tp + i, NTP))))
        stat[-1].start()
    theirs[0] = mine[ALL]
    spread.run(middle)
    for copy in stat:
        copy.wait_recv()
    parts = [theirs[rem(at.tp - j + NTP, NTP)] for j in range(NTP)]
    peak = functools.reduce(jnp.maximum, [p[0:1] for p in parts])
    total = functools.reduce(jnp.add, [p[1:2] * jnp.exp(p[0:1] - peak) for p in parts])
    label = functools.reduce(jnp.add, [p[2:3] for p in parts])
    lse = peak + jnp.log(total)
    loss = jnp.sum(jnp.log(total) + peak - label, axis=1, keepdims=True)
    sub = lax.broadcasted_iota(jnp.int32, (8, toks), 0)
    row_out[ALL] = jnp.where(sub == 0, lse, jnp.where(sub == 1, lab_row[ALL], 0.0))
    upper = lax.broadcasted_iota(jnp.int32, ids.shape, 1) >= 64
    tile_out[ALL] = jnp.where(upper == (rem(at.z, 2) == 1), ids[ALL], loss)
    tiles[0] = tile_out[ALL]
    rows_sent = []
    for i in range(NY - 1):
        to_y = to_dp(at.dp_of_y(NY - 1 - i))
        rows_sent.append(rdma(row_out, row_in.at[i], row_send.at[i], row_recv.at[i], to_y))
        rows_sent.append(rdma(tile_out, tile_in.at[i], t_send.at[i], t_recv.at[i], to_y))
    for copy in rows_sent:
        copy.start()
    run[0] = jnp.transpose(jnp.broadcast_to(lse, (128, toks)))
    inv_total = 1.0 / tok_total

    def put(i):
        half = rem(i, 2)
        return pltpu.make_async_copy(grad_v.at[half], grads.at[i], grad_sem.at[half])

    def backward(i, carry):
        start = start_of(i)
        shift = jnp.concatenate([run[0]] * (VT // 128), axis=1)
        prob = jnp.exp(z_v[i] - shift)
        hit = (lane + start == marks[:, 0:1]) & (lane >= i * VT - start)

        @pl.when(i >= 2)
        def _():
            put(i - 2).wait()

        grad_v[rem(i, 2)] = ((prob - jnp.where(hit, 1.0, 0.0)) * inv_total).astype(BF16)
        put(i).start()
        return carry

    lax.fori_loop(0, steps, backward, 0)
    for i in range(max(0, steps - 2), steps):
        put(jnp.int32(i)).wait()
    spread.run(late)
    for e in spread.events:
        if e not in near:
            spread.take(e[0])
    for copy in rows_sent:
        copy.wait_recv()
    stats[0] = row_out[ALL]
    for i in range(NY - 1):
        stats[i + 1] = row_in[i]
        tiles[i + 1] = tile_in[i]
    keep.wait()
    spread.end()
    for copy in stat + rows_sent:
        copy.wait_send()


class SumZ:
    def __init__(self, at, parts, came, total, chunks, send, recv):
        self.at, self.parts, self.came, self.total = at, parts, came, total
        self.chunks, self.send, self.recv = chunks, send, recv
        self.last = at.nz // 2

    def rows(self, c, s, way):
        lo, hi = self.chunks[c]
        if s == 1:
            mid = lo + 8 * pl.cdiv(hi - lo, 16)
            lo, hi = (lo, mid) if way > 0 else (mid, hi)
        return pl.ds(lo, hi - lo)

    def slot(self, s, way):
        return 0 if s == 1 else 2 * (s - 1) - (way > 0)

    def goal(self, s, way):
        return rem(self.at.z + way * (self.last + 1 - s) + self.at.nz, self.at.nz)

    def copy(self, c, s, way):
        rows, w = self.rows(c, s, way), WAYS.index(way)
        sems = self.send.at[w, s, c], self.recv.at[w, s, c]
        src = self.parts.at[self.goal(s, way), rows]
        return rdma(src, self.came.at[self.slot(s, way), rows], *sems, to_dp(self.at.dp_of_z(way)))

    def begin(self, c):
        rows = pl.ds(self.chunks[c][0], self.chunks[c][1] - self.chunks[c][0])
        self.total[rows] = self.parts[self.at.z, rows]
        for way in WAYS:
            self.copy(c, 1, way).start()

    def run(self, c, s):
        for way in WAYS:
            self.copy(c, s, way).wait_recv()
            rows, slot = self.rows(c, s, way), self.slot(s, way)
            if s < self.last:
                goal = self.goal(s + 1, way)
                self.parts[goal, rows] = self.parts[goal, rows] + self.came[slot, rows]
                self.copy(c, s + 1, way).start()
            else:
                self.total[rows] = self.total[rows] + self.came[slot, rows]

    def end(self):
        for c in range(len(self.chunks)):
            for s in range(self.last):
                for way in WAYS:
                    self.copy(c, s + 1, way).wait_send()


def finish_kernel(
    nz, stride, vocab_loc, tok_total, row_plan, dh_plan, table_plan, chunks,
    table, ub, stats, grads, u, r, tiles,
    d_trunk, loss, stack, all_dh,
    pb, rl, fin, land, all_tiles, table_v, ub_v, grad_v, parts, came, total, dh_v, du, rows_v, logit_v,
    rs_send, rs_recv, row_send, row_recv, z_send, z_recv, i_send, i_recv, x_send, x_recv, s_send, s_recv, t_send, t_recv,
    load_sem, stage_sem, dh_sem, rows_sem, logit_sem,
):
    at = Place(nz)
    own, width = u.shape
    win, cols = total.shape
    toks = stats.shape[2]
    block = nz * own
    slab = 128
    first = pl.multiple_of(at.y * stride, 16)
    load = pltpu.make_async_copy(table.at[pl.ds(first, win)], table_v, load_sem)

    depth, per = 4, toks // slab
    slabs = NY * per

    def staged(slot):
        return du.at[pl.ds(pl.multiple_of(slot * slab, slab), slab)]

    def fill(i):
        rows = pl.ds(pl.multiple_of(rem(i, per) * slab, slab), slab)
        slot = rem(i, depth)
        return pltpu.make_async_copy(ub.at[lax.div(i, jnp.int32(per)), rows], staged(slot), stage_sem.at[slot])

    for i in range(depth):
        fill(jnp.int32(i)).start()
    load.start()
    steps = grads.shape[0]

    def start_of(i):
        return pl.multiple_of(jnp.minimum(i * VT, vocab_loc - VT), 16)

    def bring(i):
        half = rem(i, 2)
        return [
            pltpu.make_async_copy(table.at[pl.ds(start_of(i), VT)], rows_v.at[half], rows_sem.at[half]),
            pltpu.make_async_copy(grads.at[i], logit_v.at[half], logit_sem.at[half]),
        ]

    for copy in bring(jnp.int32(0)):
        copy.start()
    greet(
        [to_tp(rem(at.tp + i, NTP)) for i in range(1, NTP)]
        + [to_dp(at.dp_of_z(i)) for i in range(1, nz)]
        + [to_dp(at.dp_of_y(way)) for way in WAYS]
    )
    sum_tp = SumTp(at, du, own, pb, rl, fin, rs_send, rs_recv)

    def narrow(n):
        def body(k, carry):
            i = n * per + k
            fill(i).wait()
            ub_v[pl.ds(pl.multiple_of(i * slab, slab), slab)] = staged(rem(i, depth))[ALL].astype(BF16)

            @pl.when(i + depth < slabs)
            def _():
                fill(i + depth).start()

            return carry

        lax.fori_loop(0, per, body, 0)

    narrow(0)
    load.wait()

    inv_total = 1.0 / tok_total

    def logits(lo, hi, ahead=lambda n: None):
        vocab = at.tp * vocab_loc + first + lo + lax.broadcasted_iota(jnp.int32, (hi - lo, toks), 0)

        def body(n, carry):
            ahead(n)
            cut = pl.ds(pl.multiple_of(n * toks, 128), toks)
            z = lax.dot_general(table_v[lo:hi, :], ub_v[cut, :], NT_DIMS, preferred_element_type=F32)
            row = stats[n]
            prob = jnp.exp(z - row[0:1])
            hit = vocab == row[1:2].astype(jnp.int32)
            grad_v[0 : hi - lo, cut] = ((prob - jnp.where(hit, 1.0, 0.0)) * inv_total).astype(BF16)
            return carry

        lax.fori_loop(0, NY, body, 0)

    def head(lo, hi):
        def body(n, carry):
            cut = pl.ds(pl.multiple_of(n * cols, 128), cols)
            parts[n, lo:hi] = jnp.dot(grad_v[0 : hi - lo, :], ub_v[:, cut], preferred_element_type=F32)
            return carry

        lax.fori_loop(0, nz, body, 0)

    sums = SumZ(at, parts, came, total, chunks, s_send, s_recv)

    def sum_step(c, k):
        if k <= sums.last:
            sums.run(c, k)

    def narrow_next(n):
        @pl.when(n + 1 < NY)
        def _():
            narrow(n + 1)

    logits(*chunks[0], narrow_next)
    head(*chunks[0])
    sums.begin(0)
    wide = min(512, width)
    du[ALL] = jnp.zeros(du.shape, F32)

    def backward(i, carry):
        for copy in bring(i):
            copy.wait()

        @pl.when(i + 1 < steps)
        def _():
            for copy in bring(i + 1):
                copy.start()

        @pl.when(i == min(5, steps - 1))
        def _():
            sum_step(0, 1)

        half = rem(i, 2)
        for n in range(width // wide):
            cut = pl.ds(n * wide, wide)
            du[:, cut] = du[:, cut] + jnp.dot(logit_v[half], rows_v[half, :, cut], preferred_element_type=F32)
        return carry

    lax.fori_loop(0, steps, backward, 0)
    sum_tp.begin()
    sum_step(0, 2)
    logits(*chunks[1])
    sum_tp.pass_on()
    head(*chunks[1])
    sums.begin(1)
    sum_tp.join()
    sum_step(0, 3)
    logits(*chunks[2])
    head(*chunks[2])
    grad = sum_tp.result()
    normed = u[ALL]
    mean_g = jnp.mean(grad, axis=-1, keepdims=True)
    mean_gu = jnp.mean(grad * normed, axis=-1, keepdims=True)
    land[at.tp] = r[:, 0:1] * (grad - mean_g - normed * mean_gu)

    def row_block(dx, dy, cross, lo, hi):
        return land.at[at.tp_of(dx, cross), pl.ds(lo, hi - lo)]

    whole_rows = Spread(at, row_plan, own, row_block, row_send, row_recv)
    whole_rows.begin()
    here = pl.ds(pl.multiple_of(at.z * own, own), own)
    turned = []
    for i in range(1, nz):
        col, to_z = pl.multiple_of(rem(at.z + i, nz) * cols, 128), to_dp(at.dp_of_z(i))
        src = land.at[at.tp, :, pl.ds(col, cols)]
        turned.append(rdma(src, all_dh.at[at.tp, 0, here], z_send.at[i], z_recv.at[i], to_z))
        turned.append(rdma(tiles, all_tiles.at[at.z], i_send.at[i], i_recv.at[i], to_z))
    for copy in turned:
        copy.start()
    my_col = pl.multiple_of(at.z * cols, 128)
    mine = pltpu.make_async_copy(land.at[at.tp, :, pl.ds(my_col, cols)], all_dh.at[at.tp, 0, here], load_sem)
    mine.start()
    all_tiles[at.z] = tiles[ALL]
    sums.begin(2)
    sum_step(1, 1)
    sum_step(0, 4)
    whole_rows.run(whole_rows.events)
    mine.wait()
    for copy in turned:
        copy.wait_recv()

    def dh_block(dx, dy, cross, lo, hi):
        return all_dh.at[at.tp_of(dx, cross), dy % NY, pl.ds(lo, hi - lo)]

    blocks = Spread(at, dh_plan, block, dh_block, x_send, x_recv)
    blocks.begin()

    pieces = {(0, 0): [(blocks.count, [], 0)]}
    for e in blocks.events:
        dx, dy = blocks.goal(e[0])
        pieces.setdefault((dx % NX, dy % NY), []).append(e)
    order = sorted((pieces[p][-1][-1] + cross * (block // 3), *p, cross) for p in pieces for cross in range(2))
    left = list(blocks.events)
    due = []
    for time, dx, dy, cross in order:
        due.append([e for e in left if e[-1] <= time])
        left = [e for e in left if e[-1] > time]
    code = [dx + NX * (dy + NY * cross) for _, dx, dy, cross in order]
    ready = 2

    def meet(k):
        blocks.run(due[k])
        _, dx, dy, cross = order[k]
        if cross:
            for part in pieces[dx, dy]:
                blocks.take(part[0])

    for k in range(ready):
        meet(k)
    for i in range(whole_rows.count + 1):
        whole_rows.take(i)
    ub_v[0:toks] = land[ALL].reshape(toks, width).astype(BF16)
    keep_rows = pltpu.make_async_copy(ub_v.at[0:toks], d_trunk, rows_sem.at[0])
    keep_rows.start()
    upper = lax.broadcasted_iota(jnp.int32, loss.shape, 1) >= 64
    loss[ALL] = sum(
        jnp.where(upper == (z % 2 == 0), all_tiles[z, rem(y - at.y + NY, NY)], 0.0) for z in range(nz) for y in range(NY)
    )

    beside = {k: (c, step) for k, c, step in BESIDE if step <= sums.last}
    low = (at.tp * vocab_loc + at.y * stride).astype(F32)

    def place_of(e):
        mark = jnp.int32(code[0])
        for k in range(1, len(order)):
            mark = jnp.where(e == k, code[k], mark)
        core = jnp.where(mark >= NX * NY, 1 - at.c, at.c)
        return 2 * rem(at.x + rem(mark, NX), NX) + core, rem(lax.div(mark, jnp.int32(NX)), NY)

    def fetch(e):
        tp, far = place_of(e)
        half = rem(e, 2)
        return pltpu.make_async_copy(all_dh.at[tp, far], dh_v.at[half], dh_sem.at[half])

    def piece(e, carry):
        for k in range(len(order)):
            met = k + 1 if k + 1 < len(order) and k + 1 >= ready else 0
            if k in beside or met:

                @pl.when(e == k)
                def _(k=k, met=met):
                    if k in beside:
                        sums.run(*beside[k])
                    if met:
                        meet(met)

        @pl.when(e + 1 < len(order))
        def _():
            fetch(e + 1).start()

        tp, far = place_of(e)
        ids = jnp.concatenate(
            [
                jnp.where(upper[0:1], all_tiles[2 * j + 1, far, pl.ds(tp, 1), :], all_tiles[2 * j, far, pl.ds(tp, 1), :])
                for j in range(nz // 2)
            ],
            axis=1,
        )
        fetch(e).wait()
        dh = dh_v[rem(e, 2)]
        hi = dh.astype(BF16)
        rest = dh - hi.astype(F32)
        mid = rest.astype(BF16)
        lo = (rest - mid.astype(F32)).astype(BF16)
        ids = (ids - low).astype(jnp.int32)
        for begin, end in chunks:
            row = lax.broadcasted_iota(jnp.int32, (end - begin, block), 0) + begin
            pick = jnp.where(row == ids, 1.0, 0.0).astype(BF16)
            found = sum(jnp.dot(pick, term, preferred_element_type=F32) for term in (hi, mid, lo))
            total[begin:end] = total[begin:end] + found
        return carry

    fetch(jnp.int32(0)).start()
    lax.fori_loop(0, len(order), piece, 0)
    for copy in turned:
        copy.wait_send()

    sends, starts, events = table_plan
    device = {(0, way): to_dp(at.dp_of_z(way)) for way in WAYS} | {(1, way): to_dp(at.dp_of_y(way)) for way in WAYS}

    def copy_of(i, arrives=False):
        axis, way, off, lo, hi = sends[i]
        if arrives:
            off = tuple(o - way * (a == axis) for a, o in enumerate(off))
        dst = stack.at[rem(at.z + off[0] + nz, nz), at.y_of(off[1]), pl.ds(lo, hi - lo)]
        src = dst if any(off) else total.at[pl.ds(lo, hi - lo)]
        return rdma(src, dst, t_send.at[i], t_recv.at[i], device[axis, way])

    for c in range(1, len(chunks)):
        sum_step(c, 4)
    for i in sum(starts, []):
        copy_of(i).start()
    keep = pltpu.make_async_copy(total, stack.at[at.z, at.y], load_sem)
    keep.start()
    for i, new, _ in events:
        copy_of(i, True).wait_recv()
        for j in new:
            copy_of(j).start()
    keep.wait()
    keep_rows.wait()
    for i in range(len(sends)):
        copy_of(i).wait_send()
    sums.end()
    whole_rows.end()
    blocks.end()


def place_kernel(chunk, tok_total, stack, rows_in, loss_in, out, rows_out, loss_out, slots, rows_v, rest_v, load_sem, store_sem, rows_sem, rest_sem):
    nz, ny, have, cols = stack.shape
    depth = slots.shape[0]
    per = have // chunk
    total = ny * per
    ahead = depth // 2

    def loads(i):
        y, row = lax.div(i, jnp.int32(per)), pl.multiple_of(rem(i, per) * chunk, 8)
        s = rem(i, depth)
        return [
            pltpu.make_async_copy(
                stack.at[j, y, pl.ds(row, chunk)], slots.at[s, :, pl.ds(j * cols, cols)], load_sem.at[s, j]
            )
            for j in range(nz)
        ]

    def store(i):
        s, row = rem(i, depth), pl.multiple_of(i * chunk, 8)
        return pltpu.make_async_copy(slots.at[s], out.at[pl.ds(row, chunk)], store_sem.at[s])

    def prime(i, carry):
        for copy in loads(i):
            copy.start()
        return carry

    def body(i, carry):
        for copy in loads(i):
            copy.wait()
        store(i).start()

        @pl.when(i + ahead < total)
        def _():
            @pl.when(i >= ahead)
            def _():
                store(i - ahead).wait()

            for copy in loads(i + ahead):
                copy.start()

        return carry

    def drain(i, carry):
        store(i).wait()
        return carry

    rows_load = pltpu.make_async_copy(rows_in, rows_v, rows_sem)
    rows_store = pltpu.make_async_copy(rows_v, rows_out, rows_sem)
    lax.fori_loop(0, ahead, prime, 0)
    rows_load.start()
    used = per * chunk
    left = have - used
    rest = pltpu.make_async_copy(stack.at[:, ny - 1, pl.ds(used, left)], rest_v, rest_sem.at[0])
    rest.start()
    tails = [
        pltpu.make_async_copy(rest_v.at[j], out.at[pl.ds(ny * used, left), pl.ds(j * cols, cols)], rest_sem.at[j])
        for j in range(nz)
    ]
    lane = lax.broadcasted_iota(jnp.int32, (1, 128), 1)
    loss_out[0, 0] = jnp.sum(jnp.where(rem(lane, 64) == 0, loss_in[0:1], 0.0)) / tok_total
    rows_load.wait()
    rows_store.start()
    rest.wait()
    for copy in tails:
        copy.start()
    lax.fori_loop(0, total, body, 0)
    lax.fori_loop(total - 2 * ahead, total, drain, 0)
    for copy in tails:
        copy.wait()
    rows_store.wait()


def vmem():
    return pl.BlockSpec(memory_space=pltpu.VMEM)


def anywhere():
    return pl.BlockSpec(memory_space=pl.ANY)


def dma(*shape):
    return pltpu.SemaphoreType.DMA(shape)


def twice(*shape):
    return [dma(*shape)] * 2


def solution(mesh):
    ndp, ntp = mesh.shape["dp"], mesh.shape["tp"]
    nz = ndp // NY

    def per_device(table, ids, labels, trunk):
        vocab_loc, width = table.shape
        batch, seq = ids.shape
        toks = batch * seq
        own = toks // NTP
        tok_total = toks * ndp
        stride = (vocab_loc - 16) // NY
        win = stride + 16
        cols = width // nz
        block = nz * own
        big = 66_000_000
        dp, tp = lax.axis_index("dp"), lax.axis_index("tp")
        row_start = tp * vocab_loc
        local_ids = ids.reshape(toks) - row_start
        part = jnp.take(table, local_ids, axis=0, mode="clip")

        tp_sems = twice(10)
        tp_scratch = [
            pltpu.VMEM((4, own, width), F32),
            pltpu.VMEM((2, own // 2, width), F32),
            pltpu.VMEM((4, own // 2, width), F32),
            pltpu.VMEM((NTP, own, width), F32),
        ]
        ids_f = ids.reshape(NTP, own).astype(F32)
        blank = jnp.zeros_like(ids_f)
        even = rem(lax.div(dp, jnp.int32(NY)), 2) == 0
        pad = ((0, 0), (0, 128 - 2 * own))
        ids_tile = jnp.pad(jnp.concatenate([jnp.where(even, ids_f, blank), jnp.where(even, blank, ids_f)], axis=1), pad)
        marks = jnp.stack([labels.reshape(toks) - row_start, local_ids], axis=1)
        lab_row = labels.reshape(1, toks).astype(F32)
        steps = pl.cdiv(vocab_loc, VT)
        token_plan = gather_plan((NX, NY), two_colours(0, own, 0.5), 16, hold=2 * own)
        sends = 2 * len(token_plan[0]) + 1
        grads, ub, u_own, r_own, stats, tiles = pl.pallas_call(
            functools.partial(token_kernel, nz, tok_total, token_plan),
            out_shape=(
                jax.ShapeDtypeStruct((steps, toks, VT), BF16),
                jax.ShapeDtypeStruct((NY, NTP, own, width), F32),
                jax.ShapeDtypeStruct((own, width), F32),
                jax.ShapeDtypeStruct((own, 128), F32),
                jax.ShapeDtypeStruct((NY, 8, toks), F32),
                jax.ShapeDtypeStruct((NY, 8, 128), F32),
            ),
            in_specs=[anywhere(), anywhere(), anywhere(), vmem(), vmem(), vmem()],
            out_specs=(anywhere(), anywhere(), vmem(), vmem(), vmem(), vmem()),
            scratch_shapes=[
                pltpu.VMEM((toks, width), F32),
                pltpu.VMEM((own, width), BF16),
                pltpu.VMEM((2, toks, VT), BF16),
                pltpu.VMEM((vocab_loc, width), BF16),
                pltpu.VMEM((toks, width), BF16),
                pltpu.VMEM((steps, toks, VT), F32),
                pltpu.VMEM((2, toks, 128), F32),
                pltpu.VMEM((8, toks), F32),
                pltpu.VMEM((NTP, 8, toks), F32),
                pltpu.VMEM((8, toks), F32),
                pltpu.VMEM((NY - 1, 8, toks), F32),
                pltpu.VMEM((8, 128), F32),
                pltpu.VMEM((NY - 1, 8, 128), F32),
                *tp_scratch,
                dma(steps), pltpu.SemaphoreType.DMA, *twice(NTP), *twice(NY - 1), *twice(NY - 1), *tp_sems, *twice(sends), dma(2),
            ],
            compiler_params=pltpu.CompilerParams(collective_id=0, has_side_effects=True, vmem_limit_bytes=big),
            name="token",
        )(table, part, trunk.reshape(toks, width), marks, lab_row, ids_tile)

        row_plan = gather_plan((NX, 1), two_colours(0, own, 1), 16)
        dh_plan = gather_plan((NX, NY), two_colours(0, block, 0.5), block // 4)
        lead = 16 * pl.cdiv(win, 48)
        middle = 2 * lead
        chunks = ((0, lead), (lead, middle), (middle, win))
        third = 8 * pl.cdiv(win, 24)
        table_chunks = ((0, third), (third, 2 * third), (2 * third, win))
        shares = SHARES if nz == 8 else (0.5,) * 3
        table_parts = sum((two_colours(lo, hi, share) for (lo, hi), share in zip(table_chunks, shares)), [])
        table_plan = gather_plan((nz, NY), table_parts, 60)
        counts = [2 * len(p[0]) + 1 for p in (row_plan, dh_plan, table_plan)]
        zs = (2, nz // 2 + 1, len(chunks))
        d_rows, loss, stack, _ = pl.pallas_call(
            functools.partial(
                finish_kernel, nz, stride, vocab_loc, tok_total, row_plan, dh_plan, table_plan, chunks
            ),
            out_shape=(
                jax.ShapeDtypeStruct((toks, width), BF16),
                jax.ShapeDtypeStruct((8, 128), F32),
                jax.ShapeDtypeStruct((nz, NY, win, cols), F32),
                jax.ShapeDtypeStruct((NTP, NY, block, cols), F32),
            ),
            in_specs=[anywhere(), anywhere(), vmem(), anywhere(), vmem(), vmem(), vmem()],
            out_specs=(anywhere(), vmem(), anywhere(), anywhere()),
            scratch_shapes=[
                *tp_scratch,
                pltpu.VMEM((nz, NY, 8, 128), F32),
                pltpu.VMEM((win, width), BF16),
                pltpu.VMEM((NY * toks, width), BF16),
                pltpu.VMEM((middle - lead, NY * toks), BF16),
                pltpu.VMEM((nz, win, cols), F32),
                pltpu.VMEM((nz - 1, win, cols), F32),
                pltpu.VMEM((win, cols), F32),
                pltpu.VMEM((2, block, cols), F32),
                pltpu.VMEM((toks, width), F32),
                pltpu.VMEM((2, VT, width), BF16),
                pltpu.VMEM((2, toks, VT), BF16),
                *tp_sems, *twice(counts[0]), *twice(nz), *twice(nz), *twice(counts[1]), *twice(*zs), *twice(counts[2]),
                pltpu.SemaphoreType.DMA, dma(4), *twice(2), dma(2),
            ],
            compiler_params=pltpu.CompilerParams(collective_id=1, has_side_effects=True, vmem_limit_bytes=67_000_000),
            name="finish",
        )(table, ub.reshape(NY, toks, width), stats, grads, u_own, r_own, tiles)
        depth = 16 if nz == 8 else 8
        chunk = next(n for n in range(112, 0, -8) if stride % n == 0 and NY * stride >= n * depth)
        d_table, d_rows, mean_loss = pl.pallas_call(
            functools.partial(place_kernel, chunk, tok_total),
            out_shape=(
                jax.ShapeDtypeStruct((vocab_loc, width), F32),
                jax.ShapeDtypeStruct((toks, width), BF16),
                jax.ShapeDtypeStruct((1, 1), F32),
            ),
            in_specs=[anywhere(), anywhere(), vmem()],
            out_specs=(anywhere(), anywhere(), pl.BlockSpec(memory_space=pltpu.SMEM)),
            scratch_shapes=[
                pltpu.VMEM((depth, chunk, width), F32), pltpu.VMEM((toks, width), BF16),
                pltpu.VMEM((nz, win - stride, cols), F32), dma(depth, nz), dma(depth), pltpu.SemaphoreType.DMA, dma(nz),
            ],
            compiler_params=pltpu.CompilerParams(vmem_limit_bytes=big),
            name="place",
        )(stack, d_rows, loss)
        return mean_loss.reshape(()), d_rows.reshape(trunk.shape), d_table

    return jax.shard_map(
        per_device,
        mesh=mesh,
        in_specs=(P("tp", None), P("dp", None), P("dp", None), P("dp", None, None)),
        out_specs=(P(), P("dp", None, None), P("tp", None)),
        check_vma=False,
    )
```

```python
import functools
import heapq

import jax
import jax.numpy as jnp
from jax import lax
from jax.experimental import pallas as pl
from jax.experimental.pallas import tpu as pltpu
from jax.sharding import PartitionSpec as P

LN_EPS = 1e-5
MESH = pl.DeviceIdType.MESH
F32, BF16 = jnp.float32, jnp.bfloat16
NY, NTP, NX = 4, 8, 4
WAYS = (1, -1)
SUB = 8
LANES = 128
BESIDE = ((0, 2, 1), (6, 1, 2), (13, 2, 2), (20, 1, 3), (26, 2, 3))
SHARES = (0.55, 0.55, 0.7)
ALL = Ellipsis
NEG = float(jnp.finfo(jnp.float32).min)
VT = 512
NT_DIMS = (((1,), (1,)), ((), ()))
NN_DIMS = (((1,), (0,)), ((), ()))


def rem(a, b):
    return lax.rem(a, jnp.int32(b))


class Place:
    def __init__(self, nz):
        self.nz = nz
        self.dp = lax.axis_index("dp")
        self.tp = lax.axis_index("tp")
        self.z, self.y = lax.div(self.dp, jnp.int32(NY)), rem(self.dp, NY)
        self.x, self.c = lax.div(self.tp, jnp.int32(2)), rem(self.tp, 2)
        self.partner = 2 * self.x + (1 - self.c)

    def tp_of(self, step, other=False):
        c = 1 - self.c if other else self.c
        return 2 * rem(self.x + step + NX, NX) + c

    def y_of(self, step):
        return rem(self.y + step + NY, NY)

    def dp_of_y(self, step):
        return self.z * NY + self.y_of(step)

    def dp_of_z(self, step):
        return rem(self.z + step + self.nz, self.nz) * NY + self.y


def repeat(count, body):
    lax.fori_loop(0, count, body, 0)


def to_tp(tp):
    return {"tp": tp}


def to_dp(dp):
    return {"dp": dp}


def rdma(src, dst, send_sem, recv_sem, device):
    return pltpu.make_async_remote_copy(
        src_ref=src, dst_ref=dst, send_sem=send_sem, recv_sem=recv_sem, device_id=device, device_id_type=MESH
    )


def greet(devices):
    barrier = pltpu.get_barrier_semaphore()
    for device in devices:
        pl.semaphore_signal(barrier, inc=1, device_id=device, device_id_type=MESH)
    return lambda: pl.semaphore_wait(barrier, len(devices))


class SumTp:
    def __init__(self, at, src, own, pb, rl, fin, send, recv):
        self.src, self.own, self.half, self.pb, self.rl, self.fin = src, own, own // 2, pb, rl, fin
        self.at, self.send, self.recv = at, send, recv
        self.steps = (2, 1, -1, 0)
        self.copies = []

    def copy(self, i, src, dst, tp):
        self.copies.append(rdma(src, dst, self.send.at[i], self.recv.at[i], to_tp(tp)))
        return self.copies[-1]

    def rows(self, step, other):
        return pl.ds(pl.multiple_of(self.at.tp_of(step, other) * self.own, self.own), self.own)

    def part(self, i, h):
        return self.pb.at[i, pl.ds(h * self.half, self.half)]

    def begin(self):
        for i, step in enumerate(self.steps):
            self.copy(i, self.src.at[self.rows(step, True)], self.pb.at[i], self.at.partner).start()

    def merge(self, i):
        self.copies[i].wait_recv()
        self.pb[i] = self.pb[i] + self.src[self.rows(self.steps[i], False), :]

    def pass_on(self):
        plus, minus = self.at.tp_of(1), self.at.tp_of(-1)
        self.merge(0)
        for h, tp in enumerate((plus, minus)):
            self.copy(4 + h, self.part(0, h), self.rl.at[h], tp).start()
        self.merge(1)
        self.merge(2)
        self.copy(6, self.part(1, 1), self.fin.at[0], plus).start()
        self.copy(7, self.part(2, 0), self.fin.at[1], minus).start()

    def join(self):
        for h, tp in enumerate((self.at.tp_of(1), self.at.tp_of(-1))):
            self.copies[4 + h].wait_recv()
            rows = pl.ds(h * self.half, self.half)
            self.pb[1 + h, rows] = self.pb[1 + h, rows] + self.rl[h]
            self.copy(SUB + h, self.part(1 + h, h), self.fin.at[2 + h], tp).start()
        self.merge(3)

    def result(self):
        for copy in self.copies[6:]:
            copy.wait_recv()
        top = self.pb[3, 0 : self.half] + self.fin[2] + self.fin[1]
        low = self.pb[3, self.half : self.own] + self.fin[0] + self.fin[3]
        for copy in self.copies:
            copy.wait_send()
        return jnp.concatenate([top, low], axis=0)


def gather_plan(sizes, parts, latency, hold=0):
    sends, events, heap, busy = [], [], [], {}

    def post(axis, way, off, lo, hi, order, now):
        end = max(now, busy.get((axis, way), now)) + hi - lo
        busy[axis, way] = end
        there = tuple(o - way * (a == axis) for a, o in enumerate(off))
        heapq.heappush(heap, (end + latency, len(sends), there, lo, hi, order))
        sends.append((axis, way, off, lo, hi))
        return len(sends) - 1

    def ring(axis, way, off, lo, hi, order, now):
        last = sizes[axis] // 2
        gone = abs(off[axis]) + 1
        if gone > last:
            return []
        if gone == last:
            mid = lo + SUB * pl.cdiv(hi - lo, 16)
            lo, hi = (lo, mid) if way > 0 else (mid, hi)
        return [] if lo == hi else [post(axis, way, off, lo, hi, order, now)]

    starts = [[] for _ in parts]
    for leg in range(2):
        for begin, (lo, hi, order, now) in zip(starts, parts):
            for way in WAYS:
                begin += ring(order[leg], way, (0, 0), lo, hi, order, now)
    while heap:
        now, i, off, lo, hi, order = heapq.heappop(heap)
        axis, way = sends[i][:2]
        if off[1] and now < hold:
            heapq.heappush(heap, (hold, i, off, lo, hi, order))
            continue
        new = ring(axis, way, off, lo, hi, order, now)
        if axis == order[0]:
            for w in WAYS:
                new += ring(order[1], w, off, lo, hi, order, now)
        events.append((i, new, now))
    return sends, starts, events


def two_colours(lo, hi, share, now=0):
    split = lo + SUB * round((hi - lo) * share / SUB)
    return [(lo, split, (0, 1), now), (split, hi, (1, 0), now)]


class Spread:
    def __init__(self, at, plan, rows, block, send, recv):
        self.sends, self.starts, self.events = plan
        self.block, self.send, self.recv, self.rows = block, send, recv, rows
        self.count = len(self.sends)
        self.other = to_tp(at.partner)
        self.device = {}
        for way in WAYS:
            self.device[0, way] = to_tp(at.tp_of(way))
            self.device[1, way] = to_dp(at.dp_of_y(way))

    def goal(self, i):
        axis, way, off = self.sends[i][:3]
        return tuple(o - way * (a == axis) for a, o in enumerate(off))

    def copy(self, i):
        axis, way, off, lo, hi = self.sends[i]
        src, dst = self.block(*off, False, lo, hi), self.block(off[0], self.goal(i)[1], False, lo, hi)
        return rdma(src, dst, self.send.at[i], self.recv.at[i], self.device[axis, way])

    def forward(self, i, cross=False):
        off, (lo, hi) = ((0, 0), (0, self.rows)) if i == self.count else (self.goal(i), self.sends[i][-2:])
        ref = self.block(*off, cross, lo, hi)
        return rdma(ref, ref, self.send.at[self.count + i], self.recv.at[self.count + i], self.other)

    def begin(self):
        for i in sum(self.starts, []):
            self.copy(i).start()
        self.forward(self.count).start()

    def run(self, events):
        for i, new, _ in events:
            ref = self.block(*self.goal(i), False, *self.sends[i][-2:])
            rdma(ref, ref, self.send.at[i], self.recv.at[i], self.other).wait_recv()
            for j in new:
                self.copy(j).start()
            self.forward(i).start()

    def take(self, i):
        self.forward(i, True).wait_recv()

    def end(self):
        for i in range(self.count):
            self.copy(i).wait_send()
        for i in range(self.count + 1):
            self.forward(i).wait_send()


def token_kernel(
    nz, tok_total, plan, table, part, trunk, marks, lab_row, ids,
    grads, ub_all, u_out, r_out, stats, tiles,
    du, trunk_v, grad_v, table_v, ub_v, z_v, run, mine, theirs, row_out, row_in, tile_out, tile_in, pb, rl, fin, land,
    load_sem, part_sem, st_send, st_recv, row_send, row_recv, t_send, t_recv, rs_send, rs_recv, x_send, x_recv,
    grad_sem,
):
    at = Place(nz)
    rows, width = table_v.shape
    toks = ub_v.shape[0]
    own = trunk_v.shape[0]
    steps = z_v.shape[0]
    whole = rows // VT
    tail = rows - whole * VT

    part_copy = pltpu.make_async_copy(part, ub_v, part_sem)
    part_copy.start()
    trunk_copy = pltpu.make_async_copy(trunk.at[pl.ds(pl.multiple_of(at.tp * own, own), own)], trunk_v, grad_sem.at[0])
    trunk_copy.start()

    def load(i):
        start = pl.multiple_of(i * VT, 16)
        return pltpu.make_async_copy(table.at[pl.ds(start, VT)], table_v.at[pl.ds(start, VT)], load_sem.at[i])

    tail_copy = pltpu.make_async_copy(
        table.at[pl.ds(whole * VT, tail)], table_v.at[pl.ds(whole * VT, tail)], load_sem.at[whole]
    )
    met_all = greet([to_tp(rem(at.tp + i, NTP)) for i in range(1, NTP)] + [to_dp(at.dp_of_y(i)) for i in range(1, NY)])
    part_copy.wait()
    for i in range(whole):
        load(i).start()
    tail_copy.start()
    du[ALL] = ub_v[ALL].astype(F32)
    sums = SumTp(at, du, own, pb, rl, fin, rs_send, rs_recv)
    met_all()
    sums.begin()
    sums.pass_on()
    sums.join()
    trunk_copy.wait()
    hidden = sums.result() + trunk_v[ALL].astype(F32)
    centered = hidden - jnp.mean(hidden, axis=-1, keepdims=True)
    inv_std = lax.rsqrt(jnp.mean(centered * centered, axis=-1, keepdims=True) + LN_EPS)
    normed = centered * inv_std
    land[at.tp] = normed.astype(BF16).astype(F32)

    def block(dx, dy, cross, lo, hi):
        tp, cut = at.tp_of(dx, cross), pl.ds(lo, hi - lo)
        return ub_all.at[dy % NY, tp, cut] if dy % NY else land.at[tp, cut]

    spread = Spread(at, plan, own, block, x_send, x_recv)
    spread.begin()
    u_out[ALL] = normed
    r_out[ALL] = jnp.broadcast_to(inv_std, r_out.shape)
    near = [e for e in spread.events if spread.goal(e[0])[1] == 0]
    spread.run(near)
    for e in near:
        spread.take(e[0])
    spread.take(spread.count)
    groups = {}
    pace = own / 7.5
    for e in [e for e in spread.events if e not in near]:
        due = max(0, int((e[-1] - near[-1][-1]) / pace)) + 2
        groups.setdefault(due, []).append(e)
    middle, late = ([e for due in sorted(groups) if (due >= steps) and (due < steps + 6) == m for e in groups[due]] for m in (True, False))

    def attend(step):
        for due, events in groups.items():
            if due < steps:

                @pl.when(step == due)
                def _(events=events):
                    spread.run(events)

    keep = pltpu.make_async_copy(land, ub_all.at[0], part_sem)
    keep.start()
    ub_v[ALL] = land[ALL].reshape(toks, width).astype(BF16)
    run[0] = jnp.full(run.shape[1:], NEG, F32)
    run[1] = jnp.zeros(run.shape[1:], F32)
    lane = lax.broadcasted_iota(jnp.int32, (toks, VT), 1)

    def start_of(i):
        return pl.multiple_of(jnp.minimum(i * VT, rows - VT), 16)

    def fold(op, v):
        return functools.reduce(op, [v[:, j : j + LANES] for j in range(0, VT, LANES)])

    def forward(i, carry):
        attend(i)

        @pl.when(i < whole)
        def _():
            load(i).wait()

        @pl.when(i == whole)
        def _():
            tail_copy.wait()

        start = start_of(i)
        z = lax.dot_general(ub_v[ALL], table_v[pl.ds(start, VT), :], NT_DIMS, preferred_element_type=F32)
        z = jnp.where(lane >= i * VT - start, z, NEG)
        z_v[i] = z
        run[0] = jnp.maximum(run[0], fold(jnp.maximum, z))
        hit = (lane + start == marks[:, 0:1]) & (lane >= i * VT - start)
        run[1] = run[1] + fold(jnp.add, jnp.where(hit, z, 0.0))
        return carry

    repeat(steps, forward)
    top = jnp.max(run[0], axis=1, keepdims=True)
    run[0] = jnp.zeros(run.shape[1:], F32)

    def exps(i, carry):
        run[0] = run[0] + fold(jnp.add, jnp.exp(z_v[i] - top))
        return carry

    repeat(steps, exps)
    total = jnp.sum(run[0], axis=1, keepdims=True)
    label = jnp.sum(run[1], axis=1, keepdims=True)
    narrow = lax.broadcasted_iota(jnp.int32, (toks, LANES), 1)
    packed = jnp.where(narrow == 0, top, jnp.where(narrow == 1, total, jnp.where(narrow == 2, label, 0.0)))
    mine[ALL] = jnp.transpose(packed)[:SUB]
    stat = []
    for i in range(1, NTP):
        stat.append(rdma(mine, theirs.at[i], st_send.at[i], st_recv.at[i], to_tp(rem(at.tp + i, NTP))))
        stat[-1].start()
    theirs[0] = mine[ALL]
    spread.run(middle)
    for copy in stat:
        copy.wait_recv()
    parts = [theirs[rem(at.tp - j + NTP, NTP)] for j in range(NTP)]
    peak = functools.reduce(jnp.maximum, [p[0:1] for p in parts])
    total = functools.reduce(jnp.add, [p[1:2] * jnp.exp(p[0:1] - peak) for p in parts])
    label = functools.reduce(jnp.add, [p[2:3] for p in parts])
    lse = peak + jnp.log(total)
    loss = jnp.sum(jnp.log(total) + peak - label, axis=1, keepdims=True)
    sub = lax.broadcasted_iota(jnp.int32, (SUB, toks), 0)
    row_out[ALL] = jnp.where(sub == 0, lse, jnp.where(sub == 1, lab_row[ALL], 0.0))
    upper = lax.broadcasted_iota(jnp.int32, ids.shape, 1) >= 64
    tile_out[ALL] = jnp.where(upper == (rem(at.z, 2) == 1), ids[ALL], loss)
    tiles[0] = tile_out[ALL]
    rows_sent = []
    for i in range(NY - 1):
        to_y = to_dp(at.dp_of_y(NY - 1 - i))
        rows_sent.append(rdma(row_out, row_in.at[i], row_send.at[i], row_recv.at[i], to_y))
        rows_sent.append(rdma(tile_out, tile_in.at[i], t_send.at[i], t_recv.at[i], to_y))
    for copy in rows_sent:
        copy.start()
    run[0] = jnp.transpose(jnp.broadcast_to(lse, (LANES, toks)))
    inv_total = 1.0 / tok_total

    def put(i):
        half = rem(i, 2)
        return pltpu.make_async_copy(grad_v.at[half], grads.at[i], grad_sem.at[half])

    def backward(i, carry):
        start = start_of(i)
        shift = jnp.concatenate([run[0]] * (VT // LANES), axis=1)
        prob = jnp.exp(z_v[i] - shift)
        hit = (lane + start == marks[:, 0:1]) & (lane >= i * VT - start)

        @pl.when(i >= 2)
        def _():
            put(i - 2).wait()

        grad_v[rem(i, 2)] = ((prob - jnp.where(hit, 1.0, 0.0)) * inv_total).astype(BF16)
        put(i).start()
        return carry

    repeat(steps, backward)
    for i in range(max(0, steps - 2), steps):
        put(jnp.int32(i)).wait()
    spread.run(late)
    for e in spread.events:
        if e not in near:
            spread.take(e[0])
    for copy in rows_sent:
        copy.wait_recv()
    stats[0] = row_out[ALL]
    for i in range(NY - 1):
        stats[i + 1] = row_in[i]
        tiles[i + 1] = tile_in[i]
    keep.wait()
    spread.end()
    for copy in stat + rows_sent:
        copy.wait_send()


class SumZ:
    def __init__(self, at, parts, came, total, chunks, send, recv):
        self.at, self.parts, self.came, self.total = at, parts, came, total
        self.chunks, self.send, self.recv = chunks, send, recv
        self.last = at.nz // 2

    def rows(self, c, s, way):
        lo, hi = self.chunks[c]
        if s == 1:
            mid = lo + SUB * pl.cdiv(hi - lo, 16)
            lo, hi = (lo, mid) if way > 0 else (mid, hi)
        return pl.ds(lo, hi - lo)

    def slot(self, s, way):
        return 0 if s == 1 else 2 * (s - 1) - (way > 0)

    def goal(self, s, way):
        return rem(self.at.z + way * (self.last + 1 - s) + self.at.nz, self.at.nz)

    def copy(self, c, s, way):
        rows, w = self.rows(c, s, way), WAYS.index(way)
        sems = self.send.at[w, s, c], self.recv.at[w, s, c]
        src = self.parts.at[self.goal(s, way), rows]
        return rdma(src, self.came.at[self.slot(s, way), rows], *sems, to_dp(self.at.dp_of_z(way)))

    def begin(self, c):
        rows = pl.ds(self.chunks[c][0], self.chunks[c][1] - self.chunks[c][0])
        self.total[rows] = self.parts[self.at.z, rows]
        for way in WAYS:
            self.copy(c, 1, way).start()

    def run(self, c, s):
        for way in WAYS:
            self.copy(c, s, way).wait_recv()
            rows, slot = self.rows(c, s, way), self.slot(s, way)
            if s < self.last:
                goal = self.goal(s + 1, way)
                self.parts[goal, rows] = self.parts[goal, rows] + self.came[slot, rows]
                self.copy(c, s + 1, way).start()
            else:
                self.total[rows] = self.total[rows] + self.came[slot, rows]

    def end(self):
        for c in range(len(self.chunks)):
            for s in range(self.last):
                for way in WAYS:
                    self.copy(c, s + 1, way).wait_send()


def finish_kernel(
    nz, stride, vocab_loc, tok_total, row_plan, dh_plan, table_plan, chunks,
    table, ub, stats, grads, u, r, tiles,
    d_trunk, loss, stack, all_dh,
    pb, rl, fin, land, all_tiles, table_v, ub_v, grad_v, parts, came, total, dh_v, du, rows_v, logit_v,
    rs_send, rs_recv, row_send, row_recv, z_send, z_recv, i_send, i_recv, x_send, x_recv, s_send, s_recv, t_send, t_recv,
    load_sem, stage_sem, dh_sem, rows_sem, logit_sem,
):
    at = Place(nz)
    own, width = u.shape
    win, cols = total.shape
    toks = stats.shape[2]
    block = nz * own
    slab = LANES
    first = pl.multiple_of(at.y * stride, 16)
    loads = [
        pltpu.make_async_copy(table.at[pl.ds(first + lo, hi - lo)], table_v.at[lo:hi], copy_sem)
        for (lo, hi), copy_sem in zip(chunks, (load_sem, dh_sem.at[0], dh_sem.at[1]))
    ]

    depth, per = 4, toks // slab
    slabs = NY * per

    def staged(slot):
        return du.at[pl.ds(pl.multiple_of(slot * slab, slab), slab)]

    def fill(i):
        rows = pl.ds(pl.multiple_of(rem(i, per) * slab, slab), slab)
        slot = rem(i, depth)
        return pltpu.make_async_copy(ub.at[lax.div(i, jnp.int32(per)), rows], staged(slot), stage_sem.at[slot])

    loads[0].start()
    for i in range(depth):
        fill(jnp.int32(i)).start()
    steps = grads.shape[0]

    def start_of(i):
        return pl.multiple_of(jnp.minimum(i * VT, vocab_loc - VT), 16)

    def bring(i):
        half = rem(i, 2)
        return [
            pltpu.make_async_copy(table.at[pl.ds(start_of(i), VT)], rows_v.at[half], rows_sem.at[half]),
            pltpu.make_async_copy(grads.at[i], logit_v.at[half], logit_sem.at[half]),
        ]

    for copy in loads[1:] + bring(jnp.int32(0)):
        copy.start()
    met_all = greet(
        [to_tp(rem(at.tp + i, NTP)) for i in range(1, NTP)]
        + [to_dp(at.dp_of_z(i)) for i in range(1, nz)]
        + [to_dp(at.dp_of_y(way)) for way in WAYS]
    )
    sum_tp = SumTp(at, du, own, pb, rl, fin, rs_send, rs_recv)

    def narrow(n):
        def body(k, carry):
            i = n * per + k
            fill(i).wait()
            ub_v[pl.ds(pl.multiple_of(i * slab, slab), slab)] = staged(rem(i, depth))[ALL].astype(BF16)

            @pl.when(i + depth < slabs)
            def _():
                fill(i + depth).start()

            return carry

        repeat(per, body)

    loads[0].wait()
    narrow(0)

    inv_total = 1.0 / tok_total

    def logits(lo, hi, ahead=lambda n: None):
        vocab = at.tp * vocab_loc + first + lo + lax.broadcasted_iota(jnp.int32, (hi - lo, toks), 0)

        def body(n, carry):
            ahead(n)
            cut = pl.ds(pl.multiple_of(n * toks, LANES), toks)
            z = lax.dot_general(table_v[lo:hi, :], ub_v[cut, :], NT_DIMS, preferred_element_type=F32)
            row = stats[n]
            prob = jnp.exp(z - row[0:1])
            hit = vocab == row[1:2].astype(jnp.int32)
            grad_v[0 : hi - lo, cut] = ((prob - jnp.where(hit, 1.0, 0.0)) * inv_total).astype(BF16)
            return carry

        repeat(NY, body)

    def head(lo, hi):
        def body(n, carry):
            cut = pl.ds(pl.multiple_of(n * cols, LANES), cols)
            parts[n, lo:hi] = jnp.dot(grad_v[0 : hi - lo, :], ub_v[:, cut], preferred_element_type=F32)
            return carry

        repeat(nz, body)

    sums = SumZ(at, parts, came, total, chunks, s_send, s_recv)

    def sum_step(c, k):
        if k <= sums.last:
            sums.run(c, k)

    def narrow_next(n):
        @pl.when(n + 1 < NY)
        def _():
            narrow(n + 1)

    logits(*chunks[0], narrow_next)
    head(*chunks[0])
    met_all()
    sums.begin(0)
    known = [
        rdma(tiles, all_tiles.at[at.z], i_send.at[i], i_recv.at[i], to_dp(at.dp_of_z(i))) for i in range(1, nz)
    ]
    for copy in known:
        copy.start()
    all_tiles[at.z] = tiles[ALL]
    wide = min(512, width)
    du[ALL] = jnp.zeros(du.shape, F32)

    def backward(i, carry):
        for copy in bring(i):
            copy.wait()

        @pl.when(i + 1 < steps)
        def _():
            for copy in bring(i + 1):
                copy.start()

        @pl.when(i == min(5, steps - 1))
        def _():
            sum_step(0, 1)

        half = rem(i, 2)
        for n in range(width // wide):
            cut = pl.ds(n * wide, wide)
            du[:, cut] = du[:, cut] + jnp.dot(logit_v[half], rows_v[half, :, cut], preferred_element_type=F32)
        return carry

    repeat(steps, backward)
    sum_tp.begin()
    sum_step(0, 2)
    for copy in loads[1:]:
        copy.wait()
    logits(*chunks[1])
    sum_tp.pass_on()
    head(*chunks[1])
    sums.begin(1)
    sum_tp.join()
    sum_step(0, 3)
    logits(*chunks[2])
    head(*chunks[2])
    grad = sum_tp.result()
    normed = u[ALL]
    mean_g = jnp.mean(grad, axis=-1, keepdims=True)
    mean_gu = jnp.mean(grad * normed, axis=-1, keepdims=True)
    land[at.tp] = r[:, 0:1] * (grad - mean_g - normed * mean_gu)

    def row_block(dx, dy, cross, lo, hi):
        return land.at[at.tp_of(dx, cross), pl.ds(lo, hi - lo)]

    whole_rows = Spread(at, row_plan, own, row_block, row_send, row_recv)
    whole_rows.begin()
    here = pl.ds(pl.multiple_of(at.z * own, own), own)
    turned = []
    for i in range(1, nz):
        col, to_z = pl.multiple_of(rem(at.z + i, nz) * cols, LANES), to_dp(at.dp_of_z(i))
        src = land.at[at.tp, :, pl.ds(col, cols)]
        turned.append(rdma(src, all_dh.at[at.tp, 0, here], z_send.at[i], z_recv.at[i], to_z))
    for copy in turned:
        copy.start()
    my_col = pl.multiple_of(at.z * cols, LANES)
    mine = pltpu.make_async_copy(land.at[at.tp, :, pl.ds(my_col, cols)], all_dh.at[at.tp, 0, here], load_sem)
    mine.start()
    sums.begin(2)
    sum_step(1, 1)
    sum_step(0, 4)
    whole_rows.run(whole_rows.events)
    mine.wait()
    for copy in turned + known:
        copy.wait_recv()

    def dh_block(dx, dy, cross, lo, hi):
        return all_dh.at[at.tp_of(dx, cross), dy % NY, pl.ds(lo, hi - lo)]

    blocks = Spread(at, dh_plan, block, dh_block, x_send, x_recv)
    blocks.begin()

    pieces = {(0, 0): [(blocks.count, [], 0)]}
    for e in blocks.events:
        dx, dy = blocks.goal(e[0])
        pieces.setdefault((dx % NX, dy % NY), []).append(e)
    order = sorted((pieces[p][-1][-1] + cross * (block // 3), *p, cross) for p in pieces for cross in range(2))
    left = list(blocks.events)
    due = []
    for time, dx, dy, cross in order:
        due.append([e for e in left if e[-1] <= time])
        left = [e for e in left if e[-1] > time]
    code = [dx + NX * (dy + NY * cross) for _, dx, dy, cross in order]
    ready = 2

    def meet(k):
        blocks.run(due[k])
        _, dx, dy, cross = order[k]
        if cross:
            for part in pieces[dx, dy]:
                blocks.take(part[0])

    for k in range(ready):
        meet(k)
    for i in range(whole_rows.count + 1):
        whole_rows.take(i)
    ub_v[0:toks] = land[ALL].reshape(toks, width).astype(BF16)
    keep_rows = pltpu.make_async_copy(ub_v.at[0:toks], d_trunk, rows_sem.at[0])
    keep_rows.start()
    upper = lax.broadcasted_iota(jnp.int32, loss.shape, 1) >= 64
    loss[ALL] = sum(
        jnp.where(upper == (z % 2 == 0), all_tiles[z, rem(y - at.y + NY, NY)], 0.0) for z in range(nz) for y in range(NY)
    )

    beside = {k: (c, step) for k, c, step in BESIDE if step <= sums.last}
    low = (at.tp * vocab_loc + at.y * stride).astype(F32)

    def place_of(e):
        mark = jnp.int32(code[0])
        for k in range(1, len(order)):
            mark = jnp.where(e == k, code[k], mark)
        core = jnp.where(mark >= NX * NY, 1 - at.c, at.c)
        return 2 * rem(at.x + rem(mark, NX), NX) + core, rem(lax.div(mark, jnp.int32(NX)), NY)

    def fetch(e):
        tp, far = place_of(e)
        half = rem(e, 2)
        return pltpu.make_async_copy(all_dh.at[tp, far], dh_v.at[half], dh_sem.at[half])

    def piece(e, carry):
        for k in range(len(order)):
            met = k + 1 if k + 1 < len(order) and k + 1 >= ready else 0
            if k in beside or met:

                @pl.when(e == k)
                def _(k=k, met=met):
                    if k in beside:
                        sums.run(*beside[k])
                    if met:
                        meet(met)

        @pl.when(e + 1 < len(order))
        def _():
            fetch(e + 1).start()

        tp, far = place_of(e)
        ids = jnp.concatenate(
            [
                jnp.where(upper[0:1], all_tiles[2 * j + 1, far, pl.ds(tp, 1), :], all_tiles[2 * j, far, pl.ds(tp, 1), :])
                for j in range(nz // 2)
            ],
            axis=1,
        )
        fetch(e).wait()
        dh = dh_v[rem(e, 2)]
        hi = dh.astype(BF16)
        rest = dh - hi.astype(F32)
        mid = rest.astype(BF16)
        lo = (rest - mid.astype(F32)).astype(BF16)
        ids = (ids - low).astype(jnp.int32)
        for begin, end in chunks:
            row = lax.broadcasted_iota(jnp.int32, (end - begin, block), 0) + begin
            pick = jnp.where(row == ids, 1.0, 0.0).astype(BF16)
            found = sum(jnp.dot(pick, term, preferred_element_type=F32) for term in (hi, mid, lo))
            total[begin:end] = total[begin:end] + found
        return carry

    fetch(jnp.int32(0)).start()
    repeat(len(order), piece)
    for copy in turned + known:
        copy.wait_send()

    sends, starts, events = table_plan
    device = {(0, way): to_dp(at.dp_of_z(way)) for way in WAYS} | {(1, way): to_dp(at.dp_of_y(way)) for way in WAYS}

    def copy_of(i, arrives=False):
        axis, way, off, lo, hi = sends[i]
        if arrives:
            off = tuple(o - way * (a == axis) for a, o in enumerate(off))
        dst = stack.at[rem(at.z + off[0] + nz, nz), at.y_of(off[1]), pl.ds(lo, hi - lo)]
        src = dst if any(off) else total.at[pl.ds(lo, hi - lo)]
        return rdma(src, dst, t_send.at[i], t_recv.at[i], device[axis, way])

    for c in range(1, len(chunks)):
        sum_step(c, 4)
    for i in sum(starts, []):
        copy_of(i).start()
    keep = pltpu.make_async_copy(total, stack.at[at.z, at.y], load_sem)
    keep.start()
    for i, new, _ in events:
        copy_of(i, True).wait_recv()
        for j in new:
            copy_of(j).start()
    keep.wait()
    keep_rows.wait()
    for i in range(len(sends)):
        copy_of(i).wait_send()
    sums.end()
    whole_rows.end()
    blocks.end()


def pick_kernel(group, table, marks, out, eights, sem):
    toks = out.shape[0]
    rows = table.shape[0]
    block = 32

    def fetch(t, carry):
        eight = pl.multiple_of(group[t] * SUB, SUB)
        mine = eights.at[pl.ds(pl.multiple_of(t * SUB, SUB), SUB)]
        pltpu.make_async_copy(table.at[pl.ds(eight, SUB)], mine, sem.at[lax.div(t, jnp.int32(part))]).start()
        return carry

    part = toks // sem.shape[0]
    lax.fori_loop(0, toks, fetch, 0, unroll=SUB)
    lane = lax.broadcasted_iota(jnp.int32, (block, SUB * block), 1)
    first = SUB * lax.broadcasted_iota(jnp.int32, (block, SUB * block), 0)

    def choose(b, carry):
        at = pl.multiple_of(b * block, block)
        row = marks[pl.ds(at, block), 1:2]
        hit = (lane - first == rem(row, SUB)) & (row >= 0) & (row < rows)
        some = eights[pl.ds(pl.multiple_of(at * SUB, SUB), SUB * block), :]
        out[pl.ds(at, block)] = jnp.dot(
            jnp.where(hit, 1.0, 0.0).astype(BF16), some, preferred_element_type=F32
        ).astype(BF16)
        return carry

    for q in range(sem.shape[0]):
        whole = pl.ds(q * part * SUB, part * SUB)
        pltpu.make_async_copy(table.at[pl.ds(0, part * SUB)], eights.at[whole], sem.at[q]).wait()
        lax.fori_loop(q * part // block, (q + 1) * part // block, choose, 0)


def place_kernel(chunk, tok_total, stack, rows_in, loss_in, out, rows_out, loss_out, slots, rows_v, rest_v, load_sem, store_sem, rows_sem, rest_sem):
    nz, ny, have, cols = stack.shape
    depth = slots.shape[0]
    per = have // chunk
    total = ny * per
    ahead = depth // 2

    def loads(i):
        y, row = lax.div(i, jnp.int32(per)), pl.multiple_of(rem(i, per) * chunk, SUB)
        s = rem(i, depth)
        return [
            pltpu.make_async_copy(
                stack.at[j, y, pl.ds(row, chunk)], slots.at[s, :, pl.ds(j * cols, cols)], load_sem.at[s, j]
            )
            for j in range(nz)
        ]

    def store(i):
        s, row = rem(i, depth), pl.multiple_of(i * chunk, SUB)
        return pltpu.make_async_copy(slots.at[s], out.at[pl.ds(row, chunk)], store_sem.at[s])

    def prime(i, carry):
        for copy in loads(i):
            copy.start()
        return carry

    def body(i, carry):
        for copy in loads(i):
            copy.wait()
        store(i).start()

        @pl.when(i + ahead < total)
        def _():
            @pl.when(i >= ahead)
            def _():
                store(i - ahead).wait()

            for copy in loads(i + ahead):
                copy.start()

        return carry

    def drain(i, carry):
        store(i).wait()
        return carry

    rows_load = pltpu.make_async_copy(rows_in, rows_v, rows_sem)
    rows_store = pltpu.make_async_copy(rows_v, rows_out, rows_sem)
    repeat(ahead, prime)
    rows_load.start()
    used = per * chunk
    left = have - used
    rest = pltpu.make_async_copy(stack.at[:, ny - 1, pl.ds(used, left)], rest_v, rest_sem.at[0])
    rest.start()
    tails = [
        pltpu.make_async_copy(rest_v.at[j], out.at[pl.ds(ny * used, left), pl.ds(j * cols, cols)], rest_sem.at[j])
        for j in range(nz)
    ]
    lane = lax.broadcasted_iota(jnp.int32, (1, LANES), 1)
    loss_out[0, 0] = jnp.sum(jnp.where(rem(lane, 64) == 0, loss_in[0:1], 0.0)) / tok_total
    rows_load.wait()
    rows_store.start()
    rest.wait()
    for copy in tails:
        copy.start()
    repeat(total, body)
    lax.fori_loop(total - 2 * ahead, total, drain, 0)
    for copy in tails:
        copy.wait()
    rows_store.wait()


def vmem():
    return pl.BlockSpec(memory_space=pltpu.VMEM)


def anywhere():
    return pl.BlockSpec(memory_space=pl.ANY)


def dma(*shape):
    return pltpu.SemaphoreType.DMA(shape)


def twice(*shape):
    return [dma(*shape)] * 2


def solution(mesh):
    ndp, ntp = mesh.shape["dp"], mesh.shape["tp"]
    nz = ndp // NY

    def per_device(table, ids, labels, trunk):
        vocab_loc, width = table.shape
        batch, seq = ids.shape
        toks = batch * seq
        own = toks // NTP
        tok_total = toks * ndp
        stride = (vocab_loc - 16) // NY
        win = stride + 16
        cols = width // nz
        block = nz * own
        big = 66_000_000
        dp, tp = lax.axis_index("dp"), lax.axis_index("tp")
        row_start = tp * vocab_loc
        local_ids = ids.reshape(toks) - row_start
        owned = (local_ids >= 0) & (local_ids < vocab_loc)

        tp_sems = twice(10)
        tp_scratch = [
            pltpu.VMEM((4, own, width), F32),
            pltpu.VMEM((2, own // 2, width), F32),
            pltpu.VMEM((4, own // 2, width), F32),
            pltpu.VMEM((NTP, own, width), F32),
        ]
        ids_f = ids.reshape(NTP, own).astype(F32)
        blank = jnp.zeros_like(ids_f)
        even = rem(lax.div(dp, jnp.int32(NY)), 2) == 0
        pad = ((0, 0), (0, LANES - 2 * own))
        ids_tile = jnp.pad(jnp.concatenate([jnp.where(even, ids_f, blank), jnp.where(even, blank, ids_f)], axis=1), pad)
        marks = jnp.stack([labels.reshape(toks) - row_start, local_ids], axis=1)
        lab_row = labels.reshape(1, toks).astype(F32)
        part = pl.pallas_call(
            pick_kernel,
            out_shape=jax.ShapeDtypeStruct((toks, width), BF16),
            in_specs=[pl.BlockSpec(memory_space=pltpu.SMEM), anywhere(), vmem()],
            out_specs=vmem(),
            scratch_shapes=[pltpu.VMEM((SUB * toks, width), BF16), dma(SUB)],
            compiler_params=pltpu.CompilerParams(vmem_limit_bytes=big),
            name="pick",
        )(jnp.where(owned, local_ids // SUB, jnp.arange(toks)), table, marks)
        steps = pl.cdiv(vocab_loc, VT)
        token_plan = gather_plan((NX, NY), two_colours(0, own, 0.5), 16, hold=2 * own)
        sends = 2 * len(token_plan[0]) + 1
        grads, ub, u_own, r_own, stats, tiles = pl.pallas_call(
            functools.partial(token_kernel, nz, tok_total, token_plan),
            out_shape=(
                jax.ShapeDtypeStruct((steps, toks, VT), BF16),
                jax.ShapeDtypeStruct((NY, NTP, own, width), F32),
                jax.ShapeDtypeStruct((own, width), F32),
                jax.ShapeDtypeStruct((own, LANES), F32),
                jax.ShapeDtypeStruct((NY, SUB, toks), F32),
                jax.ShapeDtypeStruct((NY, SUB, LANES), F32),
            ),
            in_specs=[anywhere(), anywhere(), anywhere(), vmem(), vmem(), vmem()],
            out_specs=(anywhere(), anywhere(), vmem(), vmem(), vmem(), vmem()),
            scratch_shapes=[
                pltpu.VMEM((toks, width), F32),
                pltpu.VMEM((own, width), BF16),
                pltpu.VMEM((2, toks, VT), BF16),
                pltpu.VMEM((vocab_loc, width), BF16),
                pltpu.VMEM((toks, width), BF16),
                pltpu.VMEM((steps, toks, VT), F32),
                pltpu.VMEM((2, toks, LANES), F32),
                pltpu.VMEM((SUB, toks), F32),
                pltpu.VMEM((NTP, SUB, toks), F32),
                pltpu.VMEM((SUB, toks), F32),
                pltpu.VMEM((NY - 1, SUB, toks), F32),
                pltpu.VMEM((SUB, LANES), F32),
                pltpu.VMEM((NY - 1, SUB, LANES), F32),
                *tp_scratch,
                dma(steps), pltpu.SemaphoreType.DMA, *twice(NTP), *twice(NY - 1), *twice(NY - 1), *tp_sems, *twice(sends), dma(2),
            ],
            compiler_params=pltpu.CompilerParams(collective_id=0, has_side_effects=True, vmem_limit_bytes=big),
            name="token",
        )(table, part, trunk.reshape(toks, width), marks, lab_row, ids_tile)

        row_plan = gather_plan((NX, 1), two_colours(0, own, 1), 16)
        dh_plan = gather_plan((NX, NY), two_colours(0, block, 0.5), block // 4)
        lead = 16 * pl.cdiv(win, 48)
        middle = 2 * lead
        chunks = ((0, lead), (lead, middle), (middle, win))
        third = SUB * pl.cdiv(win, 24)
        table_chunks = ((0, third), (third, 2 * third), (2 * third, win))
        shares = SHARES if nz == SUB else (0.5,) * 3
        table_parts = sum((two_colours(lo, hi, share) for (lo, hi), share in zip(table_chunks, shares)), [])
        table_plan = gather_plan((nz, NY), table_parts, 60)
        counts = [2 * len(p[0]) + 1 for p in (row_plan, dh_plan, table_plan)]
        zs = (2, nz // 2 + 1, len(chunks))
        d_rows, loss, stack, _ = pl.pallas_call(
            functools.partial(
                finish_kernel, nz, stride, vocab_loc, tok_total, row_plan, dh_plan, table_plan, chunks
            ),
            out_shape=(
                jax.ShapeDtypeStruct((toks, width), BF16),
                jax.ShapeDtypeStruct((SUB, LANES), F32),
                jax.ShapeDtypeStruct((nz, NY, win, cols), F32),
                jax.ShapeDtypeStruct((NTP, NY, block, cols), F32),
            ),
            in_specs=[anywhere(), anywhere(), vmem(), anywhere(), vmem(), vmem(), vmem()],
            out_specs=(anywhere(), vmem(), anywhere(), anywhere()),
            scratch_shapes=[
                *tp_scratch,
                pltpu.VMEM((nz, NY, SUB, LANES), F32),
                pltpu.VMEM((win, width), BF16),
                pltpu.VMEM((NY * toks, width), BF16),
                pltpu.VMEM((middle - lead, NY * toks), BF16),
                pltpu.VMEM((nz, win, cols), F32),
                pltpu.VMEM((nz - 1, win, cols), F32),
                pltpu.VMEM((win, cols), F32),
                pltpu.VMEM((2, block, cols), F32),
                pltpu.VMEM((toks, width), F32),
                pltpu.VMEM((2, VT, width), BF16),
                pltpu.VMEM((2, toks, VT), BF16),
                *tp_sems, *twice(counts[0]), *twice(nz), *twice(nz), *twice(counts[1]), *twice(*zs), *twice(counts[2]),
                pltpu.SemaphoreType.DMA, dma(4), *twice(2), dma(2),
            ],
            compiler_params=pltpu.CompilerParams(collective_id=1, has_side_effects=True, vmem_limit_bytes=67_000_000),
            name="finish",
        )(table, ub.reshape(NY, toks, width), stats, grads, u_own, r_own, tiles)
        depth = 16 if nz == SUB else SUB
        chunk = next(n for n in range(112, 0, -SUB) if stride % n == 0 and NY * stride >= n * depth)
        d_table, d_rows, mean_loss = pl.pallas_call(
            functools.partial(place_kernel, chunk, tok_total),
            out_shape=(
                jax.ShapeDtypeStruct((vocab_loc, width), F32),
                jax.ShapeDtypeStruct((toks, width), BF16),
                jax.ShapeDtypeStruct((1, 1), F32),
            ),
            in_specs=[anywhere(), anywhere(), vmem()],
            out_specs=(anywhere(), anywhere(), pl.BlockSpec(memory_space=pltpu.SMEM)),
            scratch_shapes=[
                pltpu.VMEM((depth, chunk, width), F32), pltpu.VMEM((toks, width), BF16),
                pltpu.VMEM((nz, win - stride, cols), F32), dma(depth, nz), dma(depth), pltpu.SemaphoreType.DMA, dma(nz),
            ],
            compiler_params=pltpu.CompilerParams(vmem_limit_bytes=big),
            name="place",
        )(stack, d_rows, loss)
        return mean_loss.reshape(()), d_rows.reshape(trunk.shape), d_table

    return jax.shard_map(
        per_device,
        mesh=mesh,
        in_specs=(P("tp", None), P("dp", None), P("dp", None), P("dp", None, None)),
        out_specs=(P(), P("dp", None, None), P("tp", None)),
        check_vma=False,
    )
```

```python
import functools
import heapq

import jax
import jax.numpy as jnp
from jax import lax
from jax.experimental import pallas as pl
from jax.experimental.pallas import tpu as pltpu
from jax.sharding import PartitionSpec as P

LN_EPS = 1e-5
MESH = pl.DeviceIdType.MESH
F32, BF16 = jnp.float32, jnp.bfloat16
NY, NTP, NX = 4, 8, 4
WAYS = (1, -1)
SUB = 8
LANES = 128
BESIDE = ((0, 2, 1), (6, 1, 2), (13, 2, 2), (20, 1, 3), (26, 2, 3))
SHARES = (0.55, 0.55, 0.7)
ALL = Ellipsis
NEG = float(jnp.finfo(jnp.float32).min)
VT = 512
NT_DIMS = (((1,), (1,)), ((), ()))
NN_DIMS = (((1,), (0,)), ((), ()))


def rem(a, b):
    return lax.rem(a, jnp.int32(b))


class Place:
    def __init__(self, nz):
        self.nz = nz
        self.dp = lax.axis_index("dp")
        self.tp = lax.axis_index("tp")
        self.z, self.y = lax.div(self.dp, jnp.int32(NY)), rem(self.dp, NY)
        self.x, self.c = lax.div(self.tp, jnp.int32(2)), rem(self.tp, 2)
        self.partner = 2 * self.x + (1 - self.c)

    def tp_of(self, step, other=False):
        c = 1 - self.c if other else self.c
        return 2 * rem(self.x + step + NX, NX) + c

    def y_of(self, step):
        return rem(self.y + step + NY, NY)

    def dp_of_y(self, step):
        return self.z * NY + self.y_of(step)

    def dp_of_z(self, step):
        return rem(self.z + step + self.nz, self.nz) * NY + self.y


def repeat(count, body):
    lax.fori_loop(0, count, body, 0)


def to_tp(tp):
    return {"tp": tp}


def to_dp(dp):
    return {"dp": dp}


def rdma(src, dst, send_sem, recv_sem, device):
    return pltpu.make_async_remote_copy(
        src_ref=src, dst_ref=dst, send_sem=send_sem, recv_sem=recv_sem, device_id=device, device_id_type=MESH
    )


def greet(devices):
    barrier = pltpu.get_barrier_semaphore()
    for device in devices:
        pl.semaphore_signal(barrier, inc=1, device_id=device, device_id_type=MESH)
    return lambda: pl.semaphore_wait(barrier, len(devices))


class SumTp:
    def __init__(self, at, src, own, pb, rl, fin, send, recv):
        self.src, self.own, self.half, self.pb, self.rl, self.fin = src, own, own // 2, pb, rl, fin
        self.at, self.send, self.recv = at, send, recv
        self.steps = (2, 1, -1, 0)
        self.copies = []

    def copy(self, i, src, dst, tp):
        self.copies.append(rdma(src, dst, self.send.at[i], self.recv.at[i], to_tp(tp)))
        return self.copies[-1]

    def rows(self, step, other):
        return pl.ds(pl.multiple_of(self.at.tp_of(step, other) * self.own, self.own), self.own)

    def part(self, i, h):
        return self.pb.at[i, pl.ds(h * self.half, self.half)]

    def begin(self):
        for i, step in enumerate(self.steps):
            self.copy(i, self.src.at[self.rows(step, True)], self.pb.at[i], self.at.partner).start()

    def merge(self, i):
        self.copies[i].wait_recv()
        self.pb[i] = self.pb[i] + self.src[self.rows(self.steps[i], False), :]

    def pass_on(self):
        plus, minus = self.at.tp_of(1), self.at.tp_of(-1)
        self.merge(0)
        for h, tp in enumerate((plus, minus)):
            self.copy(4 + h, self.part(0, h), self.rl.at[h], tp).start()
        self.merge(1)
        self.merge(2)
        self.copy(6, self.part(1, 1), self.fin.at[0], plus).start()
        self.copy(7, self.part(2, 0), self.fin.at[1], minus).start()

    def join(self):
        for h, tp in enumerate((self.at.tp_of(1), self.at.tp_of(-1))):
            self.copies[4 + h].wait_recv()
            rows = pl.ds(h * self.half, self.half)
            self.pb[1 + h, rows] = self.pb[1 + h, rows] + self.rl[h]
            self.copy(SUB + h, self.part(1 + h, h), self.fin.at[2 + h], tp).start()
        self.merge(3)

    def result(self):
        for copy in self.copies[6:]:
            copy.wait_recv()
        top = self.pb[3, 0 : self.half] + self.fin[2] + self.fin[1]
        low = self.pb[3, self.half : self.own] + self.fin[0] + self.fin[3]
        for copy in self.copies:
            copy.wait_send()
        return jnp.concatenate([top, low], axis=0)


def gather_plan(sizes, parts, latency, hold=0):
    sends, events, heap, busy = [], [], [], {}

    def post(axis, way, off, lo, hi, order, now):
        end = max(now, busy.get((axis, way), now)) + hi - lo
        busy[axis, way] = end
        there = tuple(o - way * (a == axis) for a, o in enumerate(off))
        heapq.heappush(heap, (end + latency, len(sends), there, lo, hi, order))
        sends.append((axis, way, off, lo, hi))
        return len(sends) - 1

    def ring(axis, way, off, lo, hi, order, now):
        last = sizes[axis] // 2
        gone = abs(off[axis]) + 1
        if gone > last:
            return []
        if gone == last:
            mid = lo + SUB * pl.cdiv(hi - lo, 16)
            lo, hi = (lo, mid) if way > 0 else (mid, hi)
        return [] if lo == hi else [post(axis, way, off, lo, hi, order, now)]

    starts = [[] for _ in parts]
    for leg in range(2):
        for begin, (lo, hi, order, now) in zip(starts, parts):
            for way in WAYS:
                begin += ring(order[leg], way, (0, 0), lo, hi, order, now)
    while heap:
        now, i, off, lo, hi, order = heapq.heappop(heap)
        axis, way = sends[i][:2]
        if off[1] and now < hold:
            heapq.heappush(heap, (hold, i, off, lo, hi, order))
            continue
        new = ring(axis, way, off, lo, hi, order, now)
        if axis == order[0]:
            for w in WAYS:
                new += ring(order[1], w, off, lo, hi, order, now)
        events.append((i, new, now))
    return sends, starts, events


def two_colours(lo, hi, share, now=0):
    split = lo + SUB * round((hi - lo) * share / SUB)
    return [(lo, split, (0, 1), now), (split, hi, (1, 0), now)]


class Spread:
    def __init__(self, at, plan, rows, block, send, recv):
        self.sends, self.starts, self.events = plan
        self.block, self.send, self.recv, self.rows = block, send, recv, rows
        self.count = len(self.sends)
        self.other = to_tp(at.partner)
        self.device = {}
        for way in WAYS:
            self.device[0, way] = to_tp(at.tp_of(way))
            self.device[1, way] = to_dp(at.dp_of_y(way))

    def goal(self, i):
        axis, way, off = self.sends[i][:3]
        return tuple(o - way * (a == axis) for a, o in enumerate(off))

    def copy(self, i):
        axis, way, off, lo, hi = self.sends[i]
        src, dst = self.block(*off, False, lo, hi), self.block(off[0], self.goal(i)[1], False, lo, hi)
        return rdma(src, dst, self.send.at[i], self.recv.at[i], self.device[axis, way])

    def forward(self, i, cross=False):
        off, (lo, hi) = ((0, 0), (0, self.rows)) if i == self.count else (self.goal(i), self.sends[i][-2:])
        ref = self.block(*off, cross, lo, hi)
        return rdma(ref, ref, self.send.at[self.count + i], self.recv.at[self.count + i], self.other)

    def begin(self):
        for i in sum(self.starts, []):
            self.copy(i).start()
        self.forward(self.count).start()

    def run(self, events):
        for i, new, _ in events:
            ref = self.block(*self.goal(i), False, *self.sends[i][-2:])
            rdma(ref, ref, self.send.at[i], self.recv.at[i], self.other).wait_recv()
            for j in new:
                self.copy(j).start()
            self.forward(i).start()

    def take(self, i):
        self.forward(i, True).wait_recv()

    def end(self):
        for i in range(self.count):
            self.copy(i).wait_send()
        for i in range(self.count + 1):
            self.forward(i).wait_send()


def columns(row):
    return jnp.transpose(jnp.broadcast_to(row.astype(F32), (LANES, row.shape[1]))).astype(jnp.int32)


def token_kernel(
    nz, tok_total, plan, table, part, trunk, labels, ids,
    grads, ub_all, u_out, r_out, stats, tiles,
    lab_v, du, trunk_v, grad_v, table_v, ub_v, z_v, run, mine, theirs, row_out, row_in, tile_out, tile_in, pb, rl, fin, land,
    load_sem, part_sem, st_send, st_recv, row_send, row_recv, t_send, t_recv, rs_send, rs_recv, x_send, x_recv,
    grad_sem,
):
    at = Place(nz)
    rows, width = table_v.shape
    toks = ub_v.shape[0]
    own = trunk_v.shape[0]
    steps = z_v.shape[0]
    whole = rows // VT
    tail = rows - whole * VT

    part_copy = pltpu.make_async_copy(part, ub_v, part_sem)
    part_copy.start()
    trunk_copy = pltpu.make_async_copy(trunk.at[pl.ds(pl.multiple_of(at.tp * own, own), own)], trunk_v, grad_sem.at[0])
    trunk_copy.start()

    def load(i):
        start = pl.multiple_of(i * VT, 16)
        return pltpu.make_async_copy(table.at[pl.ds(start, VT)], table_v.at[pl.ds(start, VT)], load_sem.at[i])

    tail_copy = pltpu.make_async_copy(
        table.at[pl.ds(whole * VT, tail)], table_v.at[pl.ds(whole * VT, tail)], load_sem.at[whole]
    )
    met_all = greet([to_tp(rem(at.tp + i, NTP)) for i in range(1, NTP)] + [to_dp(at.dp_of_y(i)) for i in range(1, NY)])
    lab_v[ALL] = columns(labels[ALL]) - at.tp * rows
    part_copy.wait()
    for i in range(whole):
        load(i).start()
    tail_copy.start()
    du[ALL] = ub_v[ALL].astype(F32)
    sums = SumTp(at, du, own, pb, rl, fin, rs_send, rs_recv)
    met_all()
    sums.begin()
    sums.pass_on()
    sums.join()
    trunk_copy.wait()
    hidden = sums.result() + trunk_v[ALL].astype(F32)
    centered = hidden - jnp.mean(hidden, axis=-1, keepdims=True)
    inv_std = lax.rsqrt(jnp.mean(centered * centered, axis=-1, keepdims=True) + LN_EPS)
    normed = centered * inv_std
    land[at.tp] = normed.astype(BF16).astype(F32)

    def block(dx, dy, cross, lo, hi):
        tp, cut = at.tp_of(dx, cross), pl.ds(lo, hi - lo)
        return ub_all.at[dy % NY, tp, cut] if dy % NY else land.at[tp, cut]

    spread = Spread(at, plan, own, block, x_send, x_recv)
    spread.begin()
    u_out[ALL] = normed
    r_out[ALL] = jnp.broadcast_to(inv_std, r_out.shape)
    near = [e for e in spread.events if spread.goal(e[0])[1] == 0]
    spread.run(near)
    for e in near:
        spread.take(e[0])
    spread.take(spread.count)
    groups = {}
    pace = own / 7.5
    for e in [e for e in spread.events if e not in near]:
        due = max(0, int((e[-1] - near[-1][-1]) / pace)) + 2
        groups.setdefault(due, []).append(e)
    middle, late = ([e for due in sorted(groups) if (due >= steps) and (due < steps + 6) == m for e in groups[due]] for m in (True, False))

    def attend(step):
        for due, events in groups.items():
            if due < steps:

                @pl.when(step == due)
                def _(events=events):
                    spread.run(events)

    keep = pltpu.make_async_copy(land, ub_all.at[0], part_sem)
    keep.start()
    ub_v[ALL] = land[ALL].reshape(toks, width).astype(BF16)
    run[0] = jnp.full(run.shape[1:], NEG, F32)
    run[1] = jnp.zeros(run.shape[1:], F32)
    lane = lax.broadcasted_iota(jnp.int32, (toks, VT), 1)

    def start_of(i):
        return pl.multiple_of(jnp.minimum(i * VT, rows - VT), 16)

    def fold(op, v):
        return functools.reduce(op, [v[:, j : j + LANES] for j in range(0, VT, LANES)])

    def forward(i, carry):
        attend(i)

        @pl.when(i < whole)
        def _():
            load(i).wait()

        @pl.when(i == whole)
        def _():
            tail_copy.wait()

        start = start_of(i)
        z = lax.dot_general(ub_v[ALL], table_v[pl.ds(start, VT), :], NT_DIMS, preferred_element_type=F32)
        z = jnp.where(lane >= i * VT - start, z, NEG)
        z_v[i] = z
        run[0] = jnp.maximum(run[0], fold(jnp.maximum, z))
        hit = (lane + start == lab_v[:, 0:1]) & (lane >= i * VT - start)
        run[1] = run[1] + fold(jnp.add, jnp.where(hit, z, 0.0))
        return carry

    repeat(steps, forward)
    top = jnp.max(run[0], axis=1, keepdims=True)
    run[0] = jnp.zeros(run.shape[1:], F32)

    def exps(i, carry):
        run[0] = run[0] + fold(jnp.add, jnp.exp(z_v[i] - top))
        return carry

    repeat(steps, exps)
    total = jnp.sum(run[0], axis=1, keepdims=True)
    label = jnp.sum(run[1], axis=1, keepdims=True)
    narrow = lax.broadcasted_iota(jnp.int32, (toks, LANES), 1)
    packed = jnp.where(narrow == 0, top, jnp.where(narrow == 1, total, jnp.where(narrow == 2, label, 0.0)))
    mine[ALL] = jnp.transpose(packed)[:SUB]
    stat = []
    for i in range(1, NTP):
        stat.append(rdma(mine, theirs.at[i], st_send.at[i], st_recv.at[i], to_tp(rem(at.tp + i, NTP))))
        stat[-1].start()
    theirs[0] = mine[ALL]
    spread.run(middle)
    for copy in stat:
        copy.wait_recv()
    parts = [theirs[rem(at.tp - j + NTP, NTP)] for j in range(NTP)]
    peak = functools.reduce(jnp.maximum, [p[0:1] for p in parts])
    total = functools.reduce(jnp.add, [p[1:2] * jnp.exp(p[0:1] - peak) for p in parts])
    label = functools.reduce(jnp.add, [p[2:3] for p in parts])
    lse = peak + jnp.log(total)
    loss = jnp.sum(jnp.log(total) + peak - label, axis=1, keepdims=True)
    sub = lax.broadcasted_iota(jnp.int32, (SUB, toks), 0)
    row_out[ALL] = jnp.where(sub == 0, lse, jnp.where(sub == 1, labels[ALL].astype(F32), 0.0))
    odd = rem(at.z, 2) == 1
    upper = lax.broadcasted_iota(jnp.int32, tile_out.shape, 1) >= 64
    every = ids[ALL].astype(F32)
    low = []
    for j in range(0, toks, LANES):
        pair = every[:, j : j + LANES]
        low += [pair, jnp.concatenate([pair[:, 64:], pair[:, :64]], axis=1)]
    low = jnp.concatenate(low, axis=0)
    high = jnp.concatenate([low[:, 64:], low[:, :64]], axis=1)
    tile_out[ALL] = jnp.where(upper == odd, jnp.where(odd, high, low), loss)
    tiles[0] = tile_out[ALL]
    rows_sent = []
    for i in range(NY - 1):
        to_y = to_dp(at.dp_of_y(NY - 1 - i))
        rows_sent.append(rdma(row_out, row_in.at[i], row_send.at[i], row_recv.at[i], to_y))
        rows_sent.append(rdma(tile_out, tile_in.at[i], t_send.at[i], t_recv.at[i], to_y))
    for copy in rows_sent:
        copy.start()
    run[0] = jnp.transpose(jnp.broadcast_to(lse, (LANES, toks)))
    inv_total = 1.0 / tok_total

    def put(i):
        half = rem(i, 2)
        return pltpu.make_async_copy(grad_v.at[half], grads.at[i], grad_sem.at[half])

    def backward(i, carry):
        start = start_of(i)
        shift = jnp.concatenate([run[0]] * (VT // LANES), axis=1)
        prob = jnp.exp(z_v[i] - shift)
        hit = (lane + start == lab_v[:, 0:1]) & (lane >= i * VT - start)

        @pl.when(i >= 2)
        def _():
            put(i - 2).wait()

        grad_v[rem(i, 2)] = ((prob - jnp.where(hit, 1.0, 0.0)) * inv_total).astype(BF16)
        put(i).start()
        return carry

    repeat(steps, backward)
    for i in range(max(0, steps - 2), steps):
        put(jnp.int32(i)).wait()
    spread.run(late)
    for e in spread.events:
        if e not in near:
            spread.take(e[0])
    for copy in rows_sent:
        copy.wait_recv()
    stats[0] = row_out[ALL]
    for i in range(NY - 1):
        stats[i + 1] = row_in[i]
        tiles[i + 1] = tile_in[i]
    keep.wait()
    spread.end()
    for copy in stat + rows_sent:
        copy.wait_send()


class SumZ:
    def __init__(self, at, parts, came, total, chunks, send, recv):
        self.at, self.parts, self.came, self.total = at, parts, came, total
        self.chunks, self.send, self.recv = chunks, send, recv
        self.last = at.nz // 2

    def rows(self, c, s, way):
        lo, hi = self.chunks[c]
        if s == 1:
            mid = lo + SUB * pl.cdiv(hi - lo, 16)
            lo, hi = (lo, mid) if way > 0 else (mid, hi)
        return pl.ds(lo, hi - lo)

    def slot(self, s, way):
        return 0 if s == 1 else 2 * (s - 1) - (way > 0)

    def goal(self, s, way):
        return rem(self.at.z + way * (self.last + 1 - s) + self.at.nz, self.at.nz)

    def copy(self, c, s, way):
        rows, w = self.rows(c, s, way), WAYS.index(way)
        sems = self.send.at[w, s, c], self.recv.at[w, s, c]
        src = self.parts.at[self.goal(s, way), rows]
        return rdma(src, self.came.at[self.slot(s, way), rows], *sems, to_dp(self.at.dp_of_z(way)))

    def begin(self, c):
        rows = pl.ds(self.chunks[c][0], self.chunks[c][1] - self.chunks[c][0])
        self.total[rows] = self.parts[self.at.z, rows]
        for way in WAYS:
            self.copy(c, 1, way).start()

    def run(self, c, s):
        for way in WAYS:
            self.copy(c, s, way).wait_recv()
            rows, slot = self.rows(c, s, way), self.slot(s, way)
            if s < self.last:
                goal = self.goal(s + 1, way)
                self.parts[goal, rows] = self.parts[goal, rows] + self.came[slot, rows]
                self.copy(c, s + 1, way).start()
            else:
                self.total[rows] = self.total[rows] + self.came[slot, rows]

    def end(self):
        for c in range(len(self.chunks)):
            for s in range(self.last):
                for way in WAYS:
                    self.copy(c, s + 1, way).wait_send()


def finish_kernel(
    nz, stride, vocab_loc, tok_total, row_plan, dh_plan, table_plan, chunks,
    table, ub, stats, grads, u, r, tiles,
    d_trunk, loss, stack, all_dh,
    pb, rl, fin, land, all_tiles, table_v, ub_v, grad_v, parts, came, total, dh_v, du, rows_v, logit_v,
    rs_send, rs_recv, row_send, row_recv, z_send, z_recv, i_send, i_recv, x_send, x_recv, s_send, s_recv, t_send, t_recv,
    load_sem, stage_sem, dh_sem, rows_sem, logit_sem,
):
    at = Place(nz)
    own, width = u.shape
    win, cols = total.shape
    toks = stats.shape[2]
    block = nz * own
    slab = LANES
    first = pl.multiple_of(at.y * stride, 16)
    loads = [
        pltpu.make_async_copy(table.at[pl.ds(first + lo, hi - lo)], table_v.at[lo:hi], copy_sem)
        for (lo, hi), copy_sem in zip(chunks, (load_sem, dh_sem.at[0], dh_sem.at[1]))
    ]

    depth, per = 4, toks // slab
    slabs = NY * per

    def staged(slot):
        return du.at[pl.ds(pl.multiple_of(slot * slab, slab), slab)]

    def fill(i):
        rows = pl.ds(pl.multiple_of(rem(i, per) * slab, slab), slab)
        slot = rem(i, depth)
        return pltpu.make_async_copy(ub.at[lax.div(i, jnp.int32(per)), rows], staged(slot), stage_sem.at[slot])

    loads[0].start()
    for i in range(depth):
        fill(jnp.int32(i)).start()
    steps = grads.shape[0]

    def start_of(i):
        return pl.multiple_of(jnp.minimum(i * VT, vocab_loc - VT), 16)

    def bring(i):
        half = rem(i, 2)
        return [
            pltpu.make_async_copy(table.at[pl.ds(start_of(i), VT)], rows_v.at[half], rows_sem.at[half]),
            pltpu.make_async_copy(grads.at[i], logit_v.at[half], logit_sem.at[half]),
        ]

    for copy in loads[1:] + bring(jnp.int32(0)):
        copy.start()
    met_all = greet(
        [to_tp(rem(at.tp + i, NTP)) for i in range(1, NTP)]
        + [to_dp(at.dp_of_z(i)) for i in range(1, nz)]
        + [to_dp(at.dp_of_y(way)) for way in WAYS]
    )
    sum_tp = SumTp(at, du, own, pb, rl, fin, rs_send, rs_recv)

    def narrow(n):
        def body(k, carry):
            i = n * per + k
            fill(i).wait()
            ub_v[pl.ds(pl.multiple_of(i * slab, slab), slab)] = staged(rem(i, depth))[ALL].astype(BF16)

            @pl.when(i + depth < slabs)
            def _():
                fill(i + depth).start()

            return carry

        repeat(per, body)

    loads[0].wait()
    narrow(0)

    inv_total = 1.0 / tok_total

    def logits(lo, hi, ahead=lambda n: None):
        vocab = at.tp * vocab_loc + first + lo + lax.broadcasted_iota(jnp.int32, (hi - lo, toks), 0)

        def body(n, carry):
            ahead(n)
            cut = pl.ds(pl.multiple_of(n * toks, LANES), toks)
            z = lax.dot_general(table_v[lo:hi, :], ub_v[cut, :], NT_DIMS, preferred_element_type=F32)
            row = stats[n]
            prob = jnp.exp(z - row[0:1])
            hit = vocab == row[1:2].astype(jnp.int32)
            grad_v[0 : hi - lo, cut] = ((prob - jnp.where(hit, 1.0, 0.0)) * inv_total).astype(BF16)
            return carry

        repeat(NY, body)

    def head(lo, hi):
        def body(n, carry):
            cut = pl.ds(pl.multiple_of(n * cols, LANES), cols)
            parts[n, lo:hi] = jnp.dot(grad_v[0 : hi - lo, :], ub_v[:, cut], preferred_element_type=F32)
            return carry

        repeat(nz, body)

    sums = SumZ(at, parts, came, total, chunks, s_send, s_recv)

    def sum_step(c, k):
        if k <= sums.last:
            sums.run(c, k)

    def narrow_next(n):
        @pl.when(n + 1 < NY)
        def _():
            narrow(n + 1)

    logits(*chunks[0], narrow_next)
    head(*chunks[0])
    met_all()
    sums.begin(0)
    known = [
        rdma(tiles, all_tiles.at[at.z], i_send.at[i], i_recv.at[i], to_dp(at.dp_of_z(i))) for i in range(1, nz)
    ]
    for copy in known:
        copy.start()
    all_tiles[at.z] = tiles[ALL]
    wide = min(512, width)
    du[ALL] = jnp.zeros(du.shape, F32)

    def backward(i, carry):
        for copy in bring(i):
            copy.wait()

        @pl.when(i + 1 < steps)
        def _():
            for copy in bring(i + 1):
                copy.start()

        @pl.when(i == min(5, steps - 1))
        def _():
            sum_step(0, 1)

        half = rem(i, 2)
        for n in range(width // wide):
            cut = pl.ds(n * wide, wide)
            du[:, cut] = du[:, cut] + jnp.dot(logit_v[half], rows_v[half, :, cut], preferred_element_type=F32)
        return carry

    repeat(steps, backward)
    sum_tp.begin()
    sum_step(0, 2)
    for copy in loads[1:]:
        copy.wait()
    logits(*chunks[1])
    sum_tp.pass_on()
    head(*chunks[1])
    sums.begin(1)
    sum_tp.join()
    sum_step(0, 3)
    logits(*chunks[2])
    head(*chunks[2])
    grad = sum_tp.result()
    normed = u[ALL]
    mean_g = jnp.mean(grad, axis=-1, keepdims=True)
    mean_gu = jnp.mean(grad * normed, axis=-1, keepdims=True)
    land[at.tp] = r[:, 0:1] * (grad - mean_g - normed * mean_gu)

    def row_block(dx, dy, cross, lo, hi):
        return land.at[at.tp_of(dx, cross), pl.ds(lo, hi - lo)]

    whole_rows = Spread(at, row_plan, own, row_block, row_send, row_recv)
    whole_rows.begin()
    here = pl.ds(pl.multiple_of(at.z * own, own), own)
    turned = []
    for i in range(1, nz):
        col, to_z = pl.multiple_of(rem(at.z + i, nz) * cols, LANES), to_dp(at.dp_of_z(i))
        src = land.at[at.tp, :, pl.ds(col, cols)]
        turned.append(rdma(src, all_dh.at[at.tp, 0, here], z_send.at[i], z_recv.at[i], to_z))
    for copy in turned:
        copy.start()
    my_col = pl.multiple_of(at.z * cols, LANES)
    mine = pltpu.make_async_copy(land.at[at.tp, :, pl.ds(my_col, cols)], all_dh.at[at.tp, 0, here], load_sem)
    mine.start()
    sums.begin(2)
    sum_step(1, 1)
    sum_step(0, 4)
    whole_rows.run(whole_rows.events)
    mine.wait()
    for copy in turned + known:
        copy.wait_recv()

    def dh_block(dx, dy, cross, lo, hi):
        return all_dh.at[at.tp_of(dx, cross), dy % NY, pl.ds(lo, hi - lo)]

    blocks = Spread(at, dh_plan, block, dh_block, x_send, x_recv)
    blocks.begin()

    pieces = {(0, 0): [(blocks.count, [], 0)]}
    for e in blocks.events:
        dx, dy = blocks.goal(e[0])
        pieces.setdefault((dx % NX, dy % NY), []).append(e)
    order = sorted((pieces[p][-1][-1] + cross * (block // 3), *p, cross) for p in pieces for cross in range(2))
    left = list(blocks.events)
    due = []
    for time, dx, dy, cross in order:
        due.append([e for e in left if e[-1] <= time])
        left = [e for e in left if e[-1] > time]
    code = [dx + NX * (dy + NY * cross) for _, dx, dy, cross in order]
    ready = 2

    def meet(k):
        blocks.run(due[k])
        _, dx, dy, cross = order[k]
        if cross:
            for part in pieces[dx, dy]:
                blocks.take(part[0])

    for k in range(ready):
        meet(k)
    for i in range(whole_rows.count + 1):
        whole_rows.take(i)
    ub_v[0:toks] = land[ALL].reshape(toks, width).astype(BF16)
    keep_rows = pltpu.make_async_copy(ub_v.at[0:toks], d_trunk, rows_sem.at[0])
    keep_rows.start()
    upper = lax.broadcasted_iota(jnp.int32, loss.shape, 1) >= 64
    loss[ALL] = sum(
        jnp.where(upper == (z % 2 == 0), all_tiles[z, rem(y - at.y + NY, NY)], 0.0) for z in range(nz) for y in range(NY)
    )

    beside = {k: (c, step) for k, c, step in BESIDE if step <= sums.last}
    low = (at.tp * vocab_loc + at.y * stride).astype(F32)

    def place_of(e):
        mark = jnp.int32(code[0])
        for k in range(1, len(order)):
            mark = jnp.where(e == k, code[k], mark)
        core = jnp.where(mark >= NX * NY, 1 - at.c, at.c)
        return 2 * rem(at.x + rem(mark, NX), NX) + core, rem(lax.div(mark, jnp.int32(NX)), NY)

    def fetch(e):
        tp, far = place_of(e)
        half = rem(e, 2)
        return pltpu.make_async_copy(all_dh.at[tp, far], dh_v.at[half], dh_sem.at[half])

    def piece(e, carry):
        for k in range(len(order)):
            met = k + 1 if k + 1 < len(order) and k + 1 >= ready else 0
            if k in beside or met:

                @pl.when(e == k)
                def _(k=k, met=met):
                    if k in beside:
                        sums.run(*beside[k])
                    if met:
                        meet(met)

        @pl.when(e + 1 < len(order))
        def _():
            fetch(e + 1).start()

        tp, far = place_of(e)
        ids = jnp.concatenate(
            [
                jnp.where(upper[0:1], all_tiles[2 * j + 1, far, pl.ds(tp, 1), :], all_tiles[2 * j, far, pl.ds(tp, 1), :])
                for j in range(nz // 2)
            ],
            axis=1,
        )
        fetch(e).wait()
        dh = dh_v[rem(e, 2)]
        hi = dh.astype(BF16)
        rest = dh - hi.astype(F32)
        mid = rest.astype(BF16)
        lo = (rest - mid.astype(F32)).astype(BF16)
        ids = (ids - low).astype(jnp.int32)
        for begin, end in chunks:
            row = lax.broadcasted_iota(jnp.int32, (end - begin, block), 0) + begin
            pick = jnp.where(row == ids, 1.0, 0.0).astype(BF16)
            found = sum(jnp.dot(pick, term, preferred_element_type=F32) for term in (hi, mid, lo))
            total[begin:end] = total[begin:end] + found
        return carry

    fetch(jnp.int32(0)).start()
    repeat(len(order), piece)
    for copy in turned + known:
        copy.wait_send()

    sends, starts, events = table_plan
    device = {(0, way): to_dp(at.dp_of_z(way)) for way in WAYS} | {(1, way): to_dp(at.dp_of_y(way)) for way in WAYS}

    def copy_of(i, arrives=False):
        axis, way, off, lo, hi = sends[i]
        if arrives:
            off = tuple(o - way * (a == axis) for a, o in enumerate(off))
        dst = stack.at[rem(at.z + off[0] + nz, nz), at.y_of(off[1]), pl.ds(lo, hi - lo)]
        src = dst if any(off) else total.at[pl.ds(lo, hi - lo)]
        return rdma(src, dst, t_send.at[i], t_recv.at[i], device[axis, way])

    for c in range(1, len(chunks)):
        sum_step(c, 4)
    for i in sum(starts, []):
        copy_of(i).start()
    keep = pltpu.make_async_copy(total, stack.at[at.z, at.y], load_sem)
    keep.start()
    for i, new, _ in events:
        copy_of(i, True).wait_recv()
        for j in new:
            copy_of(j).start()
    keep.wait()
    keep_rows.wait()
    for i in range(len(sends)):
        copy_of(i).wait_send()
    sums.end()
    whole_rows.end()
    blocks.end()


def pick_kernel(ids_s, table, ids, out, eights, local, sem):
    toks = out.shape[0]
    rows = table.shape[0]
    begin = lax.axis_index("tp") * rows
    block = 32

    def fetch(t, carry):
        row = ids_s[0, t] - begin
        eight = pl.multiple_of(jnp.where((row >= 0) & (row < rows), lax.div(row, jnp.int32(SUB)), t) * SUB, SUB)
        mine = eights.at[pl.ds(pl.multiple_of(t * SUB, SUB), SUB)]
        pltpu.make_async_copy(table.at[pl.ds(eight, SUB)], mine, sem.at[lax.div(t, jnp.int32(part))]).start()
        return carry

    part = toks // sem.shape[0]
    lax.fori_loop(0, toks, fetch, 0, unroll=SUB)
    local[ALL] = columns(ids[ALL]) - begin
    lane = lax.broadcasted_iota(jnp.int32, (block, SUB * block), 1)
    first = SUB * lax.broadcasted_iota(jnp.int32, (block, SUB * block), 0)

    def choose(b, carry):
        at = pl.multiple_of(b * block, block)
        row = local[pl.ds(at, block), 0:1]
        hit = (lane - first == rem(row, SUB)) & (row >= 0) & (row < rows)
        some = eights[pl.ds(pl.multiple_of(at * SUB, SUB), SUB * block), :]
        out[pl.ds(at, block)] = jnp.dot(
            jnp.where(hit, 1.0, 0.0).astype(BF16), some, preferred_element_type=F32
        ).astype(BF16)
        return carry

    for q in range(sem.shape[0]):
        whole = pl.ds(q * part * SUB, part * SUB)
        pltpu.make_async_copy(table.at[pl.ds(0, part * SUB)], eights.at[whole], sem.at[q]).wait()
        lax.fori_loop(q * part // block, (q + 1) * part // block, choose, 0)


def place_kernel(chunk, tok_total, stack, rows_in, loss_in, out, rows_out, loss_out, slots, rows_v, rest_v, load_sem, store_sem, rows_sem, rest_sem):
    nz, ny, have, cols = stack.shape
    depth = slots.shape[0]
    per = have // chunk
    total = ny * per
    ahead = depth // 2

    def loads(i):
        y, row = lax.div(i, jnp.int32(per)), pl.multiple_of(rem(i, per) * chunk, SUB)
        s = rem(i, depth)
        return [
            pltpu.make_async_copy(
                stack.at[j, y, pl.ds(row, chunk)], slots.at[s, :, pl.ds(j * cols, cols)], load_sem.at[s, j]
            )
            for j in range(nz)
        ]

    def store(i):
        s, row = rem(i, depth), pl.multiple_of(i * chunk, SUB)
        return pltpu.make_async_copy(slots.at[s], out.at[pl.ds(row, chunk)], store_sem.at[s])

    rows_load = pltpu.make_async_copy(rows_in, rows_v, rows_sem)
    rows_store = pltpu.make_async_copy(rows_v, rows_out, rows_sem)
    used = per * chunk
    left = have - used
    rest = pltpu.make_async_copy(stack.at[:, ny - 1, pl.ds(used, left)], rest_v, rest_sem.at[0])
    tails = [
        pltpu.make_async_copy(rest_v.at[j], out.at[pl.ds(ny * used, left), pl.ds(j * cols, cols)], rest_sem.at[j])
        for j in range(nz)
    ]

    def prime(i, carry):
        for copy in loads(i):
            copy.start()
        return carry

    def body(i, carry):
        for copy in loads(i):
            copy.wait()
        store(i).start()

        @pl.when(i == ahead)
        def _():
            rows_load.wait()
            rows_store.start()
            rest.wait()
            for copy in tails:
                copy.start()

        @pl.when(i + ahead < total)
        def _():
            @pl.when(i >= ahead)
            def _():
                store(i - ahead).wait()

            for copy in loads(i + ahead):
                copy.start()

        return carry

    def drain(i, carry):
        store(i).wait()
        return carry

    repeat(ahead, prime)
    rows_load.start()
    rest.start()
    lane = lax.broadcasted_iota(jnp.int32, (1, LANES), 1)
    loss_out[0, 0] = jnp.sum(jnp.where(rem(lane, 64) == 0, loss_in[0:1], 0.0)) / tok_total
    repeat(total, body)
    lax.fori_loop(total - 2 * ahead, total, drain, 0)
    for copy in tails:
        copy.wait()
    rows_store.wait()


def vmem():
    return pl.BlockSpec(memory_space=pltpu.VMEM)


def anywhere():
    return pl.BlockSpec(memory_space=pl.ANY)


def dma(*shape):
    return pltpu.SemaphoreType.DMA(shape)


def twice(*shape):
    return [dma(*shape)] * 2


def solution(mesh):
    ndp, ntp = mesh.shape["dp"], mesh.shape["tp"]
    nz = ndp // NY

    def per_device(table, ids, labels, trunk):
        vocab_loc, width = table.shape
        batch, seq = ids.shape
        toks = batch * seq
        own = toks // NTP
        tok_total = toks * ndp
        stride = (vocab_loc - 16) // NY
        win = stride + 16
        cols = width // nz
        block = nz * own
        big = 66_000_000
        tp_sems = twice(10)
        tp_scratch = [
            pltpu.VMEM((4, own, width), F32),
            pltpu.VMEM((2, own // 2, width), F32),
            pltpu.VMEM((4, own // 2, width), F32),
            pltpu.VMEM((NTP, own, width), F32),
        ]
        ids, labels = ids.reshape(1, toks), labels.reshape(1, toks)
        part = pl.pallas_call(
            pick_kernel,
            out_shape=jax.ShapeDtypeStruct((toks, width), BF16),
            in_specs=[pl.BlockSpec(memory_space=pltpu.SMEM), anywhere(), vmem()],
            out_specs=vmem(),
            scratch_shapes=[pltpu.VMEM((SUB * toks, width), BF16), pltpu.VMEM((toks, LANES), jnp.int32), dma(SUB)],
            compiler_params=pltpu.CompilerParams(vmem_limit_bytes=big),
            name="pick",
        )(ids, table, ids)
        steps = pl.cdiv(vocab_loc, VT)
        token_plan = gather_plan((NX, NY), two_colours(0, own, 0.5), 16, hold=2 * own)
        sends = 2 * len(token_plan[0]) + 1
        grads, ub, u_own, r_own, stats, tiles = pl.pallas_call(
            functools.partial(token_kernel, nz, tok_total, token_plan),
            out_shape=(
                jax.ShapeDtypeStruct((steps, toks, VT), BF16),
                jax.ShapeDtypeStruct((NY, NTP, own, width), F32),
                jax.ShapeDtypeStruct((own, width), F32),
                jax.ShapeDtypeStruct((own, LANES), F32),
                jax.ShapeDtypeStruct((NY, SUB, toks), F32),
                jax.ShapeDtypeStruct((NY, SUB, LANES), F32),
            ),
            in_specs=[anywhere(), anywhere(), anywhere(), vmem(), vmem()],
            out_specs=(anywhere(), anywhere(), vmem(), vmem(), vmem(), vmem()),
            scratch_shapes=[
                pltpu.VMEM((toks, LANES), jnp.int32),
                pltpu.VMEM((toks, width), F32),
                pltpu.VMEM((own, width), BF16),
                pltpu.VMEM((2, toks, VT), BF16),
                pltpu.VMEM((vocab_loc, width), BF16),
                pltpu.VMEM((toks, width), BF16),
                pltpu.VMEM((steps, toks, VT), F32),
                pltpu.VMEM((2, toks, LANES), F32),
                pltpu.VMEM((SUB, toks), F32),
                pltpu.VMEM((NTP, SUB, toks), F32),
                pltpu.VMEM((SUB, toks), F32),
                pltpu.VMEM((NY - 1, SUB, toks), F32),
                pltpu.VMEM((SUB, LANES), F32),
                pltpu.VMEM((NY - 1, SUB, LANES), F32),
                *tp_scratch,
                dma(steps), pltpu.SemaphoreType.DMA, *twice(NTP), *twice(NY - 1), *twice(NY - 1), *tp_sems, *twice(sends), dma(2),
            ],
            compiler_params=pltpu.CompilerParams(collective_id=0, has_side_effects=True, vmem_limit_bytes=big),
            name="token",
        )(table, part, trunk.reshape(toks, width), labels, ids)

        row_plan = gather_plan((NX, 1), two_colours(0, own, 1), 16)
        dh_plan = gather_plan((NX, NY), two_colours(0, block, 0.5), block // 4)
        lead = 16 * pl.cdiv(win, 48)
        middle = 2 * lead
        chunks = ((0, lead), (lead, middle), (middle, win))
        third = SUB * pl.cdiv(win, 24)
        table_chunks = ((0, third), (third, 2 * third), (2 * third, win))
        shares = SHARES if nz == SUB else (0.5,) * 3
        table_parts = sum((two_colours(lo, hi, share) for (lo, hi), share in zip(table_chunks, shares)), [])
        table_plan = gather_plan((nz, NY), table_parts, 60)
        counts = [2 * len(p[0]) + 1 for p in (row_plan, dh_plan, table_plan)]
        zs = (2, nz // 2 + 1, len(chunks))
        d_rows, loss, stack, _ = pl.pallas_call(
            functools.partial(
                finish_kernel, nz, stride, vocab_loc, tok_total, row_plan, dh_plan, table_plan, chunks
            ),
            out_shape=(
                jax.ShapeDtypeStruct((toks, width), BF16),
                jax.ShapeDtypeStruct((SUB, LANES), F32),
                jax.ShapeDtypeStruct((nz, NY, win, cols), F32),
                jax.ShapeDtypeStruct((NTP, NY, block, cols), F32),
            ),
            in_specs=[anywhere(), anywhere(), vmem(), anywhere(), vmem(), vmem(), vmem()],
            out_specs=(anywhere(), vmem(), anywhere(), anywhere()),
            scratch_shapes=[
                *tp_scratch,
                pltpu.VMEM((nz, NY, SUB, LANES), F32),
                pltpu.VMEM((win, width), BF16),
                pltpu.VMEM((NY * toks, width), BF16),
                pltpu.VMEM((middle - lead, NY * toks), BF16),
                pltpu.VMEM((nz, win, cols), F32),
                pltpu.VMEM((nz - 1, win, cols), F32),
                pltpu.VMEM((win, cols), F32),
                pltpu.VMEM((2, block, cols), F32),
                pltpu.VMEM((toks, width), F32),
                pltpu.VMEM((2, VT, width), BF16),
                pltpu.VMEM((2, toks, VT), BF16),
                *tp_sems, *twice(counts[0]), *twice(nz), *twice(nz), *twice(counts[1]), *twice(*zs), *twice(counts[2]),
                pltpu.SemaphoreType.DMA, dma(4), *twice(2), dma(2),
            ],
            compiler_params=pltpu.CompilerParams(collective_id=1, has_side_effects=True, vmem_limit_bytes=67_000_000),
            name="finish",
        )(table, ub.reshape(NY, toks, width), stats, grads, u_own, r_own, tiles)
        depth = 16 if nz == SUB else SUB
        chunk = next(n for n in range(112, 0, -SUB) if stride % n == 0 and NY * stride >= n * depth)
        d_table, d_rows, mean_loss = pl.pallas_call(
            functools.partial(place_kernel, chunk, tok_total),
            out_shape=(
                jax.ShapeDtypeStruct((vocab_loc, width), F32),
                jax.ShapeDtypeStruct((toks, width), BF16),
                jax.ShapeDtypeStruct((1, 1), F32),
            ),
            in_specs=[anywhere(), anywhere(), vmem()],
            out_specs=(anywhere(), anywhere(), pl.BlockSpec(memory_space=pltpu.SMEM)),
            scratch_shapes=[
                pltpu.VMEM((depth, chunk, width), F32), pltpu.VMEM((toks, width), BF16),
                pltpu.VMEM((nz, win - stride, cols), F32), dma(depth, nz), dma(depth), pltpu.SemaphoreType.DMA, dma(nz),
            ],
            compiler_params=pltpu.CompilerParams(vmem_limit_bytes=big),
            name="place",
        )(stack, d_rows, loss)
        return mean_loss.reshape(()), d_rows.reshape(trunk.shape), d_table

    return jax.shard_map(
        per_device,
        mesh=mesh,
        in_specs=(P("tp", None), P("dp", None), P("dp", None), P("dp", None, None)),
        out_specs=(P(), P("dp", None, None), P("tp", None)),
        check_vma=False,
    )
```

```python
import functools
import heapq

import jax
import jax.numpy as jnp
from jax import lax
from jax.experimental import pallas as pl
from jax.experimental.pallas import tpu as pltpu
from jax.sharding import PartitionSpec as P

LN_EPS = 1e-5
MESH = pl.DeviceIdType.MESH
F32, BF16 = jnp.float32, jnp.bfloat16
NY, NTP, NX = 4, 8, 4
WAYS = (1, -1)
SUB = 8
AHEAD = 3
LANES = 128
BESIDE = ((0, 2, 1), (6, 1, 2), (13, 2, 2), (20, 1, 3), (26, 2, 3))
SHARES = (0.55, 0.55, 0.7)
ALL = Ellipsis
NEG = float(jnp.finfo(jnp.float32).min)
VT = 512
NT_DIMS = (((1,), (1,)), ((), ()))
NN_DIMS = (((1,), (0,)), ((), ()))


def rem(a, b):
    return lax.rem(a, jnp.int32(b))


class Place:
    def __init__(self, nz):
        self.nz = nz
        self.dp = lax.axis_index("dp")
        self.tp = lax.axis_index("tp")
        self.z, self.y = lax.div(self.dp, jnp.int32(NY)), rem(self.dp, NY)
        self.x, self.c = lax.div(self.tp, jnp.int32(2)), rem(self.tp, 2)
        self.partner = 2 * self.x + (1 - self.c)

    def tp_of(self, step, other=False):
        c = 1 - self.c if other else self.c
        return 2 * rem(self.x + step + NX, NX) + c

    def y_of(self, step):
        return rem(self.y + step + NY, NY)

    def dp_of_y(self, step):
        return self.z * NY + self.y_of(step)

    def dp_of_z(self, step):
        return rem(self.z + step + self.nz, self.nz) * NY + self.y


def repeat(count, body):
    lax.fori_loop(0, count, body, 0)


def to_tp(tp):
    return {"tp": tp}


def to_dp(dp):
    return {"dp": dp}


def rdma(src, dst, send_sem, recv_sem, device):
    return pltpu.make_async_remote_copy(
        src_ref=src, dst_ref=dst, send_sem=send_sem, recv_sem=recv_sem, device_id=device, device_id_type=MESH
    )


def greet(devices):
    barrier = pltpu.get_barrier_semaphore()
    for device in devices:
        pl.semaphore_signal(barrier, inc=1, device_id=device, device_id_type=MESH)
    return lambda: pl.semaphore_wait(barrier, len(devices))


class SumTp:
    def __init__(self, at, src, own, pb, rl, fin, send, recv):
        self.src, self.own, self.half, self.pb, self.rl, self.fin = src, own, own // 2, pb, rl, fin
        self.at, self.send, self.recv = at, send, recv
        self.steps = (2, 1, -1, 0)
        self.copies = []

    def copy(self, i, src, dst, tp):
        self.copies.append(rdma(src, dst, self.send.at[i], self.recv.at[i], to_tp(tp)))
        return self.copies[-1]

    def rows(self, step, other):
        return pl.ds(pl.multiple_of(self.at.tp_of(step, other) * self.own, self.own), self.own)

    def part(self, i, h):
        return self.pb.at[i, pl.ds(h * self.half, self.half)]

    def begin(self):
        for i, step in enumerate(self.steps):
            self.copy(i, self.src.at[self.rows(step, True)], self.pb.at[i], self.at.partner).start()

    def merge(self, i):
        self.copies[i].wait_recv()
        self.pb[i] = self.pb[i] + self.src[self.rows(self.steps[i], False), :]

    def pass_on(self):
        plus, minus = self.at.tp_of(1), self.at.tp_of(-1)
        self.merge(0)
        for h, tp in enumerate((plus, minus)):
            self.copy(4 + h, self.part(0, h), self.rl.at[h], tp).start()
        self.merge(1)
        self.merge(2)
        self.copy(6, self.part(1, 1), self.fin.at[0], plus).start()
        self.copy(7, self.part(2, 0), self.fin.at[1], minus).start()

    def join(self):
        for h, tp in enumerate((self.at.tp_of(1), self.at.tp_of(-1))):
            self.copies[4 + h].wait_recv()
            rows = pl.ds(h * self.half, self.half)
            self.pb[1 + h, rows] = self.pb[1 + h, rows] + self.rl[h]
            self.copy(SUB + h, self.part(1 + h, h), self.fin.at[2 + h], tp).start()
        self.merge(3)

    def result(self):
        for copy in self.copies[6:]:
            copy.wait_recv()
        top = self.pb[3, 0 : self.half] + self.fin[2] + self.fin[1]
        low = self.pb[3, self.half : self.own] + self.fin[0] + self.fin[3]
        for copy in self.copies:
            copy.wait_send()
        return jnp.concatenate([top, low], axis=0)


def gather_plan(sizes, parts, latency, hold=0):
    sends, events, heap, busy = [], [], [], {}

    def post(axis, way, off, lo, hi, order, now):
        end = max(now, busy.get((axis, way), now)) + hi - lo
        busy[axis, way] = end
        there = tuple(o - way * (a == axis) for a, o in enumerate(off))
        heapq.heappush(heap, (end + latency, len(sends), there, lo, hi, order))
        sends.append((axis, way, off, lo, hi))
        return len(sends) - 1

    def ring(axis, way, off, lo, hi, order, now):
        last = sizes[axis] // 2
        gone = abs(off[axis]) + 1
        if gone > last:
            return []
        if gone == last:
            mid = lo + SUB * pl.cdiv(hi - lo, 16)
            lo, hi = (lo, mid) if way > 0 else (mid, hi)
        return [] if lo == hi else [post(axis, way, off, lo, hi, order, now)]

    starts = [[] for _ in parts]
    for leg in range(2):
        for begin, (lo, hi, order, now) in zip(starts, parts):
            for way in WAYS:
                begin += ring(order[leg], way, (0, 0), lo, hi, order, now)
    while heap:
        now, i, off, lo, hi, order = heapq.heappop(heap)
        axis, way = sends[i][:2]
        if off[1] and now < hold:
            heapq.heappush(heap, (hold, i, off, lo, hi, order))
            continue
        new = ring(axis, way, off, lo, hi, order, now)
        if axis == order[0]:
            for w in WAYS:
                new += ring(order[1], w, off, lo, hi, order, now)
        events.append((i, new, now))
    return sends, starts, events


def two_colours(lo, hi, share, now=0):
    split = lo + SUB * round((hi - lo) * share / SUB)
    return [(lo, split, (0, 1), now), (split, hi, (1, 0), now)]


class Spread:
    def __init__(self, at, plan, rows, block, send, recv):
        self.sends, self.starts, self.events = plan
        self.block, self.send, self.recv, self.rows = block, send, recv, rows
        self.count = len(self.sends)
        self.other = to_tp(at.partner)
        self.device = {}
        for way in WAYS:
            self.device[0, way] = to_tp(at.tp_of(way))
            self.device[1, way] = to_dp(at.dp_of_y(way))

    def goal(self, i):
        axis, way, off = self.sends[i][:3]
        return tuple(o - way * (a == axis) for a, o in enumerate(off))

    def copy(self, i):
        axis, way, off, lo, hi = self.sends[i]
        src, dst = self.block(*off, False, lo, hi), self.block(off[0], self.goal(i)[1], False, lo, hi)
        return rdma(src, dst, self.send.at[i], self.recv.at[i], self.device[axis, way])

    def forward(self, i, cross=False):
        off, (lo, hi) = ((0, 0), (0, self.rows)) if i == self.count else (self.goal(i), self.sends[i][-2:])
        ref = self.block(*off, cross, lo, hi)
        return rdma(ref, ref, self.send.at[self.count + i], self.recv.at[self.count + i], self.other)

    def begin(self):
        for i in sum(self.starts, []):
            self.copy(i).start()
        self.forward(self.count).start()

    def run(self, events):
        for i, new, _ in events:
            ref = self.block(*self.goal(i), False, *self.sends[i][-2:])
            rdma(ref, ref, self.send.at[i], self.recv.at[i], self.other).wait_recv()
            for j in new:
                self.copy(j).start()
            self.forward(i).start()

    def take(self, i):
        self.forward(i, True).wait_recv()

    def end(self):
        for i in range(self.count):
            self.copy(i).wait_send()
        for i in range(self.count + 1):
            self.forward(i).wait_send()


def columns(row):
    return jnp.transpose(jnp.broadcast_to(row.astype(F32), (LANES, row.shape[1]))).astype(jnp.int32)


def token_kernel(
    nz, tok_total, plan, table, part, trunk, labels, ids,
    grads, ub_all, u_out, r_out, stats, tiles,
    lab_v, du, trunk_v, grad_v, table_v, ub_v, z_v, run, mine, theirs, row_out, row_in, tile_out, tile_in, pb, rl, fin, land,
    load_sem, part_sem, st_send, st_recv, row_send, row_recv, t_send, t_recv, rs_send, rs_recv, x_send, x_recv,
    grad_sem,
):
    at = Place(nz)
    rows, width = table_v.shape
    toks = ub_v.shape[0]
    own = trunk_v.shape[0]
    steps = z_v.shape[0]
    whole = rows // VT
    tail = rows - whole * VT

    part_copy = pltpu.make_async_copy(part, ub_v, part_sem)
    part_copy.start()
    trunk_copy = pltpu.make_async_copy(trunk.at[pl.ds(pl.multiple_of(at.tp * own, own), own)], trunk_v, grad_sem.at[0])
    trunk_copy.start()

    def load(i):
        start = pl.multiple_of(i * VT, 16)
        return pltpu.make_async_copy(table.at[pl.ds(start, VT)], table_v.at[pl.ds(start, VT)], load_sem.at[i])

    tail_copy = pltpu.make_async_copy(
        table.at[pl.ds(whole * VT, tail)], table_v.at[pl.ds(whole * VT, tail)], load_sem.at[whole]
    )
    met_all = greet([to_tp(rem(at.tp + i, NTP)) for i in range(1, NTP)] + [to_dp(at.dp_of_y(i)) for i in range(1, NY)])
    lab_v[ALL] = columns(labels[ALL]) - at.tp * rows
    part_copy.wait()
    for i in range(whole):
        load(i).start()
    tail_copy.start()
    du[ALL] = ub_v[ALL].astype(F32)
    sums = SumTp(at, du, own, pb, rl, fin, rs_send, rs_recv)
    met_all()
    sums.begin()
    sums.pass_on()
    sums.join()
    trunk_copy.wait()
    hidden = sums.result() + trunk_v[ALL].astype(F32)
    centered = hidden - jnp.mean(hidden, axis=-1, keepdims=True)
    inv_std = lax.rsqrt(jnp.mean(centered * centered, axis=-1, keepdims=True) + LN_EPS)
    normed = centered * inv_std
    land[at.tp] = normed.astype(BF16).astype(F32)

    def block(dx, dy, cross, lo, hi):
        tp, cut = at.tp_of(dx, cross), pl.ds(lo, hi - lo)
        return ub_all.at[dy % NY, tp, cut] if dy % NY else land.at[tp, cut]

    spread = Spread(at, plan, own, block, x_send, x_recv)
    spread.begin()
    u_out[ALL] = normed
    r_out[ALL] = jnp.broadcast_to(inv_std, r_out.shape)
    near = [e for e in spread.events if spread.goal(e[0])[1] == 0]
    spread.run(near)
    for e in near:
        spread.take(e[0])
    spread.take(spread.count)
    groups = {}
    pace = own / 7.5
    for e in [e for e in spread.events if e not in near]:
        due = max(0, int((e[-1] - near[-1][-1]) / pace)) + 2
        groups.setdefault(due, []).append(e)
    middle, late = ([e for due in sorted(groups) if (due >= steps) and (due < steps + 6) == m for e in groups[due]] for m in (True, False))

    def attend(step):
        for due, events in groups.items():
            if due < steps:

                @pl.when(step == due)
                def _(events=events):
                    spread.run(events)

    keep = pltpu.make_async_copy(land, ub_all.at[0], part_sem)
    keep.start()
    ub_v[ALL] = land[ALL].reshape(toks, width).astype(BF16)
    run[0] = jnp.full(run.shape[1:], NEG, F32)
    run[1] = jnp.zeros(run.shape[1:], F32)
    lane = lax.broadcasted_iota(jnp.int32, (toks, VT), 1)

    def start_of(i):
        return pl.multiple_of(jnp.minimum(i * VT, rows - VT), 16)

    def fold(op, v):
        return functools.reduce(op, [v[:, j : j + LANES] for j in range(0, VT, LANES)])

    def forward(i, carry):
        attend(i)

        @pl.when(i < whole)
        def _():
            load(i).wait()

        @pl.when(i == whole)
        def _():
            tail_copy.wait()

        start = start_of(i)
        z = lax.dot_general(ub_v[ALL], table_v[pl.ds(start, VT), :], NT_DIMS, preferred_element_type=F32)
        z = jnp.where(lane >= i * VT - start, z, NEG)
        z_v[i] = z
        run[0] = jnp.maximum(run[0], fold(jnp.maximum, z))
        hit = (lane + start == lab_v[:, 0:1]) & (lane >= i * VT - start)
        run[1] = run[1] + fold(jnp.add, jnp.where(hit, z, 0.0))
        return carry

    repeat(steps, forward)
    top = jnp.max(run[0], axis=1, keepdims=True)
    run[0] = jnp.zeros(run.shape[1:], F32)

    def exps(i, carry):
        run[0] = run[0] + fold(jnp.add, jnp.exp(z_v[i] - top))
        return carry

    repeat(steps, exps)
    total = jnp.sum(run[0], axis=1, keepdims=True)
    label = jnp.sum(run[1], axis=1, keepdims=True)
    narrow = lax.broadcasted_iota(jnp.int32, (toks, LANES), 1)
    packed = jnp.where(narrow == 0, top, jnp.where(narrow == 1, total, jnp.where(narrow == 2, label, 0.0)))
    mine[ALL] = jnp.transpose(packed)[:SUB]
    stat = []
    for i in range(1, NTP):
        stat.append(rdma(mine, theirs.at[i], st_send.at[i], st_recv.at[i], to_tp(rem(at.tp + i, NTP))))
        stat[-1].start()
    theirs[0] = mine[ALL]
    spread.run(middle)
    for copy in stat:
        copy.wait_recv()
    parts = [theirs[rem(at.tp - j + NTP, NTP)] for j in range(NTP)]
    peak = functools.reduce(jnp.maximum, [p[0:1] for p in parts])
    total = functools.reduce(jnp.add, [p[1:2] * jnp.exp(p[0:1] - peak) for p in parts])
    label = functools.reduce(jnp.add, [p[2:3] for p in parts])
    lse = peak + jnp.log(total)
    loss = jnp.sum(jnp.log(total) + peak - label, axis=1, keepdims=True)
    sub = lax.broadcasted_iota(jnp.int32, (SUB, toks), 0)
    row_out[ALL] = jnp.where(sub == 0, lse, jnp.where(sub == 1, labels[ALL].astype(F32), 0.0))
    odd = rem(at.z, 2) == 1
    upper = lax.broadcasted_iota(jnp.int32, tile_out.shape, 1) >= 64
    every = ids[ALL].astype(F32)
    low = []
    for j in range(0, toks, LANES):
        pair = every[:, j : j + LANES]
        low += [pair, jnp.concatenate([pair[:, 64:], pair[:, :64]], axis=1)]
    low = jnp.concatenate(low, axis=0)
    high = jnp.concatenate([low[:, 64:], low[:, :64]], axis=1)
    tile_out[ALL] = jnp.where(upper == odd, jnp.where(odd, high, low), loss)
    tiles[0] = tile_out[ALL]
    rows_sent = []
    for i in range(NY - 1):
        to_y = to_dp(at.dp_of_y(NY - 1 - i))
        rows_sent.append(rdma(row_out, row_in.at[i], row_send.at[i], row_recv.at[i], to_y))
        rows_sent.append(rdma(tile_out, tile_in.at[i], t_send.at[i], t_recv.at[i], to_y))
    for copy in rows_sent:
        copy.start()
    run[0] = jnp.transpose(jnp.broadcast_to(lse, (LANES, toks)))
    inv_total = 1.0 / tok_total

    def put(i):
        half = rem(i, 2)
        return pltpu.make_async_copy(grad_v.at[half], grads.at[i], grad_sem.at[half])

    def backward(i, carry):
        start = start_of(i)
        shift = jnp.concatenate([run[0]] * (VT // LANES), axis=1)
        prob = jnp.exp(z_v[i] - shift)
        hit = (lane + start == lab_v[:, 0:1]) & (lane >= i * VT - start)

        @pl.when(i >= 2)
        def _():
            put(i - 2).wait()

        grad_v[rem(i, 2)] = ((prob - jnp.where(hit, 1.0, 0.0)) * inv_total).astype(BF16)
        put(i).start()
        return carry

    repeat(steps, backward)
    for i in range(max(0, steps - 2), steps):
        put(jnp.int32(i)).wait()
    spread.run(late)
    for e in spread.events:
        if e not in near:
            spread.take(e[0])
    for copy in rows_sent:
        copy.wait_recv()
    stats[0] = row_out[ALL]
    for i in range(NY - 1):
        stats[i + 1] = row_in[i]
        tiles[i + 1] = tile_in[i]
    keep.wait()
    spread.end()
    for copy in stat + rows_sent:
        copy.wait_send()


class SumZ:
    def __init__(self, at, parts, came, total, chunks, send, recv):
        self.at, self.parts, self.came, self.total = at, parts, came, total
        self.chunks, self.send, self.recv = chunks, send, recv
        self.last = at.nz // 2

    def rows(self, c, s, way):
        lo, hi = self.chunks[c]
        if s == 1:
            mid = lo + SUB * pl.cdiv(hi - lo, 16)
            lo, hi = (lo, mid) if way > 0 else (mid, hi)
        return pl.ds(lo, hi - lo)

    def slot(self, s, way):
        return 0 if s == 1 else 2 * (s - 1) - (way > 0)

    def goal(self, s, way):
        return rem(self.at.z + way * (self.last + 1 - s) + self.at.nz, self.at.nz)

    def copy(self, c, s, way):
        rows, w = self.rows(c, s, way), WAYS.index(way)
        sems = self.send.at[w, s, c], self.recv.at[w, s, c]
        src = self.parts.at[self.goal(s, way), rows]
        return rdma(src, self.came.at[self.slot(s, way), rows], *sems, to_dp(self.at.dp_of_z(way)))

    def begin(self, c):
        rows = pl.ds(self.chunks[c][0], self.chunks[c][1] - self.chunks[c][0])
        self.total[rows] = self.parts[self.at.z, rows]
        for way in WAYS:
            self.copy(c, 1, way).start()

    def run(self, c, s):
        for way in WAYS:
            self.copy(c, s, way).wait_recv()
            rows, slot = self.rows(c, s, way), self.slot(s, way)
            if s < self.last:
                goal = self.goal(s + 1, way)
                self.parts[goal, rows] = self.parts[goal, rows] + self.came[slot, rows]
                self.copy(c, s + 1, way).start()
            else:
                self.total[rows] = self.total[rows] + self.came[slot, rows]

    def end(self):
        for c in range(len(self.chunks)):
            for s in range(self.last):
                for way in WAYS:
                    self.copy(c, s + 1, way).wait_send()


def finish_kernel(
    nz, stride, vocab_loc, tok_total, row_plan, dh_plan, table_plan, chunks,
    table, ub, stats, grads, u, r, tiles,
    d_trunk, loss, stack, all_dh,
    pb, rl, fin, land, all_tiles, table_v, ub_v, grad_v, parts, came, total, dh_v, du, rows_v, logit_v,
    rs_send, rs_recv, row_send, row_recv, z_send, z_recv, i_send, i_recv, x_send, x_recv, s_send, s_recv, t_send, t_recv,
    load_sem, stage_sem, dh_sem, rows_sem, logit_sem,
):
    at = Place(nz)
    own, width = u.shape
    win, cols = total.shape
    toks = stats.shape[2]
    block = nz * own
    slab = LANES
    first = pl.multiple_of(at.y * stride, 16)
    loads = [
        pltpu.make_async_copy(table.at[pl.ds(first + lo, hi - lo)], table_v.at[lo:hi], copy_sem)
        for (lo, hi), copy_sem in zip(chunks, (load_sem, dh_sem.at[0], dh_sem.at[1]))
    ]

    depth, per = 4, toks // slab
    slabs = NY * per

    def staged(slot):
        return du.at[pl.ds(pl.multiple_of(slot * slab, slab), slab)]

    def fill(i):
        rows = pl.ds(pl.multiple_of(rem(i, per) * slab, slab), slab)
        slot = rem(i, depth)
        return pltpu.make_async_copy(ub.at[lax.div(i, jnp.int32(per)), rows], staged(slot), stage_sem.at[slot])

    loads[0].start()
    for i in range(depth):
        fill(jnp.int32(i)).start()
    steps = grads.shape[0]

    def start_of(i):
        return pl.multiple_of(jnp.minimum(i * VT, vocab_loc - VT), 16)

    def bring(i):
        half = rem(i, 2)
        return [
            pltpu.make_async_copy(table.at[pl.ds(start_of(i), VT)], rows_v.at[half], rows_sem.at[half]),
            pltpu.make_async_copy(grads.at[i], logit_v.at[half], logit_sem.at[half]),
        ]

    for copy in loads[1:] + bring(jnp.int32(0)):
        copy.start()
    met_all = greet(
        [to_tp(rem(at.tp + i, NTP)) for i in range(1, NTP)]
        + [to_dp(at.dp_of_z(i)) for i in range(1, nz)]
        + [to_dp(at.dp_of_y(way)) for way in WAYS]
    )
    sum_tp = SumTp(at, du, own, pb, rl, fin, rs_send, rs_recv)

    def narrow(n):
        def body(k, carry):
            i = n * per + k
            fill(i).wait()
            ub_v[pl.ds(pl.multiple_of(i * slab, slab), slab)] = staged(rem(i, depth))[ALL].astype(BF16)

            @pl.when(i + depth < slabs)
            def _():
                fill(i + depth).start()

            return carry

        repeat(per, body)

    loads[0].wait()
    narrow(0)

    inv_total = 1.0 / tok_total

    def logits(lo, hi, ahead=lambda n: None):
        vocab = at.tp * vocab_loc + first + lo + lax.broadcasted_iota(jnp.int32, (hi - lo, toks), 0)

        def body(n, carry):
            ahead(n)
            cut = pl.ds(pl.multiple_of(n * toks, LANES), toks)
            z = lax.dot_general(table_v[lo:hi, :], ub_v[cut, :], NT_DIMS, preferred_element_type=F32)
            row = stats[n]
            prob = jnp.exp(z - row[0:1])
            hit = vocab == row[1:2].astype(jnp.int32)
            grad_v[0 : hi - lo, cut] = ((prob - jnp.where(hit, 1.0, 0.0)) * inv_total).astype(BF16)
            return carry

        repeat(NY, body)

    def head(lo, hi):
        def body(n, carry):
            cut = pl.ds(pl.multiple_of(n * cols, LANES), cols)
            parts[n, lo:hi] = jnp.dot(grad_v[0 : hi - lo, :], ub_v[:, cut], preferred_element_type=F32)
            return carry

        repeat(nz, body)

    sums = SumZ(at, parts, came, total, chunks, s_send, s_recv)

    def sum_step(c, k):
        if k <= sums.last:
            sums.run(c, k)

    def narrow_next(n):
        @pl.when(n + 1 < NY)
        def _():
            narrow(n + 1)

    logits(*chunks[0], narrow_next)
    head(*chunks[0])
    met_all()
    sums.begin(0)
    known = [
        rdma(tiles, all_tiles.at[at.z], i_send.at[i], i_recv.at[i], to_dp(at.dp_of_z(i))) for i in range(1, nz)
    ]
    for copy in known:
        copy.start()
    all_tiles[at.z] = tiles[ALL]
    wide = min(512, width)
    du[ALL] = jnp.zeros(du.shape, F32)

    def backward(i, carry):
        for copy in bring(i):
            copy.wait()

        @pl.when(i + 1 < steps)
        def _():
            for copy in bring(i + 1):
                copy.start()

        @pl.when(i == min(5, steps - 1))
        def _():
            sum_step(0, 1)

        half = rem(i, 2)
        for n in range(width // wide):
            cut = pl.ds(n * wide, wide)
            du[:, cut] = du[:, cut] + jnp.dot(logit_v[half], rows_v[half, :, cut], preferred_element_type=F32)
        return carry

    repeat(steps, backward)
    sum_tp.begin()
    sum_step(0, 2)
    for copy in loads[1:]:
        copy.wait()
    logits(*chunks[1])
    sum_tp.pass_on()
    head(*chunks[1])
    sums.begin(1)
    sum_tp.join()
    sum_step(0, 3)
    logits(*chunks[2])
    head(*chunks[2])
    grad = sum_tp.result()
    normed = u[ALL]
    mean_g = jnp.mean(grad, axis=-1, keepdims=True)
    mean_gu = jnp.mean(grad * normed, axis=-1, keepdims=True)
    land[at.tp] = r[:, 0:1] * (grad - mean_g - normed * mean_gu)

    def row_block(dx, dy, cross, lo, hi):
        return land.at[at.tp_of(dx, cross), pl.ds(lo, hi - lo)]

    whole_rows = Spread(at, row_plan, own, row_block, row_send, row_recv)
    whole_rows.begin()
    here = pl.ds(pl.multiple_of(at.z * own, own), own)
    turned = []
    for i in range(1, nz):
        col, to_z = pl.multiple_of(rem(at.z + i, nz) * cols, LANES), to_dp(at.dp_of_z(i))
        src = land.at[at.tp, :, pl.ds(col, cols)]
        turned.append(rdma(src, all_dh.at[at.tp, 0, here], z_send.at[i], z_recv.at[i], to_z))
    for copy in turned:
        copy.start()
    my_col = pl.multiple_of(at.z * cols, LANES)
    mine = pltpu.make_async_copy(land.at[at.tp, :, pl.ds(my_col, cols)], all_dh.at[at.tp, 0, here], load_sem)
    mine.start()
    sums.begin(2)
    sum_step(1, 1)
    sum_step(0, 4)
    whole_rows.run(whole_rows.events)
    mine.wait()
    for copy in turned + known:
        copy.wait_recv()

    def dh_block(dx, dy, cross, lo, hi):
        return all_dh.at[at.tp_of(dx, cross), dy % NY, pl.ds(lo, hi - lo)]

    blocks = Spread(at, dh_plan, block, dh_block, x_send, x_recv)
    blocks.begin()

    pieces = {(0, 0): [(blocks.count, [], 0)]}
    for e in blocks.events:
        dx, dy = blocks.goal(e[0])
        pieces.setdefault((dx % NX, dy % NY), []).append(e)
    order = sorted((pieces[p][-1][-1] + cross * (block // 3), *p, cross) for p in pieces for cross in range(2))
    left = list(blocks.events)
    due = []
    for time, dx, dy, cross in order:
        due.append([e for e in left if e[-1] <= time])
        left = [e for e in left if e[-1] > time]
    code = [dx + NX * (dy + NY * cross) for _, dx, dy, cross in order]
    ready = 2

    def meet(k):
        blocks.run(due[k])
        _, dx, dy, cross = order[k]
        if cross:
            for part in pieces[dx, dy]:
                blocks.take(part[0])

    for k in range(ready):
        meet(k)
    for i in range(whole_rows.count + 1):
        whole_rows.take(i)
    ub_v[0:toks] = land[ALL].reshape(toks, width).astype(BF16)
    keep_rows = pltpu.make_async_copy(ub_v.at[0:toks], d_trunk, rows_sem.at[0])
    keep_rows.start()
    upper = lax.broadcasted_iota(jnp.int32, loss.shape, 1) >= 64
    loss[ALL] = sum(
        jnp.where(upper == (z % 2 == 0), all_tiles[z, rem(y - at.y + NY, NY)], 0.0) for z in range(nz) for y in range(NY)
    )

    beside = {k: (c, step) for k, c, step in BESIDE if step <= sums.last}
    low = (at.tp * vocab_loc + at.y * stride).astype(F32)

    def place_of(e):
        mark = jnp.int32(code[0])
        for k in range(1, len(order)):
            mark = jnp.where(e == k, code[k], mark)
        core = jnp.where(mark >= NX * NY, 1 - at.c, at.c)
        return 2 * rem(at.x + rem(mark, NX), NX) + core, rem(lax.div(mark, jnp.int32(NX)), NY)

    def fetch(e):
        tp, far = place_of(e)
        half = rem(e, 2)
        return pltpu.make_async_copy(all_dh.at[tp, far], dh_v.at[half], dh_sem.at[half])

    def piece(e, carry):
        for k in range(len(order)):
            met = k + 1 if k + 1 < len(order) and k + 1 >= ready else 0
            if k in beside or met:

                @pl.when(e == k)
                def _(k=k, met=met):
                    if k in beside:
                        sums.run(*beside[k])
                    if met:
                        meet(met)

        @pl.when(e + 1 < len(order))
        def _():
            fetch(e + 1).start()

        tp, far = place_of(e)
        ids = jnp.concatenate(
            [
                jnp.where(upper[0:1], all_tiles[2 * j + 1, far, pl.ds(tp, 1), :], all_tiles[2 * j, far, pl.ds(tp, 1), :])
                for j in range(nz // 2)
            ],
            axis=1,
        )
        fetch(e).wait()
        dh = dh_v[rem(e, 2)]
        hi = dh.astype(BF16)
        rest = dh - hi.astype(F32)
        mid = rest.astype(BF16)
        lo = (rest - mid.astype(F32)).astype(BF16)
        ids = (ids - low).astype(jnp.int32)
        for begin, end in chunks:
            row = lax.broadcasted_iota(jnp.int32, (end - begin, block), 0) + begin
            pick = jnp.where(row == ids, 1.0, 0.0).astype(BF16)
            found = sum(jnp.dot(pick, term, preferred_element_type=F32) for term in (hi, mid, lo))
            total[begin:end] = total[begin:end] + found
        return carry

    fetch(jnp.int32(0)).start()
    repeat(len(order), piece)
    for copy in turned + known:
        copy.wait_send()

    sends, starts, events = table_plan
    device = {(0, way): to_dp(at.dp_of_z(way)) for way in WAYS} | {(1, way): to_dp(at.dp_of_y(way)) for way in WAYS}

    def copy_of(i, arrives=False):
        axis, way, off, lo, hi = sends[i]
        if arrives:
            off = tuple(o - way * (a == axis) for a, o in enumerate(off))
        dst = stack.at[rem(at.z + off[0] + nz, nz), at.y_of(off[1]), pl.ds(lo, hi - lo)]
        src = dst if any(off) else total.at[pl.ds(lo, hi - lo)]
        return rdma(src, dst, t_send.at[i], t_recv.at[i], device[axis, way])

    for c in range(1, len(chunks)):
        sum_step(c, 4)
    for i in sum(starts, []):
        copy_of(i).start()
    keep = pltpu.make_async_copy(total, stack.at[at.z, at.y], load_sem)
    keep.start()
    for i, new, _ in events:
        copy_of(i, True).wait_recv()
        for j in new:
            copy_of(j).start()
    keep.wait()
    keep_rows.wait()
    for i in range(len(sends)):
        copy_of(i).wait_send()
    sums.end()
    whole_rows.end()
    blocks.end()


def pick_kernel(ids_s, table, ids, out, eights, local, sem):
    toks = out.shape[0]
    rows = table.shape[0]
    begin = lax.axis_index("tp") * rows
    block = 32

    parts = sem.shape[0]
    part = toks // parts

    def start(q):
        def fetch(t, carry):
            row = ids_s[0, t] - begin
            spare = t * SUB
            here = (row | (rows - 1 - row)) >= 0
            eight = pl.multiple_of(jnp.where(here, row & -SUB, spare), SUB)
            mine = eights.at[pl.ds(pl.multiple_of(spare, SUB), SUB)]
            pltpu.make_async_copy(table.at[pl.ds(eight, SUB)], mine, sem.at[q]).start()
            return carry

        lax.fori_loop(q * part, (q + 1) * part, fetch, 0, unroll=2 * SUB)

    start(0)
    local[ALL] = columns(ids[ALL]) - begin
    for q in range(1, AHEAD):
        start(q)
    lane = lax.broadcasted_iota(jnp.int32, (block, SUB * block), 1)
    first = SUB * lax.broadcasted_iota(jnp.int32, (block, SUB * block), 0)

    def choose(b, carry):
        at = pl.multiple_of(b * block, block)
        row = local[pl.ds(at, block), 0:1]
        hit = (lane - first == rem(row, SUB)) & (row >= 0) & (row < rows)
        some = eights[pl.ds(pl.multiple_of(at * SUB, SUB), SUB * block), :]
        out[pl.ds(at, block)] = jnp.dot(
            jnp.where(hit, 1.0, 0.0).astype(BF16), some, preferred_element_type=F32
        ).astype(BF16)
        return carry

    for q in range(parts):
        if q + AHEAD < parts:
            start(q + AHEAD)
        whole = pl.ds(q * part * SUB, part * SUB)
        pltpu.make_async_copy(table.at[pl.ds(0, part * SUB)], eights.at[whole], sem.at[q]).wait()
        lax.fori_loop(q * part // block, (q + 1) * part // block, choose, 0)


def place_kernel(chunk, tok_total, stack, rows_in, loss_in, out, rows_out, loss_out, slots, rows_v, rest_v, load_sem, store_sem, rows_sem, rest_sem):
    nz, ny, have, cols = stack.shape
    depth = slots.shape[0]
    per = have // chunk
    total = ny * per
    ahead = depth // 2

    def loads(i):
        y, row = lax.div(i, jnp.int32(per)), pl.multiple_of(rem(i, per) * chunk, SUB)
        s = rem(i, depth)
        return [
            pltpu.make_async_copy(
                stack.at[j, y, pl.ds(row, chunk)], slots.at[s, :, pl.ds(j * cols, cols)], load_sem.at[s, j]
            )
            for j in range(nz)
        ]

    def store(i):
        s, row = rem(i, depth), pl.multiple_of(i * chunk, SUB)
        return pltpu.make_async_copy(slots.at[s], out.at[pl.ds(row, chunk)], store_sem.at[s])

    rows_load = pltpu.make_async_copy(rows_in, rows_v, rows_sem)
    rows_store = pltpu.make_async_copy(rows_v, rows_out, rows_sem)
    used = per * chunk
    left = have - used
    rest = pltpu.make_async_copy(stack.at[:, ny - 1, pl.ds(used, left)], rest_v, rest_sem.at[0])
    tails = [
        pltpu.make_async_copy(rest_v.at[j], out.at[pl.ds(ny * used, left), pl.ds(j * cols, cols)], rest_sem.at[j])
        for j in range(nz)
    ]

    def prime(i, carry):
        for copy in loads(i):
            copy.start()
        return carry

    def body(i, carry):
        for copy in loads(i):
            copy.wait()
        store(i).start()

        @pl.when(i == ahead)
        def _():
            rows_load.wait()
            rows_store.start()
            rest.wait()
            for copy in tails:
                copy.start()

        @pl.when(i + ahead < total)
        def _():
            @pl.when(i >= ahead)
            def _():
                store(i - ahead).wait()

            for copy in loads(i + ahead):
                copy.start()

        return carry

    def drain(i, carry):
        store(i).wait()
        return carry

    repeat(ahead, prime)
    rows_load.start()
    rest.start()
    lane = lax.broadcasted_iota(jnp.int32, (1, LANES), 1)
    loss_out[0, 0] = jnp.sum(jnp.where(rem(lane, 64) == 0, loss_in[0:1], 0.0)) / tok_total
    repeat(total, body)
    lax.fori_loop(total - 2 * ahead, total, drain, 0)
    for copy in tails:
        copy.wait()
    rows_store.wait()


def vmem():
    return pl.BlockSpec(memory_space=pltpu.VMEM)


def anywhere():
    return pl.BlockSpec(memory_space=pl.ANY)


def dma(*shape):
    return pltpu.SemaphoreType.DMA(shape)


def twice(*shape):
    return [dma(*shape)] * 2


def solution(mesh):
    ndp, ntp = mesh.shape["dp"], mesh.shape["tp"]
    nz = ndp // NY

    def per_device(table, ids, labels, trunk):
        vocab_loc, width = table.shape
        batch, seq = ids.shape
        toks = batch * seq
        own = toks // NTP
        tok_total = toks * ndp
        stride = (vocab_loc - 16) // NY
        win = stride + 16
        cols = width // nz
        block = nz * own
        big = 66_000_000
        tp_sems = twice(10)
        tp_scratch = [
            pltpu.VMEM((4, own, width), F32),
            pltpu.VMEM((2, own // 2, width), F32),
            pltpu.VMEM((4, own // 2, width), F32),
            pltpu.VMEM((NTP, own, width), F32),
        ]
        ids, labels = ids.reshape(1, toks), labels.reshape(1, toks)
        part = pl.pallas_call(
            pick_kernel,
            out_shape=jax.ShapeDtypeStruct((toks, width), BF16),
            in_specs=[pl.BlockSpec(memory_space=pltpu.SMEM), anywhere(), vmem()],
            out_specs=vmem(),
            scratch_shapes=[pltpu.VMEM((SUB * toks, width), BF16), pltpu.VMEM((toks, LANES), jnp.int32), dma(SUB)],
            compiler_params=pltpu.CompilerParams(vmem_limit_bytes=big),
            name="pick",
        )(ids, table, ids)
        steps = pl.cdiv(vocab_loc, VT)
        token_plan = gather_plan((NX, NY), two_colours(0, own, 0.5), 16, hold=2 * own)
        sends = 2 * len(token_plan[0]) + 1
        grads, ub, u_own, r_own, stats, tiles = pl.pallas_call(
            functools.partial(token_kernel, nz, tok_total, token_plan),
            out_shape=(
                jax.ShapeDtypeStruct((steps, toks, VT), BF16),
                jax.ShapeDtypeStruct((NY, NTP, own, width), F32),
                jax.ShapeDtypeStruct((own, width), F32),
                jax.ShapeDtypeStruct((own, LANES), F32),
                jax.ShapeDtypeStruct((NY, SUB, toks), F32),
                jax.ShapeDtypeStruct((NY, SUB, LANES), F32),
            ),
            in_specs=[anywhere(), anywhere(), anywhere(), vmem(), vmem()],
            out_specs=(anywhere(), anywhere(), vmem(), vmem(), vmem(), vmem()),
            scratch_shapes=[
                pltpu.VMEM((toks, LANES), jnp.int32),
                pltpu.VMEM((toks, width), F32),
                pltpu.VMEM((own, width), BF16),
                pltpu.VMEM((2, toks, VT), BF16),
                pltpu.VMEM((vocab_loc, width), BF16),
                pltpu.VMEM((toks, width), BF16),
                pltpu.VMEM((steps, toks, VT), F32),
                pltpu.VMEM((2, toks, LANES), F32),
                pltpu.VMEM((SUB, toks), F32),
                pltpu.VMEM((NTP, SUB, toks), F32),
                pltpu.VMEM((SUB, toks), F32),
                pltpu.VMEM((NY - 1, SUB, toks), F32),
                pltpu.VMEM((SUB, LANES), F32),
                pltpu.VMEM((NY - 1, SUB, LANES), F32),
                *tp_scratch,
                dma(steps), pltpu.SemaphoreType.DMA, *twice(NTP), *twice(NY - 1), *twice(NY - 1), *tp_sems, *twice(sends), dma(2),
            ],
            compiler_params=pltpu.CompilerParams(collective_id=0, has_side_effects=True, vmem_limit_bytes=big),
            name="token",
        )(table, part, trunk.reshape(toks, width), labels, ids)

        row_plan = gather_plan((NX, 1), two_colours(0, own, 1), 16)
        dh_plan = gather_plan((NX, NY), two_colours(0, block, 0.5), block // 4)
        lead = 16 * pl.cdiv(win, 48)
        middle = 2 * lead
        chunks = ((0, lead), (lead, middle), (middle, win))
        third = SUB * pl.cdiv(win, 24)
        table_chunks = ((0, third), (third, 2 * third), (2 * third, win))
        shares = SHARES if nz == SUB else (0.5,) * 3
        table_parts = sum((two_colours(lo, hi, share) for (lo, hi), share in zip(table_chunks, shares)), [])
        table_plan = gather_plan((nz, NY), table_parts, 60)
        counts = [2 * len(p[0]) + 1 for p in (row_plan, dh_plan, table_plan)]
        zs = (2, nz // 2 + 1, len(chunks))
        d_rows, loss, stack, _ = pl.pallas_call(
            functools.partial(
                finish_kernel, nz, stride, vocab_loc, tok_total, row_plan, dh_plan, table_plan, chunks
            ),
            out_shape=(
                jax.ShapeDtypeStruct((toks, width), BF16),
                jax.ShapeDtypeStruct((SUB, LANES), F32),
                jax.ShapeDtypeStruct((nz, NY, win, cols), F32),
                jax.ShapeDtypeStruct((NTP, NY, block, cols), F32),
            ),
            in_specs=[anywhere(), anywhere(), vmem(), anywhere(), vmem(), vmem(), vmem()],
            out_specs=(anywhere(), vmem(), anywhere(), anywhere()),
            scratch_shapes=[
                *tp_scratch,
                pltpu.VMEM((nz, NY, SUB, LANES), F32),
                pltpu.VMEM((win, width), BF16),
                pltpu.VMEM((NY * toks, width), BF16),
                pltpu.VMEM((middle - lead, NY * toks), BF16),
                pltpu.VMEM((nz, win, cols), F32),
                pltpu.VMEM((nz - 1, win, cols), F32),
                pltpu.VMEM((win, cols), F32),
                pltpu.VMEM((2, block, cols), F32),
                pltpu.VMEM((toks, width), F32),
                pltpu.VMEM((2, VT, width), BF16),
                pltpu.VMEM((2, toks, VT), BF16),
                *tp_sems, *twice(counts[0]), *twice(nz), *twice(nz), *twice(counts[1]), *twice(*zs), *twice(counts[2]),
                pltpu.SemaphoreType.DMA, dma(4), *twice(2), dma(2),
            ],
            compiler_params=pltpu.CompilerParams(collective_id=1, has_side_effects=True, vmem_limit_bytes=67_000_000),
            name="finish",
        )(table, ub.reshape(NY, toks, width), stats, grads, u_own, r_own, tiles)
        depth = 16 if nz == SUB else SUB
        chunk = next(n for n in range(112, 0, -SUB) if stride % n == 0 and NY * stride >= n * depth)
        d_table, d_rows, mean_loss = pl.pallas_call(
            functools.partial(place_kernel, chunk, tok_total),
            out_shape=(
                jax.ShapeDtypeStruct((vocab_loc, width), F32),
                jax.ShapeDtypeStruct((toks, width), BF16),
                jax.ShapeDtypeStruct((1, 1), F32),
            ),
            in_specs=[anywhere(), anywhere(), vmem()],
            out_specs=(anywhere(), anywhere(), pl.BlockSpec(memory_space=pltpu.SMEM)),
            scratch_shapes=[
                pltpu.VMEM((depth, chunk, width), F32), pltpu.VMEM((toks, width), BF16),
                pltpu.VMEM((nz, win - stride, cols), F32), dma(depth, nz), dma(depth), pltpu.SemaphoreType.DMA, dma(nz),
            ],
            compiler_params=pltpu.CompilerParams(vmem_limit_bytes=big),
            name="place",
        )(stack, d_rows, loss)
        return mean_loss.reshape(()), d_rows.reshape(trunk.shape), d_table

    return jax.shard_map(
        per_device,
        mesh=mesh,
        in_specs=(P("tp", None), P("dp", None), P("dp", None), P("dp", None, None)),
        out_specs=(P(), P("dp", None, None), P("tp", None)),
        check_vma=False,
    )
```
